256 devices in a mesh: groups: 2 (over y), tx: 16 (over z), ty: 4 (over x), ka: 2 (over core).
Axes of the slice: x: 4, y: 2, z: 16, core: 2. Of those that a mesh axis runs over, the one named last changes fastest.
The devices are a block of a 4x16x16 slice.
Arguments:
- mask_raster: float32 [8192, 1024], P(('groups', 'tx'), 'ty'), parts along dimension 0, may hold values from 0 to 1
- frag_rows: int32 [32, 4, 512], P(('groups', 'tx'), 'ty'), parts along dimension 0, may hold values from 8 to 215
- frag_cols: int32 [32, 4, 512], P(('groups', 'tx'), 'ty'), parts along dimension 0, may hold values from 8 to 215
- frag_length: int32 [32, 4, 512], P(('groups', 'tx'), 'ty'), parts along dimension 0, may hold values from 4 to 32
- frag_orient: int32 [32, 4, 512], P(('groups', 'tx'), 'ty'), parts along dimension 0, may hold values from 0 to 1
- frag_moves: int32 [32, 4, 2, 512], P(('groups', 'tx'), 'ty'), parts along dimension 0, may hold values from -4 to 4
- site_rows: int32 [32, 4, 2048], P(('groups', 'tx'), 'ty'), parts along dimension 0, may hold values from 1 to 254
- site_cols: int32 [32, 4, 2048], P(('groups', 'tx'), 'ty'), parts along dimension 0, may hold values from 1 to 254
- spectra: float32 [16, 2, 128, 128], P('ka'), may hold values from -24 to 24
- weights: float32 [16], P('ka'), may hold values from 0.05 to 1
- tolerance: int32 [2], replicated, may hold values from 1 to 16
Outputs:
- intensity: float32 [8192, 1024], P(('groups', 'tx'), 'ty'), parts along dimension 0
- corrected_mask: float32 [8192, 1024], P(('groups', 'tx'), 'ty'), parts along dimension 0
- edge_errors: float32 [32, 4, 2, 2048], P(('groups', 'tx'), 'ty'), parts along dimension 0
- peak_error: float32 [4], P('groups'), parts along dimension 0
- converged_share: float32 [4], P('groups'), parts along dimension 0
The draws below stay inside these ranges and needn't reach their ends.
There are 2 independent parts, one for each index of `groups`. The reference program is written for one: setup_inputs(seed, part) draws one part's arguments, and reference() takes and returns one part's arrays. A program takes and returns all parts, laid end to end along the dimension named above; an argument that names none is the same for every part. Nothing has to cross between parts.
All inputs are finite; a program needn't handle non-finite values.
Results may differ from the reference program's by a relative error of at most 0.0003.
Values sent between devices are 32-bit elements; how exact they have to be, the bound alone decides.
A program may use at most 64 MiB of HBM per device.

```python
import math
import jax
import jax.numpy as jnp
from jax import lax

TILE = 256
HALO = 128
BAND = 128
KERNELS = 16
NFRAG = 512
SITES = 2048
ITERS = 2
ROWS = 4096
COLS = 1024
N_TX = 16
N_TY = 4


def draw_spectra(key, part):
    shape = (KERNELS, 2, BAND, BAND)
    scale = (TILE + 2 * HALO) / BAND
    values = jnp.clip(jax.random.normal(key, shape, jnp.float32), -6.0, 6.0)
    first = jnp.arange(BAND)[:, None] == BAND // 2
    second = jnp.arange(BAND)[None, :] == BAND // 2
    factor = jnp.where(first & second, 0.02, 1.0)
    return (values * scale * factor[None, None]).astype(jnp.float32)


def plant(drawn, key, low, top_value):
    spot = [jax.random.randint(jax.random.fold_in(key, axis), (), 0, length) for axis, length in enumerate(drawn.shape)]
    main_axis = drawn.shape.index(max(drawn.shape))
    neighbour = spot[:main_axis] + [(spot[main_axis] + 1) % drawn.shape[main_axis]] + spot[main_axis + 1:]
    return drawn.at[tuple(spot)].set(low).at[tuple(neighbour)].set(top_value)


def steps_of(stream_key, dims, pieces, low, largest):
    loudness = 1.0
    for dim, shards_of in pieces:
        heights = jax.random.uniform(jax.random.fold_in(jax.random.fold_in(stream_key, 6), dim), (shards_of,), jnp.float32, low / len(pieces), largest / len(pieces))
        loudness = loudness * jnp.repeat(jnp.exp(heights), dims[dim] // shards_of).reshape((-1,) + (1,) * (len(dims) - 1 - dim))
    return loudness


def setup_inputs(seed: int = 0, part: int = 0) -> dict:
    key_list = jax.random.split(jax.random.key(seed), 12)
    part_keys = jax.random.split(jax.random.fold_in(key_list[11], part), 12)
    mask_raster = jnp.clip(1.0 * jax.random.uniform(part_keys[0], (ROWS, COLS), jnp.float32) ** steps_of(part_keys[0], (ROWS, COLS), ((0, 16), (1, 4)), -0.2, 0.2), 0.0, 1.0)
    frag_rows = plant(jax.random.randint(part_keys[1], (N_TX, N_TY, NFRAG), 8, TILE - 40), jax.random.fold_in(part_keys[1], 1), 8, (TILE - 40) - 1).astype(jnp.int32)
    frag_cols = plant(jax.random.randint(part_keys[2], (N_TX, N_TY, NFRAG), 8, TILE - 40), jax.random.fold_in(part_keys[2], 1), 8, (TILE - 40) - 1).astype(jnp.int32)
    frag_length = plant(jax.random.randint(part_keys[3], (N_TX, N_TY, NFRAG), 4, 33), jax.random.fold_in(part_keys[3], 1), 4, 32).astype(jnp.int32)
    frag_orient = plant(jax.random.randint(part_keys[4], (N_TX, N_TY, NFRAG), 0, 2), jax.random.fold_in(part_keys[4], 1), 0, 1).astype(jnp.int32)
    frag_moves = plant(jax.random.randint(part_keys[5], (N_TX, N_TY, ITERS, NFRAG), -4, 5), jax.random.fold_in(part_keys[5], 1), -4, 4).astype(jnp.int32)
    site_rows = plant(jax.random.randint(part_keys[6], (N_TX, N_TY, SITES), 1, TILE - 1), jax.random.fold_in(part_keys[6], 1), 1, (TILE - 1) - 1).astype(jnp.int32)
    site_cols = plant(jax.random.randint(part_keys[7], (N_TX, N_TY, SITES), 1, TILE - 1), jax.random.fold_in(part_keys[7], 1), 1, (TILE - 1) - 1).astype(jnp.int32)
    spectra = draw_spectra(jax.random.fold_in(key_list[11], 71), part)
    weights = jnp.clip(jnp.exp(math.log(1.0) - 2.9957323 * jax.random.uniform(key_list[9], (KERNELS,), jnp.float32) ** steps_of(key_list[9], (KERNELS,), ((0, 2),), -0.2, 0.2)), 0.05, 1.0)
    tolerance = jax.random.randint(key_list[10], (ITERS,), 1, 17).astype(jnp.int32)
    return {"mask_raster": mask_raster, "frag_rows": frag_rows, "frag_cols": frag_cols, "frag_length": frag_length, "frag_orient": frag_orient, "frag_moves": frag_moves, "site_rows": site_rows, "site_cols": site_cols, "spectra": spectra, "weights": weights, "tolerance": tolerance}


LEVEL = 0.4
SLOPE_FLOOR = 0.05
SHARPNESS = 8.0

def strip_sum(row_start, col_start, frag_len, orient, shift, extent):
    lower = jnp.minimum(shift, 0)
    upper = jnp.maximum(shift, 0)
    along_rows = orient == 0
    row_low = jnp.where(along_rows, row_start, row_start + lower)
    row_high = jnp.where(along_rows, row_start + frag_len, row_start + upper)
    col_low = jnp.where(along_rows, col_start + lower, col_start)
    col_high = jnp.where(along_rows, col_start + upper, col_start + frag_len)
    position = jnp.arange(extent, dtype=jnp.int32)
    signs = jnp.sign(shift).astype(jnp.float32)
    row_select = ((position[:, None] >= row_low[None, :]) & (position[:, None] < row_high[None, :])).astype(jnp.float32) * signs[None, :]
    col_select = ((position[None, :] >= col_low[:, None]) & (position[None, :] < col_high[:, None])).astype(jnp.float32)
    return jnp.dot(row_select.astype(jnp.bfloat16), col_select.astype(jnp.bfloat16), preferred_element_type=jnp.float32)

def edge_error(image, rows_at, cols_at):
    flat = image.reshape(-1)
    width = image.shape[1]

    def sample(delta_row, delta_col):
        return flat[(rows_at + delta_row) * width + cols_at + delta_col]
    center = sample(0, 0)
    grad_rows = (sample(1, 0) - sample(-1, 0)) * 0.5
    grad_cols = (sample(0, 1) - sample(0, -1)) * 0.5
    slope = jnp.sqrt(grad_rows * grad_rows + grad_cols * grad_cols)
    return (center - LEVEL) / jnp.maximum(slope, SLOPE_FLOOR)

def reference(mask_raster, frag_rows, frag_cols, frag_length, frag_orient, frag_moves, site_rows, site_cols, spectra, weights, tolerance):
    tiles_x = mask_raster.shape[0] // TILE
    tiles_y = mask_raster.shape[1] // TILE
    count = tiles_x * tiles_y
    ext_size = TILE + 2 * HALO
    freq = (jnp.arange(BAND, dtype=jnp.int32) - BAND // 2) % ext_size
    kernel_spec = spectra[:, 0] + 1j * spectra[:, 1]
    current = mask_raster
    flat_rows = frag_rows.reshape(count, NFRAG)
    flat_cols = frag_cols.reshape(count, NFRAG)
    flat_len = frag_length.reshape(count, NFRAG)
    flat_orient = frag_orient.reshape(count, NFRAG)
    errors_all = []
    peaks = []
    shares = []
    images = None
    for iteration in range(ITERS):
        flat_moves = frag_moves[:, :, iteration, :].reshape(count, NFRAG)
        strips = lax.map(lambda items: strip_sum(items[0], items[1], items[2], items[3], items[4], TILE), (flat_rows, flat_cols, flat_len, flat_orient, flat_moves))
        region = strips.reshape(tiles_x, tiles_y, TILE, TILE).transpose(0, 2, 1, 3).reshape(tiles_x * TILE, tiles_y * TILE)
        current = jnp.clip(current + region, 0.0, 1.0)
        padded = jnp.pad(current, HALO)

        def image_tile(number):
            first = (number // tiles_y * TILE).astype(jnp.int32)
            second = (number % tiles_y * TILE).astype(jnp.int32)
            window = lax.dynamic_slice(padded, (first, second), (ext_size, ext_size))
            spectrum = jnp.fft.fft2(window)
            kept = spectrum[freq][:, freq]
            product = kernel_spec * kept[None]
            full = jnp.zeros((product.shape[0], ext_size, ext_size), product.dtype)
            full = full.at[:, freq[:, None], freq[None, :]].set(product)
            field = jnp.fft.ifft2(full, axes=(1, 2))[:, HALO:HALO + TILE, HALO:HALO + TILE]
            return lax.optimization_barrier(jnp.sum(weights[:, None, None] * (field.real * field.real + field.imag * field.imag), axis=0))
        images = lax.map(image_tile, jnp.arange(count, dtype=jnp.int32))
        errors_now = jax.vmap(edge_error)(images, site_rows.reshape(count, SITES), site_cols.reshape(count, SITES))
        errors_all.append(errors_now.reshape(tiles_x, tiles_y, SITES))
        peaks.append(jnp.max(jnp.abs(errors_now)))
        limit = tolerance[iteration].astype(jnp.float32) / 8.0
        shares.append(jnp.mean(jax.nn.sigmoid(SHARPNESS * (limit - jnp.abs(errors_now)))))
    intensity = images.reshape(tiles_x, tiles_y, TILE, TILE).transpose(0, 2, 1, 3).reshape(tiles_x * TILE, tiles_y * TILE)
    edge_errors = jnp.stack(errors_all, axis=2)
    return (intensity, current, edge_errors, jnp.stack(peaks), jnp.stack(shares))
```

```python
import functools
import math

import jax
import jax.numpy as jnp
import numpy as np
from jax import lax
from jax.experimental import pallas as pl
from jax.experimental.pallas import tpu as pltpu
from jax.sharding import PartitionSpec as P

HALO = 128
BAND = 128
ITERS = 2
LEVEL = 0.4
SLOPE_FLOOR = 0.05
SHARPNESS = 8.0
HIGHEST = lax.Precision.HIGHEST
MESH = pl.DeviceIdType.MESH
SIN_AT = 72
PACKED = 136


def bf16_pieces(x, count):
    pieces = []
    for _ in range(count):
        pieces.append(x.astype(jnp.bfloat16))
        x = x - pieces[-1].astype(jnp.float32)
    return pieces


def host_pieces(x):
    pieces = []
    for _ in range(3):
        pieces.append(x.astype(jnp.bfloat16))
        x = x - pieces[-1].astype(np.float64)
    return pieces


def tables(tile):
    ext = tile + 2 * HALO
    half = tile // 2
    theta = 2.0 * math.pi / ext
    inside = np.arange(ext) - (ext - 1) / 2
    low = BAND // 2
    rows = np.zeros((PACKED, ext))
    rows[: low + 1] = np.cos(theta * np.outer(np.arange(low + 1), inside))
    rows[SIN_AT : SIN_AT + low] = np.sin(theta * np.outer(np.arange(1, low + 1), inside))
    freq = np.arange(BAND) - low
    turns = theta * np.outer(inside, freq)
    cols = np.concatenate([np.cos(turns), np.sin(turns)], axis=1)
    expand = np.zeros((2 * BAND, PACKED))
    for u, f in enumerate(freq):
        expand[u, abs(f)] = 1.0
        if f != 0:
            expand[BAND + u, SIN_AT + abs(f) - 1] = np.sign(f)
    out = theta * np.outer(freq, np.arange(half) + 0.5)
    basis = np.concatenate([np.cos(out), np.sin(out)], axis=1)
    hi, mid, lo = host_pieces(basis)
    first = np.stack([np.concatenate(b, axis=0) for b in ((hi, hi), (mid, mid), (lo, hi))])
    second = np.ascontiguousarray(first.swapaxes(1, 2))
    flip = np.eye(half)[::-1]
    f32 = np.float32
    return rows.astype(f32), cols.astype(f32), expand.astype(f32), first, second, flip.astype(f32)


def exact(left, right):
    return jnp.dot(left, right, precision=HIGHEST, preferred_element_type=jnp.float32)


def dot(left, right):
    return jnp.dot(left, right, preferred_element_type=jnp.float32)


def halo_kernel(
    mask, rows_at, cols_at, lengths, orients, moves, spectra, weights, row_dft, col_dft, expand,
    new_mask, spec_re, spec_im, other_spectra, other_weights,
    current, above, below, packed, left, right, my_weights, send_sem, recv_sem,
):
    tx, ty, ka = lax.axis_index("tx"), lax.axis_index("ty"), lax.axis_index("ka")
    tile = mask.shape[0]
    ext = tile + 2 * HALO
    has_up, has_down = tx > 0, tx < lax.axis_size("tx") - 1
    has_left, has_right = ty > 0, ty < lax.axis_size("ty") - 1
    barrier = pltpu.get_barrier_semaphore()
    near = ((has_up, "tx", tx - 1), (has_down, "tx", tx + 1), (has_left, "ty", ty - 1), (has_right, "ty", ty + 1))
    for there, axis, index in near:
        @pl.when(there)
        def _():
            pl.semaphore_signal(barrier, inc=1, device_id={axis: index}, device_id_type=MESH)
    pl.semaphore_signal(barrier, inc=1, device_id={"ka": 1 - ka}, device_id_type=MESH)

    for k in range(my_weights.shape[0]):
        my_weights[pl.ds(k, 1), :] = jnp.full((1, my_weights.shape[1]), weights[k], jnp.float32)
    position = lax.broadcasted_iota(jnp.int32, (tile, rows_at.shape[2]), 0)
    row, col, length = rows_at[0], cols_at[0], lengths[0]
    along = orients[0] == 0
    steps = [mask[...]]
    for t in range(ITERS):
        move = moves[0, 0, t : t + 1, :]
        lower, upper = jnp.minimum(move, 0), jnp.maximum(move, 0)
        row_low = jnp.where(along, row, row + lower)
        row_high = jnp.where(along, row + length, row + upper)
        col_low = jnp.where(along, col + lower, col)
        col_high = jnp.where(along, col + upper, col + length)
        sign = jnp.where(move > 0, 1.0, 0.0) - jnp.where(move < 0, 1.0, 0.0)
        in_rows = jnp.where((position >= row_low) & (position < row_high), sign, 0.0)
        in_cols = jnp.where((position >= col_low) & (position < col_high), 1.0, 0.0)
        strips = lax.dot_general(
            in_rows.astype(jnp.bfloat16), in_cols.astype(jnp.bfloat16), (((1,), (1,)), ((), ())),
            preferred_element_type=jnp.float32,
        )
        steps.append(jnp.clip(steps[-1] + strips, 0.0, 1.0))
    new_mask[...] = steps[2]
    current[...] = jnp.where(ka == 0, steps[1], steps[2])

    count = sum(there.astype(jnp.int32) for there, _, _ in near) + 1
    pl.semaphore_wait(barrier, count)

    def hop(source, target, number, device):
        return pltpu.make_async_remote_copy(
            src_ref=source, dst_ref=target, send_sem=send_sem.at[number], recv_sem=recv_sem.at[number],
            device_id=device, device_id_type=MESH,
        )

    half = tile // 2
    to_up = hop(current.at[pl.ds(0, half)], below, 0, {"tx": tx - 1})
    to_down = hop(current.at[pl.ds(half, half)], above, 1, {"tx": tx + 1})
    to_left = hop(packed.at[:, pl.ds(0, half)], right, 2, {"ty": ty - 1})
    to_right = hop(packed.at[:, pl.ds(half, half)], left, 3, {"ty": ty + 1})
    swap_weights = hop(my_weights, other_weights, 4, {"ka": 1 - ka})
    swap_spectra = hop(spectra, other_spectra, 5, {"ka": 1 - ka})
    pl.when(has_up)(to_up.start)
    pl.when(has_down)(to_down.start)
    swap_spectra.start()
    swap_weights.start()

    part = exact(row_dft[:, HALO : HALO + tile], current[...])

    def arrived(there, copy, buffer):
        pl.when(there)(copy.wait_recv)

        @pl.when(jnp.logical_not(there))
        def _():
            buffer[...] = jnp.zeros_like(buffer)

    arrived(has_up, to_down, above)
    arrived(has_down, to_up, below)
    part = part + exact(row_dft[:, :HALO], above[...]) + exact(row_dft[:, HALO + tile :], below[...])
    packed[...] = part
    pl.when(has_left)(to_left.start)
    pl.when(has_right)(to_right.start)
    sums = exact(part, col_dft[HALO : HALO + tile, :])
    arrived(has_left, to_right, left)
    arrived(has_right, to_left, right)
    sums = sums + exact(left[...], col_dft[:HALO, :]) + exact(right[...], col_dft[HALO + tile :, :])
    full = exact(expand[...], sums)
    scale = 1.0 / (ext * ext)
    spec_re[...] = (full[:BAND, :BAND] - full[BAND:, BAND:]) * scale
    spec_im[...] = (full[BAND:, :BAND] + full[:BAND, BAND:]) * -scale

    pl.when(has_up)(to_up.wait_send)
    pl.when(has_down)(to_down.wait_send)
    pl.when(has_left)(to_left.wait_send)
    pl.when(has_right)(to_right.wait_send)
    swap_weights.wait()
    swap_spectra.wait()


def image_kernel(
    spec_re, spec_im, spectra, other_spectra, weights, other_weights, first, second, flip,
    site_rows, site_cols, tolerance,
    intensity, edge_errors, peaks, shares,
    plus, minus, image, image_in, errors, errors_in, near, far, near_send, near_recv, far_send, far_recv,
):
    tx, ty, ka = lax.axis_index("tx"), lax.axis_index("ty"), lax.axis_index("ka")
    n_tx, n_ty, n_ka = lax.axis_size("tx"), lax.axis_size("ty"), lax.axis_size("ka")
    n_near = n_ty * n_ka
    place = ty * n_ka + ka
    barrier = pltpu.get_barrier_semaphore()

    def near_peer(d):
        spot = lax.rem(place + d, n_near)
        return spot, {"ty": spot // n_ka, "ka": lax.rem(spot, n_ka)}

    def far_peer(d):
        spot = lax.rem(tx + d, n_tx)
        return spot, {"tx": spot}

    for d in range(1, n_near):
        pl.semaphore_signal(barrier, inc=1, device_id=near_peer(d)[1], device_id_type=MESH)
    for d in range(1, n_tx):
        pl.semaphore_signal(barrier, inc=1, device_id=far_peer(d)[1], device_id_type=MESH)

    half = BAND
    re, im = spec_re[...], spec_im[...]
    plus[...] = jnp.zeros_like(plus)
    minus[...] = jnp.zeros_like(minus)

    def outer(y):
        hi, mid, lo = bf16_pieces(y, 3)
        upper, lower = jnp.concatenate([hi, mid], axis=0), jnp.concatenate([hi, lo], axis=0)
        return dot(second[0], upper) + dot(second[1], upper) + dot(second[2], lower)

    def add(kernels, k, weight):
        k_re, k_im = kernels[k, 0], kernels[k, 1]
        product = jnp.concatenate([k_re * re - k_im * im, k_re * im + k_im * re], axis=0)
        hi, mid, lo = bf16_pieces(product, 3)
        upper, lower = jnp.concatenate([hi, mid], axis=1), jnp.concatenate([hi, lo], axis=1)
        inner = dot(upper, first[0]) + dot(upper, first[1]) + dot(lower, first[2])
        a, c, d, b = inner[:half, :half], inner[:half, half:], inner[half:, :half], inner[half:, half:]
        y_re = jnp.concatenate([a - b, a + b], axis=1)
        y_im = jnp.concatenate([c + d, d - c], axis=1)
        of_re, of_im = outer(y_re), outer(y_im)
        a, c, d, b = of_re[:half], of_re[half:], of_im[:half], of_im[half:]
        p_re, p_im, m_re, m_im = a - b, c + d, a + b, d - c
        plus[...] += weight * (p_re * p_re + p_im * p_im)
        minus[...] += weight * (m_re * m_re + m_im * m_im)

    @pl.loop(0, spectra.shape[0])
    def _(k):
        add(spectra, k, weights[k])
        add(other_spectra, k, other_weights[pl.ds(k, 1), :])

    both = jnp.concatenate([exact(flip[...], minus[...]), plus[...]], axis=0)
    picture = jnp.concatenate([exact(both[:, half:], flip[...]), both[:, :half]], axis=1)
    image[...] = picture
    tile = picture.shape[0]
    grad_rows = (pltpu.roll(picture, tile - 1, 0) - pltpu.roll(picture, 1, 0)) * 0.5
    grad_cols = (pltpu.roll(picture, tile - 1, 1) - pltpu.roll(picture, 1, 1)) * 0.5
    slope = jnp.sqrt(grad_rows * grad_rows + grad_cols * grad_cols)
    field = (picture - LEVEL) / jnp.maximum(slope, SLOPE_FLOOR)
    field_hi, field_lo = bf16_pieces(field, 2)

    pl.semaphore_wait(barrier, n_near - 1 + n_tx - 1)

    def to_other(source, target, number):
        return pltpu.make_async_remote_copy(
            src_ref=source, dst_ref=target, send_sem=near_send.at[n_near + number],
            recv_sem=near_recv.at[n_near + number], device_id={"ka": 1 - ka}, device_id_type=MESH,
        )

    send_image = to_other(image, image_in, 0)
    send_errors = to_other(errors, errors_in, 1)
    send_image.start()

    width = tile
    place_at = lax.broadcasted_iota(jnp.int32, (tile, width), 0)
    for chunk in range(site_rows.shape[2] // width):
        at = slice(chunk * width, (chunk + 1) * width)
        wanted = jnp.where(place_at == site_cols[0, :, at], 1.0, 0.0).astype(jnp.bfloat16)
        sampled = dot(field_hi, wanted) + dot(field_lo, wanted)
        sampled = jnp.where(place_at == site_rows[0, :, at], sampled, 0.0)
        errors[:, at] = jnp.sum(sampled, axis=0, keepdims=True)

    found = errors[...]
    size = jnp.abs(found)
    limit = tolerance[ka].astype(jnp.float32) / 8.0
    peak = jnp.max(size, axis=1, keepdims=True)
    total = jnp.sum(1.0 / (1.0 + jnp.exp(SHARPNESS * (size - limit))), axis=1, keepdims=True)
    lane = lax.broadcasted_iota(jnp.int32, (1, 128), 1)
    is_peak = lane < 64
    near[place] = jnp.where(is_peak, peak, total)

    def small(buffer, mine, d, peer, send, recv):
        return pltpu.make_async_remote_copy(
            src_ref=buffer.at[mine], dst_ref=buffer.at[mine], send_sem=send.at[d], recv_sem=recv.at[mine],
            device_id=peer, device_id_type=MESH,
        )

    def swapped(buffer, mine, peers, send, recv):
        copies = [small(buffer, mine, d, peer, send, recv) for d, (_, peer) in peers]
        for copy in copies:
            copy.start()
        for d, (spot, peer) in peers:
            small(buffer, spot, d, peer, send, recv).wait_recv()
        return copies

    near_peers = [(d, near_peer(d)) for d in range(1, n_near)]
    far_peers = [(d, far_peer(d)) for d in range(1, n_tx)]
    copies = swapped(near, place, near_peers, near_send, near_recv)
    send_errors.start()
    of_iteration = []
    for t in range(n_ka):
        found_t = [near[y * n_ka + t] for y in range(n_ty)]
        of_iteration.append(
            jnp.where(is_peak, functools.reduce(jnp.maximum, found_t), functools.reduce(jnp.add, found_t))
        )
    far[tx] = jnp.where((lane & 32) == 0, of_iteration[0], of_iteration[1])
    copies += swapped(far, tx, far_peers, far_send, far_recv)
    final = jnp.where(is_peak, jnp.max(far[...], axis=0), jnp.sum(far[...], axis=0))
    share = 1.0 / float(site_rows.shape[2] * n_tx * n_ty)
    for t in range(ITERS):
        peaks[t] = final[0, 32 * t]
        shares[t] = final[0, 64 + 32 * t] * share

    send_image.wait()
    send_errors.wait()
    intensity[...] = jnp.where(ka == ITERS - 1, image[...], image_in[...])
    edge_errors[0, 0, 0:1, :] = jnp.where(ka == 0, errors[...], errors_in[...])
    edge_errors[0, 0, 1:2, :] = jnp.where(ka == 0, errors_in[...], errors[...])
    for copy in copies:
        copy.wait_send()


def shards(
    mask_raster, frag_rows, frag_cols, frag_length, frag_orient, frag_moves,
    site_rows, site_cols, spectra, weights, tolerance,
):
    f32 = jnp.float32
    tile = mask_raster.shape[0]
    half = tile // 2
    sites = site_rows.shape[2]
    kernels = spectra.shape[0]
    n_near = lax.axis_size("ty") * lax.axis_size("ka")
    n_tx = lax.axis_size("tx")
    row_dft, col_dft, expand, first, second, flip = (jnp.asarray(t) for t in tables(tile))
    vmem = pl.BlockSpec(memory_space=pltpu.VMEM)
    smem = pl.BlockSpec(memory_space=pltpu.SMEM)
    anywhere = pl.BlockSpec(memory_space=pl.ANY)
    dma = pltpu.SemaphoreType.DMA
    new_mask, spec_re, spec_im, other_spectra, other_weights = pl.pallas_call(
        halo_kernel,
        name="halo_kernel",
        out_shape=(
            jax.ShapeDtypeStruct((tile, tile), f32),
            jax.ShapeDtypeStruct((BAND, BAND), f32),
            jax.ShapeDtypeStruct((BAND, BAND), f32),
            jax.ShapeDtypeStruct(spectra.shape, f32),
            jax.ShapeDtypeStruct((kernels, tile), f32),
        ),
        in_specs=[vmem] * 6 + [anywhere, smem] + [vmem] * 3,
        out_specs=(vmem, vmem, vmem, anywhere, anywhere),
        scratch_shapes=[
            pltpu.VMEM((tile, tile), f32),
            pltpu.VMEM((HALO, tile), f32),
            pltpu.VMEM((HALO, tile), f32),
            pltpu.VMEM((PACKED, tile), f32),
            pltpu.VMEM((PACKED, HALO), f32),
            pltpu.VMEM((PACKED, HALO), f32),
            pltpu.VMEM((kernels, tile), f32),
            dma((6,)),
            dma((6,)),
        ],
        compiler_params=pltpu.CompilerParams(
            collective_id=0, has_side_effects=True, vmem_limit_bytes=16 * 2**20
        ),
        cost_estimate=pl.CostEstimate(flops=2 * 10**9, bytes_accessed=4 * 10**6, transcendentals=0),
    )(
        mask_raster, frag_rows, frag_cols, frag_length, frag_orient, frag_moves, spectra, weights,
        row_dft, col_dft, expand,
    )
    intensity, edge_errors, peaks, shares = pl.pallas_call(
        image_kernel,
        name="image_kernel",
        out_shape=(
            jax.ShapeDtypeStruct((tile, tile), f32),
            jax.ShapeDtypeStruct((1, 1, ITERS, sites), f32),
            jax.ShapeDtypeStruct((ITERS,), f32),
            jax.ShapeDtypeStruct((ITERS,), f32),
        ),
        in_specs=[vmem] * 4 + [smem] + [vmem] * 6 + [smem],
        out_specs=(vmem, vmem, smem, smem),
        scratch_shapes=[
            pltpu.VMEM((half, tile), f32),
            pltpu.VMEM((half, tile), f32),
            pltpu.VMEM((tile, tile), f32),
            pltpu.VMEM((tile, tile), f32),
            pltpu.VMEM((1, sites), f32),
            pltpu.VMEM((1, sites), f32),
            pltpu.VMEM((n_near, 1, 128), f32),
            pltpu.VMEM((n_tx, 1, 128), f32),
            dma((n_near + 2,)),
            dma((n_near + 2,)),
            dma((n_tx,)),
            dma((n_tx,)),
        ],
        compiler_params=pltpu.CompilerParams(
            collective_id=1, has_side_effects=True, vmem_limit_bytes=24 * 2**20
        ),
        cost_estimate=pl.CostEstimate(flops=4 * 10**9, bytes_accessed=4 * 10**6, transcendentals=0),
    )(
        spec_re, spec_im, spectra, other_spectra, weights, other_weights, first, second, flip,
        site_rows, site_cols, tolerance,
    )
    return intensity, new_mask, edge_errors, peaks, shares


def solution(mesh):
    placed = (
        P(("groups", "tx"), "ty"),
        P(("groups", "tx"), "ty", None),
        P(("groups", "tx"), "ty", None),
        P(("groups", "tx"), "ty", None),
        P(("groups", "tx"), "ty", None),
        P(("groups", "tx"), "ty", None, None),
        P(("groups", "tx"), "ty", None),
        P(("groups", "tx"), "ty", None),
        P("ka", None, None, None),
        P("ka"),
        P(),
    )
    return jax.shard_map(
        shards,
        mesh=mesh,
        in_specs=placed,
        out_specs=(
            P(("groups", "tx"), "ty"),
            P(("groups", "tx"), "ty"),
            P(("groups", "tx"), "ty", None, None),
            P("groups"),
            P("groups"),
        ),
        check_vma=False,
    )
```

```python
import functools
import math

import jax
import jax.numpy as jnp
import numpy as np
from jax import lax
from jax.experimental import pallas as pl
from jax.experimental.pallas import tpu as pltpu
from jax.sharding import PartitionSpec as P

HALO = 128
BAND = 128
ITERS = 2
LEVEL = 0.4
SLOPE_FLOOR = 0.05
SHARPNESS = 8.0
HIGHEST = lax.Precision.HIGHEST
MESH = pl.DeviceIdType.MESH
SIN_AT = 72
PACKED = 136


def bf16_pieces(x, count):
    pieces = []
    for _ in range(count):
        pieces.append(x.astype(jnp.bfloat16))
        x = x - pieces[-1].astype(jnp.float32)
    return pieces


def host_pieces(x):
    pieces = []
    for _ in range(3):
        pieces.append(x.astype(jnp.bfloat16))
        x = x - pieces[-1].astype(np.float64)
    return pieces


def tables(tile):
    ext = tile + 2 * HALO
    half = tile // 2
    theta = 2.0 * math.pi / ext
    inside = np.arange(ext) - (ext - 1) / 2
    low = BAND // 2
    rows = np.zeros((PACKED, ext))
    rows[: low + 1] = np.cos(theta * np.outer(np.arange(low + 1), inside))
    rows[SIN_AT : SIN_AT + low] = np.sin(theta * np.outer(np.arange(1, low + 1), inside))
    freq = np.arange(BAND) - low
    turns = theta * np.outer(inside, freq)
    cols = np.concatenate([np.cos(turns), np.sin(turns)], axis=1)
    expand = np.zeros((2 * BAND, PACKED))
    for u, f in enumerate(freq):
        expand[u, abs(f)] = 1.0
        if f != 0:
            expand[BAND + u, SIN_AT + abs(f) - 1] = np.sign(f)
    out = theta * np.outer(freq, np.arange(half) + 0.5)
    basis = np.concatenate([np.cos(out), np.sin(out)], axis=1)
    hi, mid, lo = host_pieces(basis)
    first = np.stack([np.concatenate(b, axis=0) for b in ((hi, hi), (mid, mid), (lo, hi))])
    second = np.ascontiguousarray(first.swapaxes(1, 2))
    flip = np.eye(half)[::-1]
    f32 = np.float32
    return rows.astype(f32), cols.astype(f32), expand.astype(f32), first, second, flip.astype(f32)


def exact(left, right):
    return jnp.dot(left, right, precision=HIGHEST, preferred_element_type=jnp.float32)


def dot(left, right):
    return jnp.dot(left, right, preferred_element_type=jnp.float32)


def opc_kernel(
    mask, rows_at, cols_at, lengths, orients, moves, site_rows, site_cols, spectra, weights, tolerance,
    row_dft_in, col_dft_in, expand_in, first_in, second_in, flip_in,
    new_mask, intensity, edge_errors, stats,
    current, fragments, frag_moves, sites, kernels, my_weights, other_weights, weight_of, limits,
    row_dft, col_dft, expand, first, second, flip,
    above, below, packed, left, right, spec_re, spec_im, wanted,
    plus, minus, image, image_in, errors, errors_in, near, far, mask_out, image_out, errors_out, stats_out,
    load_sem, save_sem, halo_send, halo_recv, near_send, near_recv, far_send, far_recv, ready,
):
    tx, ty, ka = lax.axis_index("tx"), lax.axis_index("ty"), lax.axis_index("ka")
    n_tx, n_ty, n_ka = lax.axis_size("tx"), lax.axis_size("ty"), lax.axis_size("ka")
    n_near = n_ty * n_ka
    place = ty * n_ka + ka
    tile = mask.shape[0]
    ext = tile + 2 * HALO
    half = tile // 2
    has_up, has_down = tx > 0, tx < n_tx - 1
    has_left, has_right = ty > 0, ty < n_ty - 1

    pairs = [
        (mask, current), (rows_at, fragments.at[0]), (cols_at, fragments.at[1]), (lengths, fragments.at[2]),
        (orients, fragments.at[3]), (moves, frag_moves), (weights, weight_of), (row_dft_in, row_dft),
        (site_cols, sites.at[0]), (col_dft_in, col_dft), (expand_in, expand), (spectra, kernels.at[0]),
        (first_in, first), (second_in, second), (flip_in, flip), (site_rows, sites.at[1]), (tolerance, limits),
    ]
    loads = [pltpu.make_async_copy(src, dst, load_sem.at[i]) for i, (src, dst) in enumerate(pairs)]
    for load in loads:
        load.start()

    def near_peer(d):
        spot = lax.rem(place + d, n_near)
        return spot, {"ty": spot // n_ka, "ka": lax.rem(spot, n_ka)}

    def far_peer(d):
        spot = lax.rem(tx + d, n_tx)
        return spot, {"tx": spot}

    barrier = pltpu.get_barrier_semaphore()
    for d in range(1, n_near):
        pl.semaphore_signal(barrier, inc=1, device_id=near_peer(d)[1], device_id_type=MESH)

    @pl.when(has_up)
    def _():
        pl.semaphore_signal(barrier, inc=1, device_id={"tx": tx - 1}, device_id_type=MESH)

    for d in range(1, n_tx):
        @pl.when(tx + d < n_tx)
        def _():
            pl.semaphore_signal(barrier, inc=1, device_id={"tx": tx + d}, device_id_type=MESH)

    for load in loads[:7]:
        load.wait()
    position = lax.broadcasted_iota(jnp.int32, (tile, rows_at.shape[2]), 0)
    row, col, length = fragments[0, 0], fragments[1, 0], fragments[2, 0]
    along = fragments[3, 0] == 0
    steps = [current[...]]
    for t in range(ITERS):
        move = frag_moves[0, 0, t : t + 1, :]
        lower, upper = jnp.minimum(move, 0), jnp.maximum(move, 0)
        row_low = jnp.where(along, row, row + lower)
        row_high = jnp.where(along, row + length, row + upper)
        col_low = jnp.where(along, col + lower, col)
        col_high = jnp.where(along, col + upper, col + length)
        sign = jnp.where(move > 0, 1.0, 0.0) - jnp.where(move < 0, 1.0, 0.0)
        in_rows = jnp.where((position >= row_low) & (position < row_high), sign, 0.0)
        in_cols = jnp.where((position >= col_low) & (position < col_high), 1.0, 0.0)
        strips = lax.dot_general(
            in_rows.astype(jnp.bfloat16), in_cols.astype(jnp.bfloat16), (((1,), (1,)), ((), ())),
            preferred_element_type=jnp.float32,
        )
        steps.append(jnp.clip(steps[-1] + strips, 0.0, 1.0))
    mask_out[...] = steps[2]
    current[...] = jnp.where(ka == 0, steps[1], steps[2])
    for k in range(my_weights.shape[0]):
        my_weights[pl.ds(k, 1), :] = jnp.full((1, my_weights.shape[1]), weight_of[k], jnp.float32)

    pl.semaphore_wait(barrier, n_near - 1 + tx + has_down.astype(jnp.int32))

    def hop(source, target, number, device):
        return pltpu.make_async_remote_copy(
            src_ref=source, dst_ref=target, send_sem=halo_send.at[number], recv_sem=halo_recv.at[number],
            device_id=device, device_id_type=MESH,
        )

    to_up = hop(current.at[pl.ds(0, half)], below, 0, {"tx": tx - 1})
    to_down = hop(current.at[pl.ds(half, half)], above, 1, {"tx": tx + 1})
    to_left = hop(packed.at[:, pl.ds(0, half)], right, 2, {"ty": ty - 1})
    to_right = hop(packed.at[:, pl.ds(half, half)], left, 3, {"ty": ty + 1})
    swap_weights = hop(my_weights, other_weights, 4, {"ka": 1 - ka})
    swap_spectra = hop(spectra, kernels.at[1], 5, {"ka": 1 - ka})
    pl.when(has_up)(to_up.start)
    pl.when(has_down)(to_down.start)
    swap_spectra.start()
    swap_weights.start()
    pairs = ((mask_out, new_mask), (image_out, intensity), (errors_out, edge_errors), (stats_out, stats))
    saves = [pltpu.make_async_copy(src, dst, save_sem.at[i]) for i, (src, dst) in enumerate(pairs)]
    saves[0].start()
    for d in range(1, n_tx):
        @pl.when(tx - d >= 0)
        def _():
            pl.semaphore_signal(ready, inc=1, device_id={"tx": tx - d}, device_id_type=MESH)

    def arrived(there, copy, buffer):
        pl.when(there)(copy.wait_recv)

        @pl.when(jnp.logical_not(there))
        def _():
            buffer[...] = jnp.zeros_like(buffer)

    loads[7].wait()
    part = exact(row_dft[:, HALO : HALO + tile], current[...])
    loads[8].wait()
    place_at = lax.broadcasted_iota(jnp.int32, (tile, tile), 0)
    chunks = site_rows.shape[2] // tile
    for chunk in range(chunks):
        at = slice(chunk * tile, (chunk + 1) * tile)
        wanted[:, at] = jnp.where(place_at == sites[0, 0, :, at], 1.0, 0.0).astype(jnp.bfloat16)
    for load in loads[9:]:
        load.wait()
    arrived(has_up, to_down, above)
    arrived(has_down, to_up, below)
    part = part + exact(row_dft[:, :HALO], above[...]) + exact(row_dft[:, HALO + tile :], below[...])
    packed[...] = part
    pl.when(has_left)(to_left.start)
    pl.when(has_right)(to_right.start)
    sums = exact(part, col_dft[HALO : HALO + tile, :])
    plus[...] = jnp.zeros_like(plus)
    minus[...] = jnp.zeros_like(minus)
    swap_weights.wait()
    swap_spectra.wait()
    arrived(has_left, to_right, left)
    arrived(has_right, to_left, right)
    sums = sums + exact(left[...], col_dft[:HALO, :]) + exact(right[...], col_dft[HALO + tile :, :])
    full = exact(expand[...], sums)
    scale = 1.0 / (ext * ext)
    spec_re[...] = (full[:BAND, :BAND] - full[BAND:, BAND:]) * scale
    spec_im[...] = (full[BAND:, :BAND] + full[:BAND, BAND:]) * -scale

    def outer(y):
        hi, mid, lo = bf16_pieces(y, 3)
        upper, lower = jnp.concatenate([hi, mid], axis=0), jnp.concatenate([hi, lo], axis=0)
        return dot(second[0], upper) + dot(second[1], upper) + dot(second[2], lower)

    def add(k_re, k_im, weight):
        re, im = spec_re[...], spec_im[...]
        product = jnp.concatenate([k_re * re - k_im * im, k_re * im + k_im * re], axis=0)
        hi, mid, lo = bf16_pieces(product, 3)
        upper, lower = jnp.concatenate([hi, mid], axis=1), jnp.concatenate([hi, lo], axis=1)
        inner = dot(upper, first[0]) + dot(upper, first[1]) + dot(lower, first[2])
        a, c, d, b = inner[:half, :half], inner[:half, half:], inner[half:, :half], inner[half:, half:]
        y_re = jnp.concatenate([a - b, a + b], axis=1)
        y_im = jnp.concatenate([c + d, d - c], axis=1)
        of_re, of_im = outer(y_re), outer(y_im)
        a, c, d, b = of_re[:half], of_re[half:], of_im[:half], of_im[half:]
        p_re, p_im, m_re, m_im = a - b, c + d, a + b, d - c
        plus[...] += weight * (p_re * p_re + p_im * p_im)
        minus[...] += weight * (m_re * m_re + m_im * m_im)

    @pl.loop(0, spectra.shape[0])
    def _(k):
        add(kernels[0, k, 0], kernels[0, k, 1], my_weights[pl.ds(k, 1), :])
        add(kernels[1, k, 0], kernels[1, k, 1], other_weights[pl.ds(k, 1), :])

    both = jnp.concatenate([exact(flip[...], minus[...]), plus[...]], axis=0)
    picture = jnp.concatenate([exact(both[:, half:], flip[...]), both[:, :half]], axis=1)
    image[...] = picture
    grad_rows = (pltpu.roll(picture, tile - 1, 0) - pltpu.roll(picture, 1, 0)) * 0.5
    grad_cols = (pltpu.roll(picture, tile - 1, 1) - pltpu.roll(picture, 1, 1)) * 0.5
    slope = jnp.sqrt(grad_rows * grad_rows + grad_cols * grad_cols)
    field = (picture - LEVEL) / jnp.maximum(slope, SLOPE_FLOOR)
    field_hi, field_lo = bf16_pieces(field, 2)

    def to_other(source, target, number):
        return pltpu.make_async_remote_copy(
            src_ref=source, dst_ref=target, send_sem=near_send.at[n_near + number],
            recv_sem=near_recv.at[n_near + number], device_id={"ka": 1 - ka}, device_id_type=MESH,
        )

    send_image = to_other(image, image_in, 0)
    send_errors = to_other(errors, errors_in, 1)
    send_image.start()

    for chunk in range(chunks):
        at = slice(chunk * tile, (chunk + 1) * tile)
        sampled = dot(field_hi, wanted[:, at]) + dot(field_lo, wanted[:, at])
        sampled = jnp.where(place_at == sites[1, 0, :, at], sampled, 0.0)
        errors[:, at] = jnp.sum(sampled, axis=0, keepdims=True)

    found = errors[...]
    size = jnp.abs(found)
    limit = limits[ka].astype(jnp.float32) / 8.0
    peak = jnp.max(size, axis=1, keepdims=True)
    total = jnp.sum(1.0 / (1.0 + jnp.exp(SHARPNESS * (size - limit))), axis=1, keepdims=True)
    lane = lax.broadcasted_iota(jnp.int32, (1, 128), 1)
    is_peak = lane < 64
    near[place] = jnp.where(is_peak, peak, total)

    def small(buffer, mine, d, peer, send, recv):
        return pltpu.make_async_remote_copy(
            src_ref=buffer.at[mine], dst_ref=buffer.at[mine], send_sem=send.at[d], recv_sem=recv.at[mine],
            device_id=peer, device_id_type=MESH,
        )

    def swapped(buffer, mine, peers, send, recv):
        copies = [small(buffer, mine, d, peer, send, recv) for d, (_, peer) in peers]
        for copy in copies:
            copy.start()
        for d, (spot, peer) in peers:
            small(buffer, spot, d, peer, send, recv).wait_recv()
        return copies

    near_peers = [(d, near_peer(d)) for d in range(1, n_near)]
    far_peers = [(d, far_peer(d)) for d in range(1, n_tx)]

    @pl.when(has_down)
    def _():
        pl.semaphore_wait(ready, n_tx - 1 - tx)

    copies = swapped(near, place, near_peers, near_send, near_recv)
    of_iteration = []
    for t in range(n_ka):
        found_t = [near[y * n_ka + t] for y in range(n_ty)]
        of_iteration.append(
            jnp.where(is_peak, functools.reduce(jnp.maximum, found_t), functools.reduce(jnp.add, found_t))
        )
    far[tx] = jnp.where((lane & 32) == 0, of_iteration[0], of_iteration[1])
    far_copies = [small(far, tx, d, peer, far_send, far_recv) for d, (_, peer) in far_peers]
    for copy in far_copies:
        copy.start()
    send_errors.start()
    send_image.wait()
    send_errors.wait()
    image_out[...] = jnp.where(ka == ITERS - 1, image[...], image_in[...])
    errors_out[0, 0, 0:1, :] = jnp.where(ka == 0, errors[...], errors_in[...])
    errors_out[0, 0, 1:2, :] = jnp.where(ka == 0, errors_in[...], errors[...])
    saves[1].start()
    saves[2].start()
    pl.when(has_up)(to_up.wait_send)
    pl.when(has_down)(to_down.wait_send)
    pl.when(has_left)(to_left.wait_send)
    pl.when(has_right)(to_right.wait_send)
    for copy in copies:
        copy.wait_send()
    for d, (spot, peer) in far_peers:
        small(far, spot, d, peer, far_send, far_recv).wait_recv()
    stats_out[...] = jnp.where(is_peak, jnp.max(far[...], axis=0), jnp.sum(far[...], axis=0))
    saves[3].start()
    for copy in far_copies:
        copy.wait_send()
    for save in saves:
        save.wait()


def deliver_kernel(
    n_sites, image, mask, errors, stats, intensity, new_mask, edge_errors, peaks, shares,
    image_at, mask_at, errors_at, stats_at, sem,
):
    held = ((stats, stats_at, None), (image, image_at, intensity), (mask, mask_at, new_mask), (errors, errors_at, edge_errors))
    loads = [pltpu.make_async_copy(src, at, sem.at[0, i]) for i, (src, at, _) in enumerate(held)]
    copies = [pltpu.make_async_copy(at, dst, sem.at[1, i]) for i, (_, at, dst) in enumerate(held) if i > 0]
    for load in loads:
        load.start()
    loads[0].wait()
    for load, copy in zip(loads[1:], copies):
        load.wait()
        copy.start()
    final = stats_at[...]
    for t in range(ITERS):
        peaks[t] = final[0, 32 * t]
        shares[t] = final[0, 64 + 32 * t] * (1.0 / n_sites)
    for copy in copies:
        copy.wait()


def shards(
    mask_raster, frag_rows, frag_cols, frag_length, frag_orient, frag_moves,
    site_rows, site_cols, spectra, weights, tolerance,
):
    f32, i32, bf16 = jnp.float32, jnp.int32, jnp.bfloat16
    tile = mask_raster.shape[0]
    half = tile // 2
    n_sites = site_rows.shape[2]
    kernels = spectra.shape[0]
    n_near = lax.axis_size("ty") * lax.axis_size("ka")
    n_tx = lax.axis_size("tx")
    constants = [jnp.asarray(t) for t in tables(tile)]
    smem = pl.BlockSpec(memory_space=pltpu.SMEM)
    hbm = pl.BlockSpec(memory_space=pltpu.HBM)
    dma = pltpu.SemaphoreType.DMA
    errors_shape = jax.ShapeDtypeStruct((1, 1, ITERS, n_sites), f32)
    square = jax.ShapeDtypeStruct((tile, tile), f32)
    V = pltpu.VMEM
    new_mask, image, errors, stats = pl.pallas_call(
        opc_kernel,
        name="opc_kernel",
        out_shape=(square, square, errors_shape, jax.ShapeDtypeStruct((1, 128), f32)),
        in_specs=[hbm] * 17,
        out_specs=(hbm,) * 4,
        scratch_shapes=[
            V((tile, tile), f32), V((4, *frag_rows.shape), i32), V(frag_moves.shape, i32),
            V((2, *site_rows.shape), i32), V((2, *spectra.shape), f32), V((kernels, tile), f32),
            V((kernels, tile), f32), pltpu.SMEM(weights.shape, f32), pltpu.SMEM(tolerance.shape, i32),
            *(V(c.shape, c.dtype) for c in constants),
            V((HALO, tile), f32), V((HALO, tile), f32), V((PACKED, tile), f32),
            V((PACKED, HALO), f32), V((PACKED, HALO), f32), V((BAND, BAND), f32), V((BAND, BAND), f32),
            V((tile, n_sites), bf16),
            V((half, tile), f32), V((half, tile), f32), V((tile, tile), f32), V((tile, tile), f32),
            V((1, n_sites), f32), V((1, n_sites), f32), V((n_near, 1, 128), f32), V((n_tx, 1, 128), f32),
            V((tile, tile), f32), V((tile, tile), f32), V(errors_shape.shape, f32), V((1, 128), f32),
            dma((17,)), dma((4,)), dma((6,)), dma((6,)), dma((n_near + 2,)), dma((n_near + 2,)), dma((n_tx,)), dma((n_tx,)),
            pltpu.SemaphoreType.REGULAR,
        ],
        compiler_params=pltpu.CompilerParams(collective_id=0, has_side_effects=True),
        cost_estimate=pl.CostEstimate(flops=4 * 10**9, bytes_accessed=4 * 10**6, transcendentals=0),
    )(
        mask_raster, frag_rows, frag_cols, frag_length, frag_orient, frag_moves, site_rows, site_cols,
        spectra, weights, tolerance, *constants,
    )
    pair = jax.ShapeDtypeStruct((ITERS,), f32)
    return pl.pallas_call(
        functools.partial(deliver_kernel, float(n_sites * n_tx * lax.axis_size("ty"))),
        name="deliver_kernel",
        out_shape=(square, square, errors_shape, pair, pair),
        in_specs=[hbm] * 4,
        out_specs=(hbm, hbm, hbm, smem, smem),
        scratch_shapes=[
            V((tile, tile), f32), V((tile, tile), f32), V(errors_shape.shape, f32), V((1, 128), f32), dma((2, 4)),
        ],
    )(image, new_mask, errors, stats)


def solution(mesh):
    placed = (
        P(("groups", "tx"), "ty"),
        P(("groups", "tx"), "ty", None),
        P(("groups", "tx"), "ty", None),
        P(("groups", "tx"), "ty", None),
        P(("groups", "tx"), "ty", None),
        P(("groups", "tx"), "ty", None, None),
        P(("groups", "tx"), "ty", None),
        P(("groups", "tx"), "ty", None),
        P("ka", None, None, None),
        P("ka"),
        P(),
    )
    return jax.shard_map(
        shards,
        mesh=mesh,
        in_specs=placed,
        out_specs=(
            P(("groups", "tx"), "ty"),
            P(("groups", "tx"), "ty"),
            P(("groups", "tx"), "ty", None, None),
            P("groups"),
            P("groups"),
        ),
        check_vma=False,
    )
```

```python
import functools
import math

import jax
import jax.numpy as jnp
import numpy as np
from jax import lax
from jax.experimental import pallas as pl
from jax.experimental.pallas import tpu as pltpu
from jax.sharding import PartitionSpec as P

HALO = 128
BAND = 128
ITERS = 2
LEVEL = 0.4
SLOPE_FLOOR = 0.05
SHARPNESS = 8.0
HIGHEST = lax.Precision.HIGHEST
MESH = pl.DeviceIdType.MESH
SIN_AT = 72
PACKED = 136


def bf16_pieces(x, count):
    pieces = []
    for _ in range(count):
        pieces.append(x.astype(jnp.bfloat16))
        x = x - pieces[-1].astype(jnp.float32)
    return pieces


def host_pieces(x):
    pieces = []
    for _ in range(3):
        pieces.append(x.astype(jnp.bfloat16))
        x = x - pieces[-1].astype(np.float64)
    return pieces


def tables(tile):
    ext = tile + 2 * HALO
    half = tile // 2
    theta = 2.0 * math.pi / ext
    inside = np.arange(ext) - (ext - 1) / 2
    low = BAND // 2
    rows = np.zeros((PACKED, ext))
    rows[: low + 1] = np.cos(theta * np.outer(np.arange(low + 1), inside))
    rows[SIN_AT : SIN_AT + low] = np.sin(theta * np.outer(np.arange(1, low + 1), inside))
    freq = np.arange(BAND) - low
    turns = theta * np.outer(inside, freq)
    cols = np.concatenate([np.cos(turns), np.sin(turns)], axis=1)
    expand = np.zeros((2 * BAND, PACKED))
    for u, f in enumerate(freq):
        expand[u, abs(f)] = 1.0
        if f != 0:
            expand[BAND + u, SIN_AT + abs(f) - 1] = np.sign(f)
    out = theta * np.outer(freq, np.arange(half) + 0.5)
    basis = np.concatenate([np.cos(out), np.sin(out)], axis=1)
    hi, mid, lo = host_pieces(basis)
    first = np.stack([np.concatenate(b, axis=0) for b in ((hi, hi), (mid, mid), (lo, hi))])
    second = np.ascontiguousarray(first.swapaxes(1, 2))
    flip = np.eye(half)[::-1]
    f32 = np.float32
    return rows.astype(f32), cols.astype(f32), expand.astype(f32), first, second, flip.astype(f32)


def exact(left, right):
    return jnp.dot(left, right, precision=HIGHEST, preferred_element_type=jnp.float32)


def dot(left, right):
    return jnp.dot(left, right, preferred_element_type=jnp.float32)


def opc_kernel(
    mask, rows_at, cols_at, lengths, orients, moves, site_rows, site_cols, spectra, weights, tolerance,
    row_dft_in, col_dft_in, expand_in, first_in, second_in, flip_in,
    new_mask, intensity, edge_errors, stats,
    current, fragments, frag_moves, sites, kernels, my_weights, other_weights, weight_of, limits,
    row_dft, col_dft, expand, first, second, flip,
    above, below, packed, left, right, spec_re, spec_im, wanted,
    plus, minus, image, image_in, errors, errors_in, near, far, mask_out, image_out, errors_out, stats_out,
    slot_a, slot_b, slot_c, slot_d, slot_e, slot_f, slot_g, slot_h, load_sem, save_sem, halo_send, halo_recv, near_send, near_recv, far_send, far_recv, token, ready,
):
    tx, ty, ka = lax.axis_index("tx"), lax.axis_index("ty"), lax.axis_index("ka")
    n_tx, n_ty, n_ka = lax.axis_size("tx"), lax.axis_size("ty"), lax.axis_size("ka")
    n_near = n_ty * n_ka
    place = ty * n_ka + ka
    tile = mask.shape[0]
    ext = tile + 2 * HALO
    half = tile // 2
    slots = ((slot_a, slot_b), (slot_c, slot_d), (slot_e, slot_f), (slot_g, slot_h))
    has_up, has_down = tx > 0, tx < n_tx - 1
    has_left, has_right = ty > 0, ty < n_ty - 1

    pairs = [
        (mask, current), (rows_at, fragments.at[0]), (cols_at, fragments.at[1]), (lengths, fragments.at[2]),
        (orients, fragments.at[3]), (moves, frag_moves), (weights, weight_of), (row_dft_in, row_dft),
        (site_cols, sites.at[0]), (col_dft_in, col_dft), (expand_in, expand), (spectra, kernels.at[0]),
        (first_in, first), (second_in, second), (flip_in, flip), (site_rows, sites.at[1]), (tolerance, limits),
    ]
    loads = [pltpu.make_async_copy(src, dst, load_sem.at[i]) for i, (src, dst) in enumerate(pairs)]
    for load in loads:
        load.start()

    def near_peer(d):
        spot = lax.rem(place + d, n_near)
        return spot, {"ty": spot // n_ka, "ka": lax.rem(spot, n_ka)}

    def far_peer(d):
        spot = lax.rem(tx + d, n_tx)
        return spot, {"tx": spot}

    barrier = pltpu.get_barrier_semaphore()
    for d in range(1, n_near):
        pl.semaphore_signal(barrier, inc=1, device_id=near_peer(d)[1], device_id_type=MESH)

    @pl.when(has_up)
    def _():
        pl.semaphore_signal(barrier, inc=1, device_id={"tx": tx - 1}, device_id_type=MESH)

    @pl.when(has_down)
    def _():
        pl.semaphore_signal(barrier, inc=1, device_id={"tx": tx + 1}, device_id_type=MESH)

    for load in loads[:7]:
        load.wait()
    position = lax.broadcasted_iota(jnp.int32, (tile, rows_at.shape[2]), 0)
    row, col, length = fragments[0, 0], fragments[1, 0], fragments[2, 0]
    along = fragments[3, 0] == 0
    steps = [current[...]]
    for t in range(ITERS):
        move = frag_moves[0, 0, t : t + 1, :]
        lower, upper = jnp.minimum(move, 0), jnp.maximum(move, 0)
        row_low = jnp.where(along, row, row + lower)
        row_high = jnp.where(along, row + length, row + upper)
        col_low = jnp.where(along, col + lower, col)
        col_high = jnp.where(along, col + upper, col + length)
        sign = jnp.where(move > 0, 1.0, 0.0) - jnp.where(move < 0, 1.0, 0.0)
        in_rows = jnp.where((position >= row_low) & (position < row_high), sign, 0.0)
        in_cols = jnp.where((position >= col_low) & (position < col_high), 1.0, 0.0)
        strips = lax.dot_general(
            in_rows.astype(jnp.bfloat16), in_cols.astype(jnp.bfloat16), (((1,), (1,)), ((), ())),
            preferred_element_type=jnp.float32,
        )
        steps.append(jnp.clip(steps[-1] + strips, 0.0, 1.0))
    mask_out[...] = steps[2]
    current[...] = jnp.where(ka == 0, steps[1], steps[2])
    for k in range(my_weights.shape[0]):
        my_weights[pl.ds(k, 1), :] = jnp.full((1, my_weights.shape[1]), weight_of[k], jnp.float32)

    pl.semaphore_wait(barrier, n_near - 1 + has_up.astype(jnp.int32) + has_down.astype(jnp.int32))

    def hop(source, target, number, device):
        return pltpu.make_async_remote_copy(
            src_ref=source, dst_ref=target, send_sem=halo_send.at[number], recv_sem=halo_recv.at[number],
            device_id=device, device_id_type=MESH,
        )

    to_up = hop(current.at[pl.ds(0, half)], below, 0, {"tx": tx - 1})
    to_down = hop(current.at[pl.ds(half, half)], above, 1, {"tx": tx + 1})
    to_left = hop(packed.at[:, pl.ds(0, half)], right, 2, {"ty": ty - 1})
    to_right = hop(packed.at[:, pl.ds(half, half)], left, 3, {"ty": ty + 1})
    swap_weights = hop(my_weights, other_weights, 4, {"ka": 1 - ka})
    swap_spectra = hop(spectra, kernels.at[1], 5, {"ka": 1 - ka})
    pl.when(has_up)(to_up.start)
    pl.when(has_down)(to_down.start)
    swap_spectra.start()
    swap_weights.start()
    pairs = ((mask_out, new_mask), (image_out, intensity), (errors_out, edge_errors), (stats_out, stats))
    saves = [pltpu.make_async_copy(src, dst, save_sem.at[i]) for i, (src, dst) in enumerate(pairs)]
    saves[0].start()
    def arrived(there, copy, buffer):
        pl.when(there)(copy.wait_recv)

        @pl.when(jnp.logical_not(there))
        def _():
            buffer[...] = jnp.zeros_like(buffer)

    loads[7].wait()
    part = exact(row_dft[:, HALO : HALO + tile], current[...])
    loads[8].wait()
    place_at = lax.broadcasted_iota(jnp.int32, (tile, tile), 0)
    chunks = site_rows.shape[2] // tile
    for chunk in range(chunks):
        at = slice(chunk * tile, (chunk + 1) * tile)
        wanted[:, at] = jnp.where(place_at == sites[0, 0, :, at], 1.0, 0.0).astype(jnp.bfloat16)
    for load in loads[9:]:
        load.wait()
    arrived(has_up, to_down, above)
    arrived(has_down, to_up, below)
    part = part + exact(row_dft[:, :HALO], above[...]) + exact(row_dft[:, HALO + tile :], below[...])
    packed[...] = part
    pl.when(has_left)(to_left.start)
    pl.when(has_right)(to_right.start)
    sums = exact(part, col_dft[HALO : HALO + tile, :])
    plus[...] = jnp.zeros_like(plus)
    minus[...] = jnp.zeros_like(minus)
    swap_weights.wait()
    swap_spectra.wait()
    arrived(has_left, to_right, left)
    arrived(has_right, to_left, right)
    sums = sums + exact(left[...], col_dft[:HALO, :]) + exact(right[...], col_dft[HALO + tile :, :])
    full = exact(expand[...], sums)
    scale = 1.0 / (ext * ext)
    spec_re[...] = (full[:BAND, :BAND] - full[BAND:, BAND:]) * scale
    spec_im[...] = (full[BAND:, :BAND] + full[:BAND, BAND:]) * -scale

    def inward(at, pair, k):
        k_re, k_im = kernels[at, k, 0], kernels[at, k, 1]
        re, im = spec_re[...], spec_im[...]
        product = jnp.concatenate([k_re * re - k_im * im, k_re * im + k_im * re], axis=0)
        hi, mid, lo = bf16_pieces(product, 3)
        upper, lower = jnp.concatenate([hi, mid], axis=1), jnp.concatenate([hi, lo], axis=1)
        inner = dot(upper, first[0]) + dot(upper, first[1]) + dot(lower, first[2])
        a, c, d, b = inner[:half, :half], inner[:half, half:], inner[half:, :half], inner[half:, half:]
        for slot, y in zip(pair, ((a - b, a + b), (c + d, d - c))):
            for side, part in enumerate(y):
                at_side = slice(side * half, (side + 1) * half)
                hi, mid, lo = bf16_pieces(part, 3)
                slot[0, :half, at_side] = hi
                slot[0, half:, at_side] = mid
                slot[1, :half, at_side] = hi
                slot[1, half:, at_side] = lo

    def outward(pair, weight):
        of_re, of_im = (
            dot(second[0], slot[0]) + dot(second[1], slot[0]) + dot(second[2], slot[1]) for slot in pair
        )
        a, c, d, b = of_re[:half], of_re[half:], of_im[:half], of_im[half:]
        p_re, p_im, m_re, m_im = a - b, c + d, a + b, d - c
        plus[...] += weight * (p_re * p_re + p_im * p_im)
        minus[...] += weight * (m_re * m_re + m_im * m_im)

    last = spectra.shape[0] - 1
    inward(0, slots[0], 0)
    inward(1, slots[1], 0)

    @pl.loop(0, spectra.shape[0] // 2)
    def _(i):
        k = 2 * i
        following = jnp.minimum(k + 2, last)
        outward(slots[0], my_weights[pl.ds(k, 1), :])
        inward(0, slots[2], k + 1)
        outward(slots[1], other_weights[pl.ds(k, 1), :])
        inward(1, slots[3], k + 1)
        outward(slots[2], my_weights[pl.ds(k + 1, 1), :])
        inward(0, slots[0], following)
        outward(slots[3], other_weights[pl.ds(k + 1, 1), :])
        inward(1, slots[1], following)

    both = jnp.concatenate([exact(flip[...], minus[...]), plus[...]], axis=0)
    picture = jnp.concatenate([exact(both[:, half:], flip[...]), both[:, :half]], axis=1)
    image[...] = picture
    grad_rows = (pltpu.roll(picture, tile - 1, 0) - pltpu.roll(picture, 1, 0)) * 0.5
    grad_cols = (pltpu.roll(picture, tile - 1, 1) - pltpu.roll(picture, 1, 1)) * 0.5
    slope = jnp.sqrt(grad_rows * grad_rows + grad_cols * grad_cols)
    field = (picture - LEVEL) / jnp.maximum(slope, SLOPE_FLOOR)
    field_hi, field_lo = bf16_pieces(field, 2)

    def to_other(source, target, number):
        return pltpu.make_async_remote_copy(
            src_ref=source, dst_ref=target, send_sem=near_send.at[n_near + number],
            recv_sem=near_recv.at[n_near + number], device_id={"ka": 1 - ka}, device_id_type=MESH,
        )

    send_image = to_other(image, image_in, 0)
    send_errors = to_other(errors, errors_in, 1)
    send_image.start()

    for chunk in range(chunks):
        at = slice(chunk * tile, (chunk + 1) * tile)
        sampled = dot(field_hi, wanted[:, at]) + dot(field_lo, wanted[:, at])
        sampled = jnp.where(place_at == sites[1, 0, :, at], sampled, 0.0)
        errors[:, at] = jnp.sum(sampled, axis=0, keepdims=True)

    found = errors[...]
    size = jnp.abs(found)
    limit = limits[ka].astype(jnp.float32) / 8.0
    peak = jnp.max(size, axis=1, keepdims=True)
    total = jnp.sum(1.0 / (1.0 + jnp.exp(SHARPNESS * (size - limit))), axis=1, keepdims=True)
    lane = lax.broadcasted_iota(jnp.int32, (1, 128), 1)
    is_peak = lane < 64
    near[place] = jnp.where(is_peak, peak, total)

    def small(buffer, mine, d, peer, send, recv):
        return pltpu.make_async_remote_copy(
            src_ref=buffer.at[mine], dst_ref=buffer.at[mine], send_sem=send.at[d], recv_sem=recv.at[mine],
            device_id=peer, device_id_type=MESH,
        )

    def swapped(buffer, mine, peers, send, recv):
        copies = [small(buffer, mine, d, peer, send, recv) for d, (_, peer) in peers]
        for copy in copies:
            copy.start()
        for d, (spot, peer) in peers:
            small(buffer, spot, d, peer, send, recv).wait_recv()
        return copies

    near_peers = [(d, near_peer(d)) for d in range(1, n_near)]

    @pl.when(has_up)
    def _():
        pl.semaphore_wait(token, 1)

    @pl.when(has_down)
    def _():
        pl.semaphore_signal(token, inc=1, device_id={"tx": tx + 1}, device_id_type=MESH)

    copies = swapped(near, place, near_peers, near_send, near_recv)
    of_iteration = []
    for t in range(n_ka):
        found_t = [near[y * n_ka + t] for y in range(n_ty)]
        of_iteration.append(
            jnp.where(is_peak, functools.reduce(jnp.maximum, found_t), functools.reduce(jnp.add, found_t))
        )
    far[tx] = jnp.where((lane & 32) == 0, of_iteration[0], of_iteration[1])

    def far_copy(d, up):
        spot = tx - d if up else tx + d
        return small(far, tx, d - 1 if up else n_tx - 1 + d - 1, {"tx": spot}, far_send, far_recv)

    for d in range(1, n_tx):
        @pl.when(tx - d >= 0)
        def _():
            far_copy(d, True).start()

    for d in range(1, n_tx):
        @pl.when(tx - d >= 0)
        def _():
            pl.semaphore_signal(ready, inc=1, device_id={"tx": tx - d}, device_id_type=MESH)

    @pl.when(has_down)
    def _():
        pl.semaphore_wait(ready, n_tx - 1 - tx)

    for d in range(1, n_tx):
        @pl.when(tx + d < n_tx)
        def _():
            far_copy(d, False).start()

    send_errors.start()
    send_image.wait()
    send_errors.wait()
    image_out[...] = jnp.where(ka == ITERS - 1, image[...], image_in[...])
    errors_out[0, 0, 0:1, :] = jnp.where(ka == 0, errors[...], errors_in[...])
    errors_out[0, 0, 1:2, :] = jnp.where(ka == 0, errors_in[...], errors[...])
    saves[1].start()
    saves[2].start()
    pl.when(has_up)(to_up.wait_send)
    pl.when(has_down)(to_down.wait_send)
    pl.when(has_left)(to_left.wait_send)
    pl.when(has_right)(to_right.wait_send)
    for copy in copies:
        copy.wait_send()
    for d in range(1, n_tx):
        spot, peer = far_peer(d)
        small(far, spot, 0, peer, far_send, far_recv).wait_recv()
    stats_out[...] = jnp.where(is_peak, jnp.max(far[...], axis=0), jnp.sum(far[...], axis=0))
    saves[3].start()
    for d in range(1, n_tx):
        for up in (True, False):
            pl.when(tx - d >= 0 if up else tx + d < n_tx)(far_copy(d, up).wait_send)
    for save in saves:
        save.wait()


def deliver_kernel(
    n_sites, image, mask, errors, stats, intensity, new_mask, edge_errors, peaks, shares,
    image_at, mask_at, errors_at, stats_at, peaks_at, shares_at, sem,
):
    held = ((stats, stats_at, None), (image, image_at, intensity), (mask, mask_at, new_mask), (errors, errors_at, edge_errors))
    loads = [pltpu.make_async_copy(src, at, sem.at[0, i]) for i, (src, at, _) in enumerate(held)]
    copies = [pltpu.make_async_copy(at, dst, sem.at[1, i]) for i, (_, at, dst) in enumerate(held) if i > 0]
    for load in loads:
        load.start()
    loads[0].wait()
    final = stats_at[...]
    for t in range(ITERS):
        peaks_at[t] = final[0, 32 * t]
        shares_at[t] = final[0, 64 + 32 * t] * (1.0 / n_sites)
    pairs = ((peaks_at, peaks), (shares_at, shares))
    copies += [pltpu.make_async_copy(at, dst, sem.at[1, 4 * i]) for i, (at, dst) in enumerate(pairs)]
    for copy in copies[3:]:
        copy.start()
    for load, copy in zip(loads[1:], copies):
        load.wait()
        copy.start()
    for copy in copies:
        copy.wait()


def shards(
    mask_raster, frag_rows, frag_cols, frag_length, frag_orient, frag_moves,
    site_rows, site_cols, spectra, weights, tolerance,
):
    f32, i32, bf16 = jnp.float32, jnp.int32, jnp.bfloat16
    tile = mask_raster.shape[0]
    half = tile // 2
    n_sites = site_rows.shape[2]
    kernels = spectra.shape[0]
    n_near = lax.axis_size("ty") * lax.axis_size("ka")
    n_tx = lax.axis_size("tx")
    constants = [jnp.asarray(t) for t in tables(tile)]
    hbm = pl.BlockSpec(memory_space=pltpu.HBM)
    dma = pltpu.SemaphoreType.DMA
    errors_shape = jax.ShapeDtypeStruct((1, 1, ITERS, n_sites), f32)
    square = jax.ShapeDtypeStruct((tile, tile), f32)
    V = pltpu.VMEM
    new_mask, image, errors, stats = pl.pallas_call(
        opc_kernel,
        name="opc_kernel",
        out_shape=(square, square, errors_shape, jax.ShapeDtypeStruct((1, 128), f32)),
        in_specs=[hbm] * 17,
        out_specs=(hbm,) * 4,
        scratch_shapes=[
            V((tile, tile), f32), V((4, *frag_rows.shape), i32), V(frag_moves.shape, i32),
            V((2, *site_rows.shape), i32), V((2, *spectra.shape), f32), V((kernels, tile), f32),
            V((kernels, tile), f32), pltpu.SMEM(weights.shape, f32), pltpu.SMEM(tolerance.shape, i32),
            *(V(c.shape, c.dtype) for c in constants),
            V((HALO, tile), f32), V((HALO, tile), f32), V((PACKED, tile), f32),
            V((PACKED, HALO), f32), V((PACKED, HALO), f32), V((BAND, BAND), f32), V((BAND, BAND), f32),
            V((tile, n_sites), bf16),
            V((half, tile), f32), V((half, tile), f32), V((tile, tile), f32), V((tile, tile), f32),
            V((1, n_sites), f32), V((1, n_sites), f32), V((n_near, 1, 128), f32), V((n_tx, 1, 128), f32),
            V((tile, tile), f32), V((tile, tile), f32), V(errors_shape.shape, f32), V((1, 128), f32),
            *([V((2, tile, tile), bf16)] * 8), dma((17,)), dma((4,)), dma((6,)), dma((6,)), dma((n_near + 2,)), dma((n_near + 2,)), dma((2 * n_tx,)), dma((n_tx,)),
            pltpu.SemaphoreType.REGULAR, pltpu.SemaphoreType.REGULAR,
        ],
        compiler_params=pltpu.CompilerParams(collective_id=0, has_side_effects=True),
        cost_estimate=pl.CostEstimate(flops=4 * 10**9, bytes_accessed=4 * 10**6, transcendentals=0),
    )(
        mask_raster, frag_rows, frag_cols, frag_length, frag_orient, frag_moves, site_rows, site_cols,
        spectra, weights, tolerance, *constants,
    )
    pair = jax.ShapeDtypeStruct((ITERS,), f32)
    return pl.pallas_call(
        functools.partial(deliver_kernel, float(n_sites * n_tx * lax.axis_size("ty"))),
        name="deliver_kernel",
        out_shape=(square, square, errors_shape, pair, pair),
        in_specs=[hbm] * 4,
        out_specs=(hbm,) * 5,
        scratch_shapes=[
            V((tile, tile), f32), V((tile, tile), f32), V(errors_shape.shape, f32), V((1, 128), f32),
            pltpu.SMEM((ITERS,), f32), pltpu.SMEM((ITERS,), f32), dma((2, 5)),
        ],
    )(image, new_mask, errors, stats)


def solution(mesh):
    placed = (
        P(("groups", "tx"), "ty"),
        P(("groups", "tx"), "ty", None),
        P(("groups", "tx"), "ty", None),
        P(("groups", "tx"), "ty", None),
        P(("groups", "tx"), "ty", None),
        P(("groups", "tx"), "ty", None, None),
        P(("groups", "tx"), "ty", None),
        P(("groups", "tx"), "ty", None),
        P("ka", None, None, None),
        P("ka"),
        P(),
    )
    return jax.shard_map(
        shards,
        mesh=mesh,
        in_specs=placed,
        out_specs=(
            P(("groups", "tx"), "ty"),
            P(("groups", "tx"), "ty"),
            P(("groups", "tx"), "ty", None, None),
            P("groups"),
            P("groups"),
        ),
        check_vma=False,
    )
```

```python
import functools
import math

import jax
import jax.numpy as jnp
import numpy as np
from jax import lax
from jax.experimental import pallas as pl
from jax.experimental.pallas import tpu as pltpu
from jax.sharding import PartitionSpec as P

HALO = 128
BAND = 128
ITERS = 2
LEVEL = 0.4
SLOPE_FLOOR = 0.05
SHARPNESS = 8.0
HIGHEST = lax.Precision.HIGHEST
MESH = pl.DeviceIdType.MESH
SIN_AT = 72
PACKED = 136


def bf16_pieces(x, count):
    pieces = []
    for _ in range(count):
        pieces.append(x.astype(jnp.bfloat16))
        x = x - pieces[-1].astype(jnp.float32)
    return pieces


def host_pieces(x):
    pieces = []
    for _ in range(3):
        pieces.append(x.astype(jnp.bfloat16))
        x = x - pieces[-1].astype(np.float64)
    return pieces


def tables(tile):
    ext = tile + 2 * HALO
    half = tile // 2
    theta = 2.0 * math.pi / ext
    inside = np.arange(ext) - (ext - 1) / 2
    low = BAND // 2
    rows = np.zeros((PACKED, ext))
    rows[: low + 1] = np.cos(theta * np.outer(np.arange(low + 1), inside))
    rows[SIN_AT : SIN_AT + low] = np.sin(theta * np.outer(np.arange(1, low + 1), inside))
    freq = np.arange(BAND) - low
    turns = theta * np.outer(inside, freq)
    cols = np.concatenate([np.cos(turns), np.sin(turns)], axis=1)
    expand = np.zeros((2 * BAND, PACKED))
    for u, f in enumerate(freq):
        expand[u, abs(f)] = 1.0
        if f != 0:
            expand[BAND + u, SIN_AT + abs(f) - 1] = np.sign(f)
    out = theta * np.outer(freq, np.arange(half) + 0.5)
    basis = np.concatenate([np.cos(out), np.sin(out)], axis=1)
    hi, mid, lo = host_pieces(basis)
    first = np.stack([np.concatenate(b, axis=0) for b in ((hi, hi), (mid, mid), (lo, hi))])
    second = np.ascontiguousarray(first.swapaxes(1, 2))
    flip = np.eye(half)[::-1]
    f32 = np.float32
    return rows.astype(f32), cols.astype(f32), expand.astype(f32), first, second, flip.astype(f32)


def exact(left, right):
    return jnp.dot(left, right, precision=HIGHEST, preferred_element_type=jnp.float32)


def dot(left, right):
    return jnp.dot(left, right, preferred_element_type=jnp.float32)


def opc_kernel(
    mask, rows_at, cols_at, lengths, orients, moves, site_rows, site_cols, spectra, weights, tolerance,
    row_dft_in, col_dft_in, expand_in, first_in, second_in, flip_in,
    new_mask, intensity, edge_errors, stats,
    current, fragments, frag_moves, sites, kernels, my_weights, other_weights, weight_of, limits,
    row_dft, col_dft, expand, first, second, flip,
    above, below, packed, left, right, spec_re, spec_im, wanted,
    plus, minus, image, image_in, errors, errors_in, near, far, mask_out, image_out, errors_out, stats_out,
    slot_a, slot_b, slot_c, slot_d, slot_e, slot_f, slot_g, slot_h, load_sem, save_sem, halo_send, halo_recv, near_send, near_recv, far_send, far_recv, ready,
):
    tx, ty, ka = lax.axis_index("tx"), lax.axis_index("ty"), lax.axis_index("ka")
    n_tx, n_ty, n_ka = lax.axis_size("tx"), lax.axis_size("ty"), lax.axis_size("ka")
    n_near = n_ty * n_ka
    place = ty * n_ka + ka
    tile = mask.shape[0]
    ext = tile + 2 * HALO
    half = tile // 2
    slots = ((slot_a, slot_b), (slot_c, slot_d), (slot_e, slot_f), (slot_g, slot_h))
    has_up, has_down = tx > 0, tx < n_tx - 1
    has_left, has_right = ty > 0, ty < n_ty - 1

    pairs = [
        (mask, current), (rows_at, fragments.at[0]), (cols_at, fragments.at[1]), (lengths, fragments.at[2]),
        (orients, fragments.at[3]), (moves, frag_moves), (weights, weight_of), (row_dft_in, row_dft),
        (site_cols, sites.at[0]), (col_dft_in, col_dft), (expand_in, expand), (spectra, kernels.at[0]),
        (first_in, first), (second_in, second), (flip_in, flip), (site_rows, sites.at[1]), (tolerance, limits),
    ]
    loads = [pltpu.make_async_copy(src, dst, load_sem.at[i]) for i, (src, dst) in enumerate(pairs)]
    for load in loads:
        load.start()

    def near_peer(d):
        spot = lax.rem(place + d, n_near)
        return spot, {"ty": spot // n_ka, "ka": lax.rem(spot, n_ka)}

    def far_peer(d):
        spot = lax.rem(tx + d, n_tx)
        return spot, {"tx": spot}

    barrier = pltpu.get_barrier_semaphore()
    for d in range(1, n_near):
        pl.semaphore_signal(barrier, inc=1, device_id=near_peer(d)[1], device_id_type=MESH)

    @pl.when(has_up)
    def _():
        pl.semaphore_signal(barrier, inc=1, device_id={"tx": tx - 1}, device_id_type=MESH)

    for d in range(1, n_tx):
        @pl.when(tx + d < n_tx)
        def _():
            pl.semaphore_signal(barrier, inc=1, device_id={"tx": tx + d}, device_id_type=MESH)

    for load in loads[:7]:
        load.wait()
    position = lax.broadcasted_iota(jnp.int32, (tile, rows_at.shape[2]), 0)
    row, col, length = fragments[0, 0], fragments[1, 0], fragments[2, 0]
    along = fragments[3, 0] == 0
    steps = [current[...]]
    for t in range(ITERS):
        move = frag_moves[0, 0, t : t + 1, :]
        lower, upper = jnp.minimum(move, 0), jnp.maximum(move, 0)
        row_low = jnp.where(along, row, row + lower)
        row_high = jnp.where(along, row + length, row + upper)
        col_low = jnp.where(along, col + lower, col)
        col_high = jnp.where(along, col + upper, col + length)
        sign = jnp.where(move > 0, 1.0, 0.0) - jnp.where(move < 0, 1.0, 0.0)
        in_rows = jnp.where((position >= row_low) & (position < row_high), sign, 0.0)
        in_cols = jnp.where((position >= col_low) & (position < col_high), 1.0, 0.0)
        strips = lax.dot_general(
            in_rows.astype(jnp.bfloat16), in_cols.astype(jnp.bfloat16), (((1,), (1,)), ((), ())),
            preferred_element_type=jnp.float32,
        )
        steps.append(jnp.clip(steps[-1] + strips, 0.0, 1.0))
    mask_out[...] = steps[2]
    current[...] = jnp.where(ka == 0, steps[1], steps[2])
    for k in range(my_weights.shape[0]):
        my_weights[pl.ds(k, 1), :] = jnp.full((1, my_weights.shape[1]), weight_of[k], jnp.float32)

    pl.semaphore_wait(barrier, n_near - 1 + tx + has_down.astype(jnp.int32))

    def hop(source, target, number, device):
        return pltpu.make_async_remote_copy(
            src_ref=source, dst_ref=target, send_sem=halo_send.at[number], recv_sem=halo_recv.at[number],
            device_id=device, device_id_type=MESH,
        )

    to_up = hop(current.at[pl.ds(0, half)], below, 0, {"tx": tx - 1})
    to_down = hop(current.at[pl.ds(half, half)], above, 1, {"tx": tx + 1})
    to_left = hop(packed.at[:, pl.ds(0, half)], right, 2, {"ty": ty - 1})
    to_right = hop(packed.at[:, pl.ds(half, half)], left, 3, {"ty": ty + 1})
    swap_weights = hop(my_weights, other_weights, 4, {"ka": 1 - ka})
    swap_spectra = hop(spectra, kernels.at[1], 5, {"ka": 1 - ka})
    pl.when(has_up)(to_up.start)
    pl.when(has_down)(to_down.start)
    swap_spectra.start()
    swap_weights.start()
    pairs = ((mask_out, new_mask), (image_out, intensity), (errors_out, edge_errors), (stats_out, stats))
    saves = [pltpu.make_async_copy(src, dst, save_sem.at[i]) for i, (src, dst) in enumerate(pairs)]
    saves[0].start()
    for d in range(1, n_tx):
        @pl.when(tx - d >= 0)
        def _():
            pl.semaphore_signal(ready, inc=1, device_id={"tx": tx - d}, device_id_type=MESH)

    def arrived(there, copy, buffer):
        pl.when(there)(copy.wait_recv)

        @pl.when(jnp.logical_not(there))
        def _():
            buffer[...] = jnp.zeros_like(buffer)

    loads[7].wait()
    part = exact(row_dft[:, HALO : HALO + tile], current[...])
    loads[8].wait()
    place_at = lax.broadcasted_iota(jnp.int32, (tile, tile), 0)
    chunks = site_rows.shape[2] // tile
    for chunk in range(chunks):
        at = slice(chunk * tile, (chunk + 1) * tile)
        wanted[:, at] = jnp.where(place_at == sites[0, 0, :, at], 1.0, 0.0).astype(jnp.bfloat16)
    for load in loads[9:]:
        load.wait()
    arrived(has_up, to_down, above)
    arrived(has_down, to_up, below)
    part = part + exact(row_dft[:, :HALO], above[...]) + exact(row_dft[:, HALO + tile :], below[...])
    packed[...] = part
    pl.when(has_left)(to_left.start)
    pl.when(has_right)(to_right.start)
    sums = exact(part, col_dft[HALO : HALO + tile, :])
    plus[...] = jnp.zeros_like(plus)
    minus[...] = jnp.zeros_like(minus)
    swap_weights.wait()
    swap_spectra.wait()
    arrived(has_left, to_right, left)
    arrived(has_right, to_left, right)
    sums = sums + exact(left[...], col_dft[:HALO, :]) + exact(right[...], col_dft[HALO + tile :, :])
    full = exact(expand[...], sums)
    scale = 1.0 / (ext * ext)
    spec_re[...] = (full[:BAND, :BAND] - full[BAND:, BAND:]) * scale
    spec_im[...] = (full[BAND:, :BAND] + full[:BAND, BAND:]) * -scale

    def inward(at, pair, k):
        k_re, k_im = kernels[at, k, 0], kernels[at, k, 1]
        re, im = spec_re[...], spec_im[...]
        product = jnp.concatenate([k_re * re - k_im * im, k_re * im + k_im * re], axis=0)
        hi, mid, lo = bf16_pieces(product, 3)
        upper, lower = jnp.concatenate([hi, mid], axis=1), jnp.concatenate([hi, lo], axis=1)
        inner = dot(upper, first[0]) + dot(upper, first[1]) + dot(lower, first[2])
        a, c, d, b = inner[:half, :half], inner[:half, half:], inner[half:, :half], inner[half:, half:]
        for slot, y in zip(pair, ((a - b, a + b), (c + d, d - c))):
            for side, part in enumerate(y):
                at_side = slice(side * half, (side + 1) * half)
                hi, mid, lo = bf16_pieces(part, 3)
                slot[0, :half, at_side] = hi
                slot[0, half:, at_side] = mid
                slot[1, :half, at_side] = hi
                slot[1, half:, at_side] = lo

    def outward(pair, weight):
        of_re, of_im = (
            dot(second[0], slot[0]) + dot(second[1], slot[0]) + dot(second[2], slot[1]) for slot in pair
        )
        a, c, d, b = of_re[:half], of_re[half:], of_im[:half], of_im[half:]
        p_re, p_im, m_re, m_im = a - b, c + d, a + b, d - c
        plus[...] += weight * (p_re * p_re + p_im * p_im)
        minus[...] += weight * (m_re * m_re + m_im * m_im)

    last = spectra.shape[0] - 1
    inward(0, slots[0], 0)
    inward(1, slots[1], 0)

    @pl.loop(0, spectra.shape[0] // 2)
    def _(i):
        k = 2 * i
        following = jnp.minimum(k + 2, last)
        outward(slots[0], my_weights[pl.ds(k, 1), :])
        inward(0, slots[2], k + 1)
        outward(slots[1], other_weights[pl.ds(k, 1), :])
        inward(1, slots[3], k + 1)
        outward(slots[2], my_weights[pl.ds(k + 1, 1), :])
        inward(0, slots[0], following)
        outward(slots[3], other_weights[pl.ds(k + 1, 1), :])
        inward(1, slots[1], following)

    both = jnp.concatenate([exact(flip[...], minus[...]), plus[...]], axis=0)
    picture = jnp.concatenate([exact(both[:, half:], flip[...]), both[:, :half]], axis=1)
    image[...] = picture
    grad_rows = (pltpu.roll(picture, tile - 1, 0) - pltpu.roll(picture, 1, 0)) * 0.5
    grad_cols = (pltpu.roll(picture, tile - 1, 1) - pltpu.roll(picture, 1, 1)) * 0.5
    slope = jnp.sqrt(grad_rows * grad_rows + grad_cols * grad_cols)
    field = (picture - LEVEL) / jnp.maximum(slope, SLOPE_FLOOR)
    field_hi, field_lo = bf16_pieces(field, 2)

    def to_other(source, target, number):
        return pltpu.make_async_remote_copy(
            src_ref=source, dst_ref=target, send_sem=near_send.at[n_near + number],
            recv_sem=near_recv.at[n_near + number], device_id={"ka": 1 - ka}, device_id_type=MESH,
        )

    send_image = to_other(image, image_in, 0)
    send_errors = to_other(errors, errors_in, 1)
    send_image.start()

    for chunk in range(chunks):
        at = slice(chunk * tile, (chunk + 1) * tile)
        sampled = dot(field_hi, wanted[:, at]) + dot(field_lo, wanted[:, at])
        sampled = jnp.where(place_at == sites[1, 0, :, at], sampled, 0.0)
        errors[:, at] = jnp.sum(sampled, axis=0, keepdims=True)

    found = errors[...]
    size = jnp.abs(found)
    limit = limits[ka].astype(jnp.float32) / 8.0
    peak = jnp.max(size, axis=1, keepdims=True)
    total = jnp.sum(1.0 / (1.0 + jnp.exp(SHARPNESS * (size - limit))), axis=1, keepdims=True)
    lane = lax.broadcasted_iota(jnp.int32, (1, 128), 1)
    is_peak = lane < 64
    near[place] = jnp.where(is_peak, peak, total)

    def small(buffer, mine, d, peer, send, recv):
        return pltpu.make_async_remote_copy(
            src_ref=buffer.at[mine], dst_ref=buffer.at[mine], send_sem=send.at[d], recv_sem=recv.at[mine],
            device_id=peer, device_id_type=MESH,
        )

    def swapped(buffer, mine, peers, send, recv):
        copies = [small(buffer, mine, d, peer, send, recv) for d, (_, peer) in peers]
        for copy in copies:
            copy.start()
        for d, (spot, peer) in peers:
            small(buffer, spot, d, peer, send, recv).wait_recv()
        return copies

    near_peers = [(d, near_peer(d)) for d in range(1, n_near)]

    @pl.when(has_down)
    def _():
        pl.semaphore_wait(ready, n_tx - 1 - tx)

    copies = swapped(near, place, near_peers, near_send, near_recv)
    of_iteration = []
    for t in range(n_ka):
        found_t = [near[y * n_ka + t] for y in range(n_ty)]
        of_iteration.append(
            jnp.where(is_peak, functools.reduce(jnp.maximum, found_t), functools.reduce(jnp.add, found_t))
        )
    far[tx] = jnp.where((lane & 32) == 0, of_iteration[0], of_iteration[1])
    far_copies = [small(far, tx, d, far_peer(d)[1], far_send, far_recv) for d in range(1, n_tx)]
    for copy in far_copies:
        copy.start()
    send_errors.start()
    send_image.wait()
    send_errors.wait()
    image_out[...] = jnp.where(ka == ITERS - 1, image[...], image_in[...])
    errors_out[0, 0, 0:1, :] = jnp.where(ka == 0, errors[...], errors_in[...])
    errors_out[0, 0, 1:2, :] = jnp.where(ka == 0, errors_in[...], errors[...])
    saves[1].start()
    saves[2].start()
    pl.when(has_up)(to_up.wait_send)
    pl.when(has_down)(to_down.wait_send)
    pl.when(has_left)(to_left.wait_send)
    pl.when(has_right)(to_right.wait_send)
    for copy in copies:
        copy.wait_send()
    for d in range(1, n_tx):
        spot, peer = far_peer(d)
        small(far, spot, 0, peer, far_send, far_recv).wait_recv()
    stats_out[...] = jnp.where(is_peak, jnp.max(far[...], axis=0), jnp.sum(far[...], axis=0))
    saves[3].start()
    for copy in far_copies:
        copy.wait_send()
    for save in saves:
        save.wait()


def deliver_kernel(
    n_sites, image, mask, errors, stats, intensity, new_mask, edge_errors, peaks, shares,
    image_at, mask_at, errors_at, stats_at, peaks_at, shares_at, sem,
):
    held = ((stats, stats_at, None), (image, image_at, intensity), (mask, mask_at, new_mask), (errors, errors_at, edge_errors))
    loads = [pltpu.make_async_copy(src, at, sem.at[0, i]) for i, (src, at, _) in enumerate(held)]
    copies = [pltpu.make_async_copy(at, dst, sem.at[1, i]) for i, (_, at, dst) in enumerate(held) if i > 0]
    for load in loads:
        load.start()
    loads[0].wait()
    final = stats_at[...]
    for t in range(ITERS):
        peaks_at[t] = final[0, 32 * t]
        shares_at[t] = final[0, 64 + 32 * t] * (1.0 / n_sites)
    pairs = ((peaks_at, peaks), (shares_at, shares))
    copies += [pltpu.make_async_copy(at, dst, sem.at[1, 4 * i]) for i, (at, dst) in enumerate(pairs)]
    for copy in copies[3:]:
        copy.start()
    for load, copy in zip(loads[1:], copies):
        load.wait()
        copy.start()
    for copy in copies:
        copy.wait()


def shards(
    mask_raster, frag_rows, frag_cols, frag_length, frag_orient, frag_moves,
    site_rows, site_cols, spectra, weights, tolerance,
):
    f32, i32, bf16 = jnp.float32, jnp.int32, jnp.bfloat16
    tile = mask_raster.shape[0]
    half = tile // 2
    n_sites = site_rows.shape[2]
    kernels = spectra.shape[0]
    n_near = lax.axis_size("ty") * lax.axis_size("ka")
    n_tx = lax.axis_size("tx")
    constants = [jnp.asarray(t) for t in tables(tile)]
    hbm = pl.BlockSpec(memory_space=pltpu.HBM)
    dma = pltpu.SemaphoreType.DMA
    errors_shape = jax.ShapeDtypeStruct((1, 1, ITERS, n_sites), f32)
    square = jax.ShapeDtypeStruct((tile, tile), f32)
    V = pltpu.VMEM
    new_mask, image, errors, stats = pl.pallas_call(
        opc_kernel,
        name="opc_kernel",
        out_shape=(square, square, errors_shape, jax.ShapeDtypeStruct((1, 128), f32)),
        in_specs=[hbm] * 17,
        out_specs=(hbm,) * 4,
        scratch_shapes=[
            V((tile, tile), f32), V((4, *frag_rows.shape), i32), V(frag_moves.shape, i32),
            V((2, *site_rows.shape), i32), V((2, *spectra.shape), f32), V((kernels, tile), f32),
            V((kernels, tile), f32), pltpu.SMEM(weights.shape, f32), pltpu.SMEM(tolerance.shape, i32),
            *(V(c.shape, c.dtype) for c in constants),
            V((HALO, tile), f32), V((HALO, tile), f32), V((PACKED, tile), f32),
            V((PACKED, HALO), f32), V((PACKED, HALO), f32), V((BAND, BAND), f32), V((BAND, BAND), f32),
            V((tile, n_sites), bf16),
            V((half, tile), f32), V((half, tile), f32), V((tile, tile), f32), V((tile, tile), f32),
            V((1, n_sites), f32), V((1, n_sites), f32), V((n_near, 1, 128), f32), V((n_tx, 1, 128), f32),
            V((tile, tile), f32), V((tile, tile), f32), V(errors_shape.shape, f32), V((1, 128), f32),
            *([V((2, tile, tile), bf16)] * 8), dma((17,)), dma((4,)), dma((6,)), dma((6,)), dma((n_near + 2,)), dma((n_near + 2,)), dma((n_tx,)), dma((n_tx,)),
            pltpu.SemaphoreType.REGULAR,
        ],
        compiler_params=pltpu.CompilerParams(collective_id=0, has_side_effects=True),
        cost_estimate=pl.CostEstimate(flops=4 * 10**9, bytes_accessed=4 * 10**6, transcendentals=0),
    )(
        mask_raster, frag_rows, frag_cols, frag_length, frag_orient, frag_moves, site_rows, site_cols,
        spectra, weights, tolerance, *constants,
    )
    pair = jax.ShapeDtypeStruct((ITERS,), f32)
    return pl.pallas_call(
        functools.partial(deliver_kernel, float(n_sites * n_tx * lax.axis_size("ty"))),
        name="deliver_kernel",
        out_shape=(square, square, errors_shape, pair, pair),
        in_specs=[hbm] * 4,
        out_specs=(hbm,) * 5,
        scratch_shapes=[
            V((tile, tile), f32), V((tile, tile), f32), V(errors_shape.shape, f32), V((1, 128), f32),
            pltpu.SMEM((ITERS,), f32), pltpu.SMEM((ITERS,), f32), dma((2, 5)),
        ],
    )(image, new_mask, errors, stats)


def solution(mesh):
    placed = (
        P(("groups", "tx"), "ty"),
        P(("groups", "tx"), "ty", None),
        P(("groups", "tx"), "ty", None),
        P(("groups", "tx"), "ty", None),
        P(("groups", "tx"), "ty", None),
        P(("groups", "tx"), "ty", None, None),
        P(("groups", "tx"), "ty", None),
        P(("groups", "tx"), "ty", None),
        P("ka", None, None, None),
        P("ka"),
        P(),
    )
    return jax.shard_map(
        shards,
        mesh=mesh,
        in_specs=placed,
        out_specs=(
            P(("groups", "tx"), "ty"),
            P(("groups", "tx"), "ty"),
            P(("groups", "tx"), "ty", None, None),
            P("groups"),
            P("groups"),
        ),
        check_vma=False,
    )
```

```python
import functools
import math

import jax
import jax.numpy as jnp
import numpy as np
from jax import lax
from jax.experimental import pallas as pl
from jax.experimental.pallas import tpu as pltpu
from jax.sharding import PartitionSpec as P

HALO = 128
BAND = 128
ITERS = 2
LEVEL = 0.4
SLOPE_FLOOR = 0.05
SHARPNESS = 8.0
MESH = pl.DeviceIdType.MESH
SIN_AT = 72
PACKED = 144


def bf16_pieces(x, count):
    pieces = []
    for _ in range(count):
        pieces.append(x.astype(jnp.bfloat16))
        x = x - pieces[-1].astype(jnp.float32)
    return pieces


def host_pieces(x):
    pieces = []
    for _ in range(3):
        pieces.append(x.astype(jnp.bfloat16))
        x = x - pieces[-1].astype(np.float64)
    return pieces


def tables(tile):
    ext = tile + 2 * HALO
    half = tile // 2
    theta = 2.0 * math.pi / ext
    inside = np.arange(ext) - (ext - 1) / 2
    low = BAND // 2
    order = np.roll(np.arange(ext), -HALO)
    order = np.concatenate([order[:tile], order[-HALO:], order[tile:-HALO]])
    inside = inside[order]
    rows = np.zeros((PACKED, ext))
    rows[: low + 1] = np.cos(theta * np.outer(np.arange(low + 1), inside))
    rows[SIN_AT : SIN_AT + low] = np.sin(theta * np.outer(np.arange(1, low + 1), inside))
    rows = np.concatenate(host_pieces(rows), axis=0)
    rows = np.stack([rows[:, :tile], rows[:, tile:]])
    freq = np.arange(BAND) - low
    turns = theta * np.outer(inside, freq)
    cols = np.stack(host_pieces(np.concatenate([np.cos(turns), np.sin(turns)], axis=1)))
    cols = np.stack([cols[:, :tile], cols[:, tile:]])
    expand = np.zeros((2 * BAND, PACKED))
    for u, f in enumerate(freq):
        expand[u, abs(f)] = 1.0
        if f != 0:
            expand[BAND + u, SIN_AT + abs(f) - 1] = np.sign(f)
    out = theta * np.outer(freq, np.arange(half) + 0.5)
    basis = np.concatenate([np.cos(out), np.sin(out)], axis=1)
    hi, mid, lo = host_pieces(basis)
    first = np.stack([np.concatenate(b, axis=0) for b in ((hi, hi), (mid, mid), (lo, hi))])
    second = np.ascontiguousarray(first.swapaxes(1, 2))
    flip = np.eye(half)[::-1]
    flip = np.concatenate([flip, flip], axis=1)
    bf16 = jnp.bfloat16
    return rows, cols, expand.astype(bf16), first, second, flip.astype(bf16), flip.T.astype(bf16)


def dot(left, right):
    return jnp.dot(left, right, preferred_element_type=jnp.float32)


def pieces_sum(of_hi, of_mid, of_lo):
    n = of_lo.shape[0]
    return of_hi[:n] + ((of_mid[:n] + of_hi[n : 2 * n]) + ((of_lo + of_hi[2 * n :]) + of_mid[n:]))


def rows_product(table, x):
    n = PACKED
    hi, mid, lo = bf16_pieces(x, 3)
    return pieces_sum(dot(table[...], hi), dot(table[: 2 * n], mid), dot(table[:n], lo))


def cols_product(x, table):
    n = PACKED
    pieces = jnp.concatenate(bf16_pieces(x, 3), axis=0)
    return pieces_sum(dot(pieces, table[0]), dot(pieces[: 2 * n], table[1]), dot(pieces[:n], table[2]))


def opc_kernel(
    mask, rows_at, cols_at, lengths, orients, moves, site_rows, site_cols, spectra, weights, tolerance,
    row_dft_in, col_dft_in, expand_in, first_in, second_in, flip_rows_in, flip_cols_in,
    new_mask, intensity, edge_errors, stats,
    current, fragments, frag_moves, sites, kernels, my_weights, other_weights, weight_of, limits,
    row_dft, col_dft, expand, first, second, flip_rows, flip_cols,
    halo_rows, packed, halo_cols, sums, spec_re, spec_im, wanted,
    plus, minus, image, image_in, errors, errors_in, near, far, mask_out, image_out, errors_out, stats_out,
    slot_a, slot_b, slot_c, slot_d, slot_e, slot_f, slot_g, slot_h, load_sem, save_sem, halo_send, halo_recv, near_send, near_recv, far_send, far_recv, ready,
):
    tx, ty, ka = lax.axis_index("tx"), lax.axis_index("ty"), lax.axis_index("ka")
    n_tx, n_ty, n_ka = lax.axis_size("tx"), lax.axis_size("ty"), lax.axis_size("ka")
    n_near = n_ty * n_ka
    place = ty * n_ka + ka
    tile = mask.shape[0]
    ext = tile + 2 * HALO
    half = tile // 2
    slots = ((slot_a, slot_b), (slot_c, slot_d), (slot_e, slot_f), (slot_g, slot_h))
    has_up, has_down = tx > 0, tx < n_tx - 1
    has_left, has_right = ty > 0, ty < n_ty - 1

    pairs = [
        (mask, current), (rows_at, fragments.at[0]), (cols_at, fragments.at[1]), (lengths, fragments.at[2]),
        (orients, fragments.at[3]), (moves, frag_moves), (weights, weight_of), (row_dft_in, row_dft),
        (site_cols, sites.at[0]), (col_dft_in, col_dft), (expand_in, expand), (spectra, kernels.at[0]),
        (first_in, first), (second_in, second), (flip_rows_in, flip_rows), (flip_cols_in, flip_cols),
        (site_rows, sites.at[1]), (tolerance, limits),
    ]
    loads = [pltpu.make_async_copy(src, dst, load_sem.at[i]) for i, (src, dst) in enumerate(pairs)]
    for load in loads:
        load.start()

    def near_peer(d):
        spot = lax.rem(place + d, n_near)
        return spot, {"ty": spot // n_ka, "ka": lax.rem(spot, n_ka)}

    def far_peer(d):
        spot = lax.rem(tx + d, n_tx)
        return spot, {"tx": spot}

    barrier = pltpu.get_barrier_semaphore()
    for d in range(1, n_near):
        pl.semaphore_signal(barrier, inc=1, device_id=near_peer(d)[1], device_id_type=MESH)

    @pl.when(has_up)
    def _():
        pl.semaphore_signal(barrier, inc=1, device_id={"tx": tx - 1}, device_id_type=MESH)

    for d in range(1, n_tx):
        @pl.when(tx + d < n_tx)
        def _():
            pl.semaphore_signal(barrier, inc=1, device_id={"tx": tx + d}, device_id_type=MESH)

    for load in loads[:7]:
        load.wait()
    position = lax.broadcasted_iota(jnp.int32, (tile, rows_at.shape[2]), 0)
    row, col, length = fragments[0, 0], fragments[1, 0], fragments[2, 0]
    along = fragments[3, 0] == 0
    steps = [current[...]]
    for t in range(ITERS):
        move = frag_moves[0, 0, t : t + 1, :]
        lower, upper = jnp.minimum(move, 0), jnp.maximum(move, 0)
        row_low = jnp.where(along, row, row + lower)
        row_high = jnp.where(along, row + length, row + upper)
        col_low = jnp.where(along, col + lower, col)
        col_high = jnp.where(along, col + upper, col + length)
        sign = jnp.where(move > 0, 1.0, 0.0) - jnp.where(move < 0, 1.0, 0.0)
        in_rows = jnp.where((position >= row_low) & (position < row_high), sign, 0.0)
        in_cols = jnp.where((position >= col_low) & (position < col_high), 1.0, 0.0)
        strips = lax.dot_general(
            in_rows.astype(jnp.bfloat16), in_cols.astype(jnp.bfloat16), (((1,), (1,)), ((), ())),
            preferred_element_type=jnp.float32,
        )
        steps.append(jnp.clip(steps[-1] + strips, 0.0, 1.0))
    mask_out[...] = steps[2]
    current[...] = jnp.where(ka == 0, steps[1], steps[2])
    for k in range(my_weights.shape[0]):
        my_weights[pl.ds(k, 1), :] = jnp.full((1, my_weights.shape[1]), weight_of[k], jnp.float32)

    pl.semaphore_wait(barrier, n_near - 1 + tx + has_down.astype(jnp.int32))

    def hop(source, target, number, device):
        return pltpu.make_async_remote_copy(
            src_ref=source, dst_ref=target, send_sem=halo_send.at[number], recv_sem=halo_recv.at[number],
            device_id=device, device_id_type=MESH,
        )

    above, below = halo_rows.at[pl.ds(0, HALO)], halo_rows.at[pl.ds(HALO, HALO)]
    left, right = halo_cols.at[:, pl.ds(0, HALO)], halo_cols.at[:, pl.ds(HALO, HALO)]
    to_up = hop(current.at[pl.ds(0, half)], below, 0, {"tx": tx - 1})
    to_down = hop(current.at[pl.ds(half, half)], above, 1, {"tx": tx + 1})
    to_left = hop(packed.at[:, pl.ds(0, half)], right, 2, {"ty": ty - 1})
    to_right = hop(packed.at[:, pl.ds(half, half)], left, 3, {"ty": ty + 1})
    swap_weights = hop(my_weights, other_weights, 4, {"ka": 1 - ka})
    swap_spectra = hop(spectra, kernels.at[1], 5, {"ka": 1 - ka})
    pl.when(has_up)(to_up.start)
    pl.when(has_down)(to_down.start)
    swap_spectra.start()
    swap_weights.start()
    pairs = ((mask_out, new_mask), (image_out, intensity), (errors_out, edge_errors), (stats_out, stats))
    saves = [pltpu.make_async_copy(src, dst, save_sem.at[i]) for i, (src, dst) in enumerate(pairs)]
    saves[0].start()
    for d in range(1, n_tx):
        @pl.when(tx - d >= 0)
        def _():
            pl.semaphore_signal(ready, inc=1, device_id={"tx": tx - d}, device_id_type=MESH)

    def arrived(there, copy, buffer):
        pl.when(there)(copy.wait_recv)

        @pl.when(jnp.logical_not(there))
        def _():
            buffer[...] = jnp.zeros_like(buffer)

    loads[7].wait()
    packed[...] = rows_product(row_dft.at[0], current[...])
    loads[8].wait()
    place_at = lax.broadcasted_iota(jnp.int32, (tile, tile), 0)
    chunks = site_rows.shape[2] // tile
    for chunk in range(chunks):
        at = slice(chunk * tile, (chunk + 1) * tile)
        wanted[:, at] = jnp.where(place_at == sites[0, 0, :, at], 1.0, 0.0).astype(jnp.bfloat16)
    for load in loads[9:]:
        load.wait()
    arrived(has_up, to_down, above)
    arrived(has_down, to_up, below)
    packed[...] += rows_product(row_dft.at[1], halo_rows[...])
    pl.when(has_left)(to_left.start)
    pl.when(has_right)(to_right.start)
    sums[...] = cols_product(packed[...], col_dft.at[0])
    plus[...] = jnp.zeros_like(plus)
    minus[...] = jnp.zeros_like(minus)
    swap_weights.wait()
    swap_spectra.wait()
    arrived(has_left, to_right, left)
    arrived(has_right, to_left, right)
    total = sums[...] + cols_product(halo_cols[...], col_dft.at[1])
    full = sum(dot(expand[...], piece) for piece in bf16_pieces(total, 3))
    scale = 1.0 / (ext * ext)
    spec_re[...] = (full[:BAND, :BAND] - full[BAND:, BAND:]) * scale
    spec_im[...] = (full[BAND:, :BAND] + full[:BAND, BAND:]) * -scale

    def inward(at, pair, k):
        k_re, k_im = kernels[at, k, 0], kernels[at, k, 1]
        re, im = spec_re[...], spec_im[...]
        product = jnp.concatenate([k_re * re - k_im * im, k_re * im + k_im * re], axis=0)
        hi, mid, lo = bf16_pieces(product, 3)
        upper, lower = jnp.concatenate([hi, mid], axis=1), jnp.concatenate([hi, lo], axis=1)
        inner = dot(upper, first[0]) + dot(upper, first[1]) + dot(lower, first[2])
        a, c, d, b = inner[:half, :half], inner[:half, half:], inner[half:, :half], inner[half:, half:]
        for slot, y in zip(pair, ((a - b, a + b), (c + d, d - c))):
            for side, part in enumerate(y):
                at_side = slice(side * half, (side + 1) * half)
                hi, mid, lo = bf16_pieces(part, 3)
                slot[0, :half, at_side] = hi
                slot[0, half:, at_side] = mid
                slot[1, :half, at_side] = hi
                slot[1, half:, at_side] = lo

    def outward(pair, weight):
        of_re, of_im = (
            dot(second[0], slot[0]) + dot(second[1], slot[0]) + dot(second[2], slot[1]) for slot in pair
        )
        a, c, d, b = of_re[:half], of_re[half:], of_im[:half], of_im[half:]
        p_re, p_im, m_re, m_im = a - b, c + d, a + b, d - c
        plus[...] += weight * (p_re * p_re + p_im * p_im)
        minus[...] += weight * (m_re * m_re + m_im * m_im)

    last = spectra.shape[0] - 1
    inward(0, slots[0], 0)
    inward(1, slots[1], 0)

    @pl.loop(0, spectra.shape[0] // 2)
    def _(i):
        k = 2 * i
        following = jnp.minimum(k + 2, last)
        outward(slots[0], my_weights[pl.ds(k, 1), :])
        inward(0, slots[2], k + 1)
        outward(slots[1], other_weights[pl.ds(k, 1), :])
        inward(1, slots[3], k + 1)
        outward(slots[2], my_weights[pl.ds(k + 1, 1), :])
        inward(0, slots[0], following)
        outward(slots[3], other_weights[pl.ds(k + 1, 1), :])
        inward(1, slots[1], following)

    hi, mid, lo = bf16_pieces(minus[...], 3)
    turned = dot(flip_rows[...], jnp.concatenate([hi, mid], axis=0)) + dot(flip_rows[:, :half], lo)
    both = jnp.concatenate([turned, plus[...]], axis=0)
    hi, mid, lo = bf16_pieces(both[:, half:], 3)
    turned = dot(jnp.concatenate([hi, mid], axis=1), flip_cols[...]) + dot(lo, flip_cols[:half])
    picture = jnp.concatenate([turned, both[:, :half]], axis=1)
    image[...] = picture
    grad_rows = (pltpu.roll(picture, tile - 1, 0) - pltpu.roll(picture, 1, 0)) * 0.5
    grad_cols = (pltpu.roll(picture, tile - 1, 1) - pltpu.roll(picture, 1, 1)) * 0.5
    slope = jnp.sqrt(grad_rows * grad_rows + grad_cols * grad_cols)
    field = (picture - LEVEL) / jnp.maximum(slope, SLOPE_FLOOR)
    field_hi, field_lo = bf16_pieces(field, 2)

    def to_other(source, target, number):
        return pltpu.make_async_remote_copy(
            src_ref=source, dst_ref=target, send_sem=near_send.at[n_near + number],
            recv_sem=near_recv.at[n_near + number], device_id={"ka": 1 - ka}, device_id_type=MESH,
        )

    send_image = to_other(image, image_in, 0)
    send_errors = to_other(errors, errors_in, 1)
    send_image.start()

    for chunk in range(chunks):
        at = slice(chunk * tile, (chunk + 1) * tile)
        sampled = dot(field_hi, wanted[:, at]) + dot(field_lo, wanted[:, at])
        sampled = jnp.where(place_at == sites[1, 0, :, at], sampled, 0.0)
        errors[:, at] = jnp.sum(sampled, axis=0, keepdims=True)

    found = errors[...]
    size = jnp.abs(found)
    limit = limits[ka].astype(jnp.float32) / 8.0
    peak = jnp.max(size, axis=1, keepdims=True)
    total = jnp.sum(1.0 / (1.0 + jnp.exp(SHARPNESS * (size - limit))), axis=1, keepdims=True)
    lane = lax.broadcasted_iota(jnp.int32, (1, 128), 1)
    is_peak = lane < 64
    near[place] = jnp.where(is_peak, peak, total)

    def small(buffer, mine, d, peer, send, recv):
        return pltpu.make_async_remote_copy(
            src_ref=buffer.at[mine], dst_ref=buffer.at[mine], send_sem=send.at[d], recv_sem=recv.at[mine],
            device_id=peer, device_id_type=MESH,
        )

    def swapped(buffer, mine, peers, send, recv):
        copies = [small(buffer, mine, d, peer, send, recv) for d, (_, peer) in peers]
        for copy in copies:
            copy.start()
        for d, (spot, peer) in peers:
            small(buffer, spot, d, peer, send, recv).wait_recv()
        return copies

    near_peers = [(d, near_peer(d)) for d in range(1, n_near)]

    @pl.when(has_down)
    def _():
        pl.semaphore_wait(ready, n_tx - 1 - tx)

    copies = swapped(near, place, near_peers, near_send, near_recv)
    of_iteration = []
    for t in range(n_ka):
        found_t = [near[y * n_ka + t] for y in range(n_ty)]
        of_iteration.append(
            jnp.where(is_peak, functools.reduce(jnp.maximum, found_t), functools.reduce(jnp.add, found_t))
        )
    far[tx] = jnp.where((lane & 32) == 0, of_iteration[0], of_iteration[1])
    far_copies = [small(far, tx, d, far_peer(d)[1], far_send, far_recv) for d in range(1, n_tx)]
    for copy in far_copies:
        copy.start()
    send_errors.start()
    send_image.wait()
    send_errors.wait()
    image_out[...] = jnp.where(ka == ITERS - 1, image[...], image_in[...])
    errors_out[0, 0, 0:1, :] = jnp.where(ka == 0, errors[...], errors_in[...])
    errors_out[0, 0, 1:2, :] = jnp.where(ka == 0, errors_in[...], errors[...])
    saves[1].start()
    saves[2].start()
    pl.when(has_up)(to_up.wait_send)
    pl.when(has_down)(to_down.wait_send)
    pl.when(has_left)(to_left.wait_send)
    pl.when(has_right)(to_right.wait_send)
    for copy in copies:
        copy.wait_send()
    for d in range(1, n_tx):
        spot, peer = far_peer(d)
        small(far, spot, 0, peer, far_send, far_recv).wait_recv()
    stats_out[...] = jnp.where(is_peak, jnp.max(far[...], axis=0), jnp.sum(far[...], axis=0))
    saves[3].start()
    for copy in far_copies:
        copy.wait_send()
    for save in saves:
        save.wait()


def deliver_kernel(
    n_sites, image, mask, errors, stats, intensity, new_mask, edge_errors, peaks, shares,
    image_at, mask_at, errors_at, stats_at, peaks_at, shares_at, sem,
):
    held = ((stats, stats_at, None), (image, image_at, intensity), (mask, mask_at, new_mask), (errors, errors_at, edge_errors))
    loads = [pltpu.make_async_copy(src, at, sem.at[0, i]) for i, (src, at, _) in enumerate(held)]
    copies = [pltpu.make_async_copy(at, dst, sem.at[1, i]) for i, (_, at, dst) in enumerate(held) if i > 0]
    for load in loads:
        load.start()
    loads[0].wait()
    final = stats_at[...]
    for t in range(ITERS):
        peaks_at[t] = final[0, 32 * t]
        shares_at[t] = final[0, 64 + 32 * t] * (1.0 / n_sites)
    pairs = ((peaks_at, peaks), (shares_at, shares))
    copies += [pltpu.make_async_copy(at, dst, sem.at[1, 4 * i]) for i, (at, dst) in enumerate(pairs)]
    for copy in copies[3:]:
        copy.start()
    for load, copy in zip(loads[1:], copies):
        load.wait()
        copy.start()
    for copy in copies:
        copy.wait()


def shards(
    mask_raster, frag_rows, frag_cols, frag_length, frag_orient, frag_moves,
    site_rows, site_cols, spectra, weights, tolerance,
):
    f32, i32, bf16 = jnp.float32, jnp.int32, jnp.bfloat16
    tile = mask_raster.shape[0]
    half = tile // 2
    n_sites = site_rows.shape[2]
    kernels = spectra.shape[0]
    n_near = lax.axis_size("ty") * lax.axis_size("ka")
    n_tx = lax.axis_size("tx")
    constants = [jnp.asarray(t) for t in tables(tile)]
    hbm = pl.BlockSpec(memory_space=pltpu.HBM)
    dma = pltpu.SemaphoreType.DMA
    errors_shape = jax.ShapeDtypeStruct((1, 1, ITERS, n_sites), f32)
    square = jax.ShapeDtypeStruct((tile, tile), f32)
    V = pltpu.VMEM
    new_mask, image, errors, stats = pl.pallas_call(
        opc_kernel,
        name="opc_kernel",
        out_shape=(square, square, errors_shape, jax.ShapeDtypeStruct((1, 128), f32)),
        in_specs=[hbm] * 18,
        out_specs=(hbm,) * 4,
        scratch_shapes=[
            V((tile, tile), f32), V((4, *frag_rows.shape), i32), V(frag_moves.shape, i32),
            V((2, *site_rows.shape), i32), V((2, *spectra.shape), f32), V((kernels, tile), f32),
            V((kernels, tile), f32), pltpu.SMEM(weights.shape, f32), pltpu.SMEM(tolerance.shape, i32),
            *(V(c.shape, c.dtype) for c in constants),
            V((2 * HALO, tile), f32), V((PACKED, tile), f32), V((PACKED, 2 * HALO), f32), V((PACKED, 2 * BAND), f32),
            V((BAND, BAND), f32), V((BAND, BAND), f32),
            V((tile, n_sites), bf16),
            V((half, tile), f32), V((half, tile), f32), V((tile, tile), f32), V((tile, tile), f32),
            V((1, n_sites), f32), V((1, n_sites), f32), V((n_near, 1, 128), f32), V((n_tx, 1, 128), f32),
            V((tile, tile), f32), V((tile, tile), f32), V(errors_shape.shape, f32), V((1, 128), f32),
            *([V((2, tile, tile), bf16)] * 8), dma((18,)), dma((4,)), dma((6,)), dma((6,)), dma((n_near + 2,)), dma((n_near + 2,)), dma((n_tx,)), dma((n_tx,)),
            pltpu.SemaphoreType.REGULAR,
        ],
        compiler_params=pltpu.CompilerParams(collective_id=0, has_side_effects=True),
        cost_estimate=pl.CostEstimate(flops=4 * 10**9, bytes_accessed=4 * 10**6, transcendentals=0),
    )(
        mask_raster, frag_rows, frag_cols, frag_length, frag_orient, frag_moves, site_rows, site_cols,
        spectra, weights, tolerance, *constants,
    )
    pair = jax.ShapeDtypeStruct((ITERS,), f32)
    return pl.pallas_call(
        functools.partial(deliver_kernel, float(n_sites * n_tx * lax.axis_size("ty"))),
        name="deliver_kernel",
        out_shape=(square, square, errors_shape, pair, pair),
        in_specs=[hbm] * 4,
        out_specs=(hbm,) * 5,
        scratch_shapes=[
            V((tile, tile), f32), V((tile, tile), f32), V(errors_shape.shape, f32), V((1, 128), f32),
            pltpu.SMEM((ITERS,), f32), pltpu.SMEM((ITERS,), f32), dma((2, 5)),
        ],
    )(image, new_mask, errors, stats)


def solution(mesh):
    placed = (
        P(("groups", "tx"), "ty"),
        P(("groups", "tx"), "ty", None),
        P(("groups", "tx"), "ty", None),
        P(("groups", "tx"), "ty", None),
        P(("groups", "tx"), "ty", None),
        P(("groups", "tx"), "ty", None, None),
        P(("groups", "tx"), "ty", None),
        P(("groups", "tx"), "ty", None),
        P("ka", None, None, None),
        P("ka"),
        P(),
    )
    return jax.shard_map(
        shards,
        mesh=mesh,
        in_specs=placed,
        out_specs=(
            P(("groups", "tx"), "ty"),
            P(("groups", "tx"), "ty"),
            P(("groups", "tx"), "ty", None, None),
            P("groups"),
            P("groups"),
        ),
        check_vma=False,
    )
```

```python
import functools
import math

import jax
import jax.numpy as jnp
import numpy as np
from jax import lax
from jax.experimental import pallas as pl
from jax.experimental.pallas import tpu as pltpu
from jax.sharding import PartitionSpec as P

HALO = 128
BAND = 128
ITERS = 2
LEVEL = 0.4
SLOPE_FLOOR = 0.05
SHARPNESS = 8.0
MESH = pl.DeviceIdType.MESH
SIN_AT = 72
PACKED = 144


def bf16_pieces(x, count):
    pieces = []
    for _ in range(count):
        pieces.append(x.astype(jnp.bfloat16))
        x = x - pieces[-1].astype(jnp.float32)
    return pieces


def host_pieces(x):
    pieces = []
    for _ in range(3):
        pieces.append(x.astype(jnp.bfloat16))
        x = x - pieces[-1].astype(np.float64)
    return pieces


def tables(tile):
    ext = tile + 2 * HALO
    half = tile // 2
    theta = 2.0 * math.pi / ext
    inside = np.arange(ext) - (ext - 1) / 2
    low = BAND // 2
    order = np.roll(np.arange(ext), -HALO)
    order = np.concatenate([order[:tile], order[-HALO:], order[tile:-HALO]])
    inside = inside[order]
    rows = np.zeros((PACKED, ext))
    rows[: low + 1] = np.cos(theta * np.outer(np.arange(low + 1), inside))
    rows[SIN_AT : SIN_AT + low] = np.sin(theta * np.outer(np.arange(1, low + 1), inside))
    rows = np.concatenate(host_pieces(rows), axis=0)
    rows = np.stack([rows[:, :tile], rows[:, tile:]])
    freq = np.arange(BAND) - low
    turns = theta * np.outer(inside, freq)
    cols = np.stack(host_pieces(np.concatenate([np.cos(turns), np.sin(turns)], axis=1)))
    cols = np.stack([cols[:, :tile], cols[:, tile:]])
    expand = np.zeros((2 * BAND, PACKED))
    for u, f in enumerate(freq):
        expand[u, abs(f)] = 1.0
        if f != 0:
            expand[BAND + u, SIN_AT + abs(f) - 1] = np.sign(f)
    out = theta * np.outer(freq, np.arange(half) + 0.5)
    basis = np.concatenate([np.cos(out), np.sin(out)], axis=1)
    hi, mid, lo = host_pieces(basis)
    first = np.stack([np.concatenate(b, axis=0) for b in ((hi, hi), (mid, mid), (lo, hi))])
    second = np.ascontiguousarray(first.swapaxes(1, 2))
    flip = np.eye(half)[::-1]
    flip = np.concatenate([flip, flip], axis=1)
    bf16 = jnp.bfloat16
    return rows, cols, expand.astype(bf16), first, second, flip.astype(bf16), flip.T.astype(bf16)


def dot(left, right):
    return jnp.dot(left, right, preferred_element_type=jnp.float32)


def pieces_sum(of_hi, of_mid, of_lo):
    n = of_lo.shape[0]
    return of_hi[:n] + ((of_mid[:n] + of_hi[n : 2 * n]) + ((of_lo + of_hi[2 * n :]) + of_mid[n:]))


def rows_product(table, x):
    n = PACKED
    hi, mid, lo = bf16_pieces(x, 3)
    return pieces_sum(dot(table[...], hi), dot(table[: 2 * n], mid), dot(table[:n], lo))


def cols_product(x, table):
    n = PACKED
    pieces = jnp.concatenate(bf16_pieces(x, 3), axis=0)
    return pieces_sum(dot(pieces, table[0]), dot(pieces[: 2 * n], table[1]), dot(pieces[:n], table[2]))


def opc_kernel(
    mask, rows_at, cols_at, lengths, orients, moves, site_rows, site_cols, spectra, weights, tolerance,
    row_dft_in, col_dft_in, expand_in, first_in, second_in, flip_rows_in, flip_cols_in,
    new_mask, intensity, edge_errors, stats,
    current, fragments, frag_moves, sites, kernels, my_weights, other_weights, weight_of, limits,
    row_dft, col_dft, expand, first, second, flip_rows, flip_cols,
    halo_rows, packed, halo_cols, sums, spec_re, spec_im, wanted,
    plus, minus, image, image_in, errors, errors_in, near, far, mask_out, image_out, errors_out, stats_out,
    slot_a, slot_b, slot_c, slot_d, slot_e, slot_f, slot_g, slot_h, load_sem, save_sem, halo_send, halo_recv, near_send, near_recv, far_send, far_recv, relay_out, relay_in, relay_send, relay_recv, ready,
):
    tx, ty, ka = lax.axis_index("tx"), lax.axis_index("ty"), lax.axis_index("ka")
    n_tx, n_ty, n_ka = lax.axis_size("tx"), lax.axis_size("ty"), lax.axis_size("ka")
    n_near = n_ty * n_ka
    place = ty * n_ka + ka
    tile = mask.shape[0]
    ext = tile + 2 * HALO
    half = tile // 2
    slots = ((slot_a, slot_b), (slot_c, slot_d), (slot_e, slot_f), (slot_g, slot_h))
    has_up, has_down = tx > 0, tx < n_tx - 1
    has_left, has_right = ty > 0, ty < n_ty - 1

    pairs = [
        (mask, current), (rows_at, fragments.at[0]), (cols_at, fragments.at[1]), (lengths, fragments.at[2]),
        (orients, fragments.at[3]), (moves, frag_moves), (weights, weight_of), (row_dft_in, row_dft),
        (site_cols, sites.at[0]), (col_dft_in, col_dft), (expand_in, expand), (spectra, kernels.at[0]),
        (first_in, first), (second_in, second), (flip_rows_in, flip_rows), (flip_cols_in, flip_cols),
        (site_rows, sites.at[1]), (tolerance, limits),
    ]
    loads = [pltpu.make_async_copy(src, dst, load_sem.at[i]) for i, (src, dst) in enumerate(pairs)]
    for load in loads:
        load.start()

    def near_peer(d):
        spot = lax.rem(place + d, n_near)
        return spot, {"ty": spot // n_ka, "ka": lax.rem(spot, n_ka)}

    reach = n_tx // 4
    far_spots = [lax.rem(tx + d, n_tx) for d in (*range(1, reach + 1), *range(n_tx - reach, n_tx))]
    below_me = [spot < tx for spot in far_spots]
    n_below = sum(lower.astype(jnp.int32) for lower in below_me)

    barrier = pltpu.get_barrier_semaphore()
    for d in range(1, n_near):
        pl.semaphore_signal(barrier, inc=1, device_id=near_peer(d)[1], device_id_type=MESH)

    @pl.when(has_up)
    def _():
        pl.semaphore_signal(barrier, inc=1, device_id={"tx": tx - 1}, device_id_type=MESH)

    for spot, lower in zip(far_spots, below_me):
        @pl.when(jnp.logical_not(lower))
        def _():
            pl.semaphore_signal(barrier, inc=1, device_id={"tx": spot}, device_id_type=MESH)

    for load in loads[:7]:
        load.wait()
    position = lax.broadcasted_iota(jnp.int32, (tile, rows_at.shape[2]), 0)
    row, col, length = fragments[0, 0], fragments[1, 0], fragments[2, 0]
    along = fragments[3, 0] == 0
    steps = [current[...]]
    for t in range(ITERS):
        move = frag_moves[0, 0, t : t + 1, :]
        lower, upper = jnp.minimum(move, 0), jnp.maximum(move, 0)
        row_low = jnp.where(along, row, row + lower)
        row_high = jnp.where(along, row + length, row + upper)
        col_low = jnp.where(along, col + lower, col)
        col_high = jnp.where(along, col + upper, col + length)
        sign = jnp.where(move > 0, 1.0, 0.0) - jnp.where(move < 0, 1.0, 0.0)
        in_rows = jnp.where((position >= row_low) & (position < row_high), sign, 0.0)
        in_cols = jnp.where((position >= col_low) & (position < col_high), 1.0, 0.0)
        strips = lax.dot_general(
            in_rows.astype(jnp.bfloat16), in_cols.astype(jnp.bfloat16), (((1,), (1,)), ((), ())),
            preferred_element_type=jnp.float32,
        )
        steps.append(jnp.clip(steps[-1] + strips, 0.0, 1.0))
    mask_out[...] = steps[2]
    current[...] = jnp.where(ka == 0, steps[1], steps[2])
    for k in range(my_weights.shape[0]):
        my_weights[pl.ds(k, 1), :] = jnp.full((1, my_weights.shape[1]), weight_of[k], jnp.float32)

    pl.semaphore_wait(barrier, n_near - 1 + n_below + has_down.astype(jnp.int32))

    def hop(source, target, number, device):
        return pltpu.make_async_remote_copy(
            src_ref=source, dst_ref=target, send_sem=halo_send.at[number], recv_sem=halo_recv.at[number],
            device_id=device, device_id_type=MESH,
        )

    above, below = halo_rows.at[pl.ds(0, HALO)], halo_rows.at[pl.ds(HALO, HALO)]
    left, right = halo_cols.at[:, pl.ds(0, HALO)], halo_cols.at[:, pl.ds(HALO, HALO)]
    to_up = hop(current.at[pl.ds(0, half)], below, 0, {"tx": tx - 1})
    to_down = hop(current.at[pl.ds(half, half)], above, 1, {"tx": tx + 1})
    to_left = hop(packed.at[:, pl.ds(0, half)], right, 2, {"ty": ty - 1})
    to_right = hop(packed.at[:, pl.ds(half, half)], left, 3, {"ty": ty + 1})
    swap_weights = hop(my_weights, other_weights, 4, {"ka": 1 - ka})
    swap_spectra = hop(spectra, kernels.at[1], 5, {"ka": 1 - ka})
    pl.when(has_up)(to_up.start)
    pl.when(has_down)(to_down.start)
    swap_spectra.start()
    swap_weights.start()
    pairs = ((mask_out, new_mask), (image_out, intensity), (errors_out, edge_errors), (stats_out, stats))
    saves = [pltpu.make_async_copy(src, dst, save_sem.at[i]) for i, (src, dst) in enumerate(pairs)]
    saves[0].start()
    for spot, lower in zip(far_spots, below_me):
        @pl.when(lower)
        def _():
            pl.semaphore_signal(ready, inc=1, device_id={"tx": spot}, device_id_type=MESH)

    def arrived(there, copy, buffer):
        pl.when(there)(copy.wait_recv)

        @pl.when(jnp.logical_not(there))
        def _():
            buffer[...] = jnp.zeros_like(buffer)

    loads[7].wait()
    packed[...] = rows_product(row_dft.at[0], current[...])
    loads[8].wait()
    place_at = lax.broadcasted_iota(jnp.int32, (tile, tile), 0)
    chunks = site_rows.shape[2] // tile
    for chunk in range(chunks):
        at = slice(chunk * tile, (chunk + 1) * tile)
        wanted[:, at] = jnp.where(place_at == sites[0, 0, :, at], 1.0, 0.0).astype(jnp.bfloat16)
    for load in loads[9:]:
        load.wait()
    arrived(has_up, to_down, above)
    arrived(has_down, to_up, below)
    packed[...] += rows_product(row_dft.at[1], halo_rows[...])
    pl.when(has_left)(to_left.start)
    pl.when(has_right)(to_right.start)
    sums[...] = cols_product(packed[...], col_dft.at[0])
    plus[...] = jnp.zeros_like(plus)
    minus[...] = jnp.zeros_like(minus)
    swap_weights.wait()
    swap_spectra.wait()
    arrived(has_left, to_right, left)
    arrived(has_right, to_left, right)
    total = sums[...] + cols_product(halo_cols[...], col_dft.at[1])
    full = sum(dot(expand[...], piece) for piece in bf16_pieces(total, 3))
    scale = 1.0 / (ext * ext)
    spec_re[...] = (full[:BAND, :BAND] - full[BAND:, BAND:]) * scale
    spec_im[...] = (full[BAND:, :BAND] + full[:BAND, BAND:]) * -scale

    def inward(at, pair, k):
        k_re, k_im = kernels[at, k, 0], kernels[at, k, 1]
        re, im = spec_re[...], spec_im[...]
        product = jnp.concatenate([k_re * re - k_im * im, k_re * im + k_im * re], axis=0)
        hi, mid, lo = bf16_pieces(product, 3)
        upper, lower = jnp.concatenate([hi, mid], axis=1), jnp.concatenate([hi, lo], axis=1)
        inner = dot(upper, first[0]) + dot(upper, first[1]) + dot(lower, first[2])
        a, c, d, b = inner[:half, :half], inner[:half, half:], inner[half:, :half], inner[half:, half:]
        for slot, y in zip(pair, ((a - b, a + b), (c + d, d - c))):
            for side, part in enumerate(y):
                at_side = slice(side * half, (side + 1) * half)
                hi, mid, lo = bf16_pieces(part, 3)
                slot[0, :half, at_side] = hi
                slot[0, half:, at_side] = mid
                slot[1, :half, at_side] = hi
                slot[1, half:, at_side] = lo

    def outward(pair, weight):
        of_re, of_im = (
            dot(second[0], slot[0]) + dot(second[1], slot[0]) + dot(second[2], slot[1]) for slot in pair
        )
        a, c, d, b = of_re[:half], of_re[half:], of_im[:half], of_im[half:]
        p_re, p_im, m_re, m_im = a - b, c + d, a + b, d - c
        plus[...] += weight * (p_re * p_re + p_im * p_im)
        minus[...] += weight * (m_re * m_re + m_im * m_im)

    last = spectra.shape[0] - 1
    inward(0, slots[0], 0)
    inward(1, slots[1], 0)

    @pl.loop(0, spectra.shape[0] // 2)
    def _(i):
        k = 2 * i
        following = jnp.minimum(k + 2, last)
        outward(slots[0], my_weights[pl.ds(k, 1), :])
        inward(0, slots[2], k + 1)
        outward(slots[1], other_weights[pl.ds(k, 1), :])
        inward(1, slots[3], k + 1)
        outward(slots[2], my_weights[pl.ds(k + 1, 1), :])
        inward(0, slots[0], following)
        outward(slots[3], other_weights[pl.ds(k + 1, 1), :])
        inward(1, slots[1], following)

    hi, mid, lo = bf16_pieces(minus[...], 3)
    turned = dot(flip_rows[...], jnp.concatenate([hi, mid], axis=0)) + dot(flip_rows[:, :half], lo)
    both = jnp.concatenate([turned, plus[...]], axis=0)
    hi, mid, lo = bf16_pieces(both[:, half:], 3)
    turned = dot(jnp.concatenate([hi, mid], axis=1), flip_cols[...]) + dot(lo, flip_cols[:half])
    picture = jnp.concatenate([turned, both[:, :half]], axis=1)
    image[...] = picture
    grad_rows = (pltpu.roll(picture, tile - 1, 0) - pltpu.roll(picture, 1, 0)) * 0.5
    grad_cols = (pltpu.roll(picture, tile - 1, 1) - pltpu.roll(picture, 1, 1)) * 0.5
    slope = jnp.sqrt(grad_rows * grad_rows + grad_cols * grad_cols)
    field = (picture - LEVEL) / jnp.maximum(slope, SLOPE_FLOOR)
    field_hi, field_lo = bf16_pieces(field, 2)

    def to_other(source, target, number):
        return pltpu.make_async_remote_copy(
            src_ref=source, dst_ref=target, send_sem=near_send.at[n_near + number],
            recv_sem=near_recv.at[n_near + number], device_id={"ka": 1 - ka}, device_id_type=MESH,
        )

    send_image = to_other(image, image_in, 0)
    send_errors = to_other(errors, errors_in, 1)
    send_image.start()

    for chunk in range(chunks):
        at = slice(chunk * tile, (chunk + 1) * tile)
        sampled = dot(field_hi, wanted[:, at]) + dot(field_lo, wanted[:, at])
        sampled = jnp.where(place_at == sites[1, 0, :, at], sampled, 0.0)
        errors[:, at] = jnp.sum(sampled, axis=0, keepdims=True)

    found = errors[...]
    size = jnp.abs(found)
    limit = limits[ka].astype(jnp.float32) / 8.0
    peak = jnp.max(size, axis=1, keepdims=True)
    total = jnp.sum(1.0 / (1.0 + jnp.exp(SHARPNESS * (size - limit))), axis=1, keepdims=True)
    lane = lax.broadcasted_iota(jnp.int32, (1, 128), 1)
    is_peak = lane < 64
    near[place] = jnp.where(is_peak, peak, total)

    def small(buffer, mine, d, peer, send, recv):
        return pltpu.make_async_remote_copy(
            src_ref=buffer.at[mine], dst_ref=buffer.at[mine], send_sem=send.at[d], recv_sem=recv.at[mine],
            device_id=peer, device_id_type=MESH,
        )

    def swapped(buffer, mine, peers, send, recv):
        copies = [small(buffer, mine, d, peer, send, recv) for d, (_, peer) in peers]
        for copy in copies:
            copy.start()
        for d, (spot, peer) in peers:
            small(buffer, spot, d, peer, send, recv).wait_recv()
        return copies

    near_peers = [(d, near_peer(d)) for d in range(1, n_near)]

    @pl.when(n_below < len(far_spots))
    def _():
        pl.semaphore_wait(ready, len(far_spots) - n_below)

    copies = swapped(near, place, near_peers, near_send, near_recv)
    of_iteration = []
    for t in range(n_ka):
        found_t = [near[y * n_ka + t] for y in range(n_ty)]
        of_iteration.append(
            jnp.where(is_peak, functools.reduce(jnp.maximum, found_t), functools.reduce(jnp.add, found_t))
        )
    far[tx] = jnp.where((lane & 32) == 0, of_iteration[0], of_iteration[1])
    far_copies = [small(far, tx, i, {"tx": spot}, far_send, far_recv) for i, spot in enumerate(far_spots)]
    for copy in far_copies:
        copy.start()
    send_errors.start()
    send_image.wait()
    send_errors.wait()
    image_out[...] = jnp.where(ka == ITERS - 1, image[...], image_in[...])
    errors_out[0, 0, 0:1, :] = jnp.where(ka == 0, errors[...], errors_in[...])
    errors_out[0, 0, 1:2, :] = jnp.where(ka == 0, errors_in[...], errors[...])
    saves[1].start()
    saves[2].start()
    pl.when(has_up)(to_up.wait_send)
    pl.when(has_down)(to_down.wait_send)
    pl.when(has_left)(to_left.wait_send)
    pl.when(has_right)(to_right.wait_send)
    for copy in copies:
        copy.wait_send()

    def combined(spots):
        held = [far[spot] for spot in spots]
        return jnp.where(is_peak, functools.reduce(jnp.maximum, held), functools.reduce(jnp.add, held))

    def arrived_from(i):
        small(far, far_spots[i], i, {"tx": far_spots[i]}, far_send, far_recv).wait_recv()

    def relayed(side, spot):
        return pltpu.make_async_remote_copy(
            src_ref=relay_out.at[side], dst_ref=relay_in.at[side], send_sem=relay_send.at[side],
            recv_sem=relay_recv.at[side], device_id={"tx": spot}, device_id_type=MESH,
        )

    for i in range(reach + 1, 2 * reach):
        arrived_from(i)
    relays = []
    if reach > 1:
        relay_out[0] = combined(far_spots[reach + 1 :])
        relays.append(relayed(0, far_spots[reach - 1]))
        relays[0].start()
    for i in range(reach):
        arrived_from(i)
    relay_out[1] = combined(far_spots[:reach])
    relays.append(relayed(1, far_spots[reach]))
    relays[-1].start()
    arrived_from(reach)
    whole = [combined([*far_spots, tx])]
    for copy in relays:
        copy.wait_recv()
    for side in ((0, 1) if reach > 1 else (1,)):
        whole.append(relay_in[side])
    stats_out[...] = jnp.where(is_peak, functools.reduce(jnp.maximum, whole), functools.reduce(jnp.add, whole))
    saves[3].start()
    for copy in far_copies + relays:
        copy.wait_send()
    for save in saves:
        save.wait()


def deliver_kernel(
    n_sites, image, mask, errors, stats, intensity, new_mask, edge_errors, peaks, shares,
    image_at, mask_at, errors_at, stats_at, peaks_at, shares_at, sem,
):
    held = ((stats, stats_at, None), (image, image_at, intensity), (mask, mask_at, new_mask), (errors, errors_at, edge_errors))
    loads = [pltpu.make_async_copy(src, at, sem.at[0, i]) for i, (src, at, _) in enumerate(held)]
    copies = [pltpu.make_async_copy(at, dst, sem.at[1, i]) for i, (_, at, dst) in enumerate(held) if i > 0]
    for load in loads:
        load.start()
    loads[0].wait()
    final = stats_at[...]
    for t in range(ITERS):
        peaks_at[t] = final[0, 32 * t]
        shares_at[t] = final[0, 64 + 32 * t] * (1.0 / n_sites)
    pairs = ((peaks_at, peaks), (shares_at, shares))
    copies += [pltpu.make_async_copy(at, dst, sem.at[1, 4 * i]) for i, (at, dst) in enumerate(pairs)]
    for copy in copies[3:]:
        copy.start()
    for load, copy in zip(loads[1:], copies):
        load.wait()
        copy.start()
    for copy in copies:
        copy.wait()


def shards(
    mask_raster, frag_rows, frag_cols, frag_length, frag_orient, frag_moves,
    site_rows, site_cols, spectra, weights, tolerance,
):
    f32, i32, bf16 = jnp.float32, jnp.int32, jnp.bfloat16
    tile = mask_raster.shape[0]
    half = tile // 2
    n_sites = site_rows.shape[2]
    kernels = spectra.shape[0]
    n_near = lax.axis_size("ty") * lax.axis_size("ka")
    n_tx = lax.axis_size("tx")
    constants = [jnp.asarray(t) for t in tables(tile)]
    hbm = pl.BlockSpec(memory_space=pltpu.HBM)
    dma = pltpu.SemaphoreType.DMA
    errors_shape = jax.ShapeDtypeStruct((1, 1, ITERS, n_sites), f32)
    square = jax.ShapeDtypeStruct((tile, tile), f32)
    V = pltpu.VMEM
    new_mask, image, errors, stats = pl.pallas_call(
        opc_kernel,
        name="opc_kernel",
        out_shape=(square, square, errors_shape, jax.ShapeDtypeStruct((1, 128), f32)),
        in_specs=[hbm] * 18,
        out_specs=(hbm,) * 4,
        scratch_shapes=[
            V((tile, tile), f32), V((4, *frag_rows.shape), i32), V(frag_moves.shape, i32),
            V((2, *site_rows.shape), i32), V((2, *spectra.shape), f32), V((kernels, tile), f32),
            V((kernels, tile), f32), pltpu.SMEM(weights.shape, f32), pltpu.SMEM(tolerance.shape, i32),
            *(V(c.shape, c.dtype) for c in constants),
            V((2 * HALO, tile), f32), V((PACKED, tile), f32), V((PACKED, 2 * HALO), f32), V((PACKED, 2 * BAND), f32),
            V((BAND, BAND), f32), V((BAND, BAND), f32),
            V((tile, n_sites), bf16),
            V((half, tile), f32), V((half, tile), f32), V((tile, tile), f32), V((tile, tile), f32),
            V((1, n_sites), f32), V((1, n_sites), f32), V((n_near, 1, 128), f32), V((n_tx, 1, 128), f32),
            V((tile, tile), f32), V((tile, tile), f32), V(errors_shape.shape, f32), V((1, 128), f32),
            *([V((2, tile, tile), bf16)] * 8), dma((18,)), dma((4,)), dma((6,)), dma((6,)), dma((n_near + 2,)), dma((n_near + 2,)), dma((n_tx,)), dma((n_tx,)),
            V((2, 1, 128), f32), V((2, 1, 128), f32), dma((2,)), dma((2,)),
            pltpu.SemaphoreType.REGULAR,
        ],
        compiler_params=pltpu.CompilerParams(collective_id=0, has_side_effects=True),
        cost_estimate=pl.CostEstimate(flops=4 * 10**9, bytes_accessed=4 * 10**6, transcendentals=0),
    )(
        mask_raster, frag_rows, frag_cols, frag_length, frag_orient, frag_moves, site_rows, site_cols,
        spectra, weights, tolerance, *constants,
    )
    pair = jax.ShapeDtypeStruct((ITERS,), f32)
    return pl.pallas_call(
        functools.partial(deliver_kernel, float(n_sites * n_tx * lax.axis_size("ty"))),
        name="deliver_kernel",
        out_shape=(square, square, errors_shape, pair, pair),
        in_specs=[hbm] * 4,
        out_specs=(hbm,) * 5,
        scratch_shapes=[
            V((tile, tile), f32), V((tile, tile), f32), V(errors_shape.shape, f32), V((1, 128), f32),
            pltpu.SMEM((ITERS,), f32), pltpu.SMEM((ITERS,), f32), dma((2, 5)),
        ],
    )(image, new_mask, errors, stats)


def solution(mesh):
    placed = (
        P(("groups", "tx"), "ty"),
        P(("groups", "tx"), "ty", None),
        P(("groups", "tx"), "ty", None),
        P(("groups", "tx"), "ty", None),
        P(("groups", "tx"), "ty", None),
        P(("groups", "tx"), "ty", None, None),
        P(("groups", "tx"), "ty", None),
        P(("groups", "tx"), "ty", None),
        P("ka", None, None, None),
        P("ka"),
        P(),
    )
    return jax.shard_map(
        shards,
        mesh=mesh,
        in_specs=placed,
        out_specs=(
            P(("groups", "tx"), "ty"),
            P(("groups", "tx"), "ty"),
            P(("groups", "tx"), "ty", None, None),
            P("groups"),
            P("groups"),
        ),
        check_vma=False,
    )
```

```python
import functools
import math

import jax
import jax.numpy as jnp
import numpy as np
from jax import lax
from jax.experimental import pallas as pl
from jax.experimental.pallas import tpu as pltpu
from jax.sharding import PartitionSpec as P

HALO = 128
BAND = 128
ITERS = 2
LEVEL = 0.4
SLOPE_FLOOR = 0.05
SHARPNESS = 8.0
MESH = pl.DeviceIdType.MESH
SIN_AT = 72
PACKED = 144


def bf16_pieces(x, count):
    pieces = []
    for _ in range(count):
        pieces.append(x.astype(jnp.bfloat16))
        x = x - pieces[-1].astype(jnp.float32)
    return pieces


def host_pieces(x):
    pieces = []
    for _ in range(3):
        pieces.append(x.astype(jnp.bfloat16))
        x = x - pieces[-1].astype(np.float64)
    return pieces


def tables(tile):
    ext = tile + 2 * HALO
    half = tile // 2
    theta = 2.0 * math.pi / ext
    inside = np.arange(ext) - (ext - 1) / 2
    low = BAND // 2
    order = np.roll(np.arange(ext), -HALO)
    order = np.concatenate([order[:tile], order[-HALO:], order[tile:-HALO]])
    inside = inside[order]
    rows = np.zeros((PACKED, ext))
    rows[: low + 1] = np.cos(theta * np.outer(np.arange(low + 1), inside))
    rows[SIN_AT : SIN_AT + low] = np.sin(theta * np.outer(np.arange(1, low + 1), inside))
    rows = np.concatenate(host_pieces(rows), axis=0)
    rows = np.stack([rows[:, :tile], rows[:, tile:]])
    freq = np.arange(BAND) - low
    turns = theta * np.outer(inside, freq)
    cols = np.stack(host_pieces(np.concatenate([np.cos(turns), np.sin(turns)], axis=1)))
    cols = np.stack([cols[:, :tile], cols[:, tile:]])
    expand = np.zeros((2 * BAND, PACKED))
    for u, f in enumerate(freq):
        expand[u, abs(f)] = 1.0
        if f != 0:
            expand[BAND + u, SIN_AT + abs(f) - 1] = np.sign(f)
    out = theta * np.outer(freq, np.arange(half) + 0.5)
    basis = np.concatenate([np.cos(out), np.sin(out)], axis=1)
    hi, mid, lo = host_pieces(basis)
    first = np.stack([np.concatenate(b, axis=0) for b in ((hi, hi), (mid, mid), (lo, hi))])
    second = np.ascontiguousarray(first.swapaxes(1, 2))
    flip = np.eye(half)[::-1]
    flip = np.concatenate([flip, flip], axis=1)
    bf16 = jnp.bfloat16
    return rows, cols, expand.astype(bf16), first, second, flip.astype(bf16), flip.T.astype(bf16)


def dot(left, right):
    return jnp.dot(left, right, preferred_element_type=jnp.float32)


def pieces_sum(of_hi, of_mid, of_lo):
    n = of_lo.shape[0]
    return of_hi[:n] + ((of_mid[:n] + of_hi[n : 2 * n]) + ((of_lo + of_hi[2 * n :]) + of_mid[n:]))


def rows_product(table, x):
    n = PACKED
    hi, mid, lo = bf16_pieces(x, 3)
    return pieces_sum(dot(table[...], hi), dot(table[: 2 * n], mid), dot(table[:n], lo))


def cols_product(x, table):
    n = PACKED
    pieces = jnp.concatenate(bf16_pieces(x, 3), axis=0)
    return pieces_sum(dot(pieces, table[0]), dot(pieces[: 2 * n], table[1]), dot(pieces[:n], table[2]))


def opc_kernel(
    mask, rows_at, cols_at, lengths, orients, moves, site_rows, site_cols, spectra, weights, tolerance,
    row_dft_in, col_dft_in, expand_in, first_in, second_in, flip_rows_in, flip_cols_in,
    new_mask, intensity, edge_errors, stats,
    current, fragments, frag_moves, sites, kernels, my_weights, other_weights, weight_of, limits,
    row_dft, col_dft, expand, first, second, flip_rows, flip_cols,
    halo_rows, packed, halo_cols, sums, spec_re, spec_im, wanted,
    plus, minus, image, image_in, errors, errors_in, near, far, mask_out, image_out, errors_out, stats_out,
    slot_a, slot_b, slot_c, slot_d, slot_e, slot_f, slot_g, slot_h, load_sem, save_sem, halo_send, halo_recv, near_send, near_recv, far_send, far_recv, relay_out, relay_in, relay_send, relay_recv, ready,
):
    tx, ty, ka = lax.axis_index("tx"), lax.axis_index("ty"), lax.axis_index("ka")
    n_tx, n_ty, n_ka = lax.axis_size("tx"), lax.axis_size("ty"), lax.axis_size("ka")
    n_near = n_ty * n_ka
    place = ty * n_ka + ka
    tile = mask.shape[0]
    ext = tile + 2 * HALO
    half = tile // 2
    slots = ((slot_a, slot_b), (slot_c, slot_d), (slot_e, slot_f), (slot_g, slot_h))
    has_up, has_down = tx > 0, tx < n_tx - 1
    has_left, has_right = ty > 0, ty < n_ty - 1

    pairs = [
        (mask, current), (rows_at, fragments.at[0]), (cols_at, fragments.at[1]), (lengths, fragments.at[2]),
        (orients, fragments.at[3]), (moves, frag_moves), (weights, weight_of), (row_dft_in, row_dft),
        (site_cols, sites.at[0]), (col_dft_in, col_dft), (expand_in, expand), (spectra, kernels.at[0]),
        (first_in, first), (second_in, second), (flip_rows_in, flip_rows), (flip_cols_in, flip_cols),
        (site_rows, sites.at[1]), (tolerance, limits),
    ]
    loads = [pltpu.make_async_copy(src, dst, load_sem.at[i]) for i, (src, dst) in enumerate(pairs)]
    for load in loads:
        load.start()

    def near_peer(d):
        spot = lax.rem(place + d, n_near)
        return spot, {"ty": spot // n_ka, "ka": lax.rem(spot, n_ka)}

    quarter = n_tx // 4
    extra = max(quarter // 2, 1)
    reach = 2 * quarter - extra
    far_spots = [lax.rem(tx + d, n_tx) for d in (*range(1, reach + 1), *range(n_tx - reach, n_tx))]
    below_me = [spot < tx for spot in far_spots]
    n_below = sum(lower.astype(jnp.int32) for lower in below_me)

    barrier = pltpu.get_barrier_semaphore()
    for d in range(1, n_near):
        pl.semaphore_signal(barrier, inc=1, device_id=near_peer(d)[1], device_id_type=MESH)

    @pl.when(has_up)
    def _():
        pl.semaphore_signal(barrier, inc=1, device_id={"tx": tx - 1}, device_id_type=MESH)

    for spot, lower in zip(far_spots, below_me):
        @pl.when(jnp.logical_not(lower))
        def _():
            pl.semaphore_signal(barrier, inc=1, device_id={"tx": spot}, device_id_type=MESH)

    for load in loads[:7]:
        load.wait()
    position = lax.broadcasted_iota(jnp.int32, (tile, rows_at.shape[2]), 0)
    row, col, length = fragments[0, 0], fragments[1, 0], fragments[2, 0]
    along = fragments[3, 0] == 0
    steps = [current[...]]
    for t in range(ITERS):
        move = frag_moves[0, 0, t : t + 1, :]
        lower, upper = jnp.minimum(move, 0), jnp.maximum(move, 0)
        row_low = jnp.where(along, row, row + lower)
        row_high = jnp.where(along, row + length, row + upper)
        col_low = jnp.where(along, col + lower, col)
        col_high = jnp.where(along, col + upper, col + length)
        sign = jnp.where(move > 0, 1.0, 0.0) - jnp.where(move < 0, 1.0, 0.0)
        in_rows = jnp.where((position >= row_low) & (position < row_high), sign, 0.0)
        in_cols = jnp.where((position >= col_low) & (position < col_high), 1.0, 0.0)
        strips = lax.dot_general(
            in_rows.astype(jnp.bfloat16), in_cols.astype(jnp.bfloat16), (((1,), (1,)), ((), ())),
            preferred_element_type=jnp.float32,
        )
        steps.append(jnp.clip(steps[-1] + strips, 0.0, 1.0))
    mask_out[...] = steps[2]
    current[...] = jnp.where(ka == 0, steps[1], steps[2])
    for k in range(my_weights.shape[0]):
        my_weights[pl.ds(k, 1), :] = jnp.full((1, my_weights.shape[1]), weight_of[k], jnp.float32)

    pl.semaphore_wait(barrier, n_near - 1 + n_below + has_down.astype(jnp.int32))

    def hop(source, target, number, device):
        return pltpu.make_async_remote_copy(
            src_ref=source, dst_ref=target, send_sem=halo_send.at[number], recv_sem=halo_recv.at[number],
            device_id=device, device_id_type=MESH,
        )

    above, below = halo_rows.at[pl.ds(0, HALO)], halo_rows.at[pl.ds(HALO, HALO)]
    left, right = halo_cols.at[:, pl.ds(0, HALO)], halo_cols.at[:, pl.ds(HALO, HALO)]
    to_up = hop(current.at[pl.ds(0, half)], below, 0, {"tx": tx - 1})
    to_down = hop(current.at[pl.ds(half, half)], above, 1, {"tx": tx + 1})
    to_left = hop(packed.at[:, pl.ds(0, half)], right, 2, {"ty": ty - 1})
    to_right = hop(packed.at[:, pl.ds(half, half)], left, 3, {"ty": ty + 1})
    swap_weights = hop(my_weights, other_weights, 4, {"ka": 1 - ka})
    swap_spectra = hop(spectra, kernels.at[1], 5, {"ka": 1 - ka})
    pl.when(has_up)(to_up.start)
    pl.when(has_down)(to_down.start)
    swap_spectra.start()
    swap_weights.start()
    pairs = ((mask_out, new_mask), (image_out, intensity), (errors_out, edge_errors), (stats_out, stats))
    saves = [pltpu.make_async_copy(src, dst, save_sem.at[i]) for i, (src, dst) in enumerate(pairs)]
    saves[0].start()
    for spot, lower in zip(far_spots, below_me):
        @pl.when(lower)
        def _():
            pl.semaphore_signal(ready, inc=1, device_id={"tx": spot}, device_id_type=MESH)

    def arrived(there, copy, buffer):
        pl.when(there)(copy.wait_recv)

        @pl.when(jnp.logical_not(there))
        def _():
            buffer[...] = jnp.zeros_like(buffer)

    loads[7].wait()
    packed[...] = rows_product(row_dft.at[0], current[...])
    loads[8].wait()
    place_at = lax.broadcasted_iota(jnp.int32, (tile, tile), 0)
    chunks = site_rows.shape[2] // tile
    for chunk in range(chunks):
        at = slice(chunk * tile, (chunk + 1) * tile)
        wanted[:, at] = jnp.where(place_at == sites[0, 0, :, at], 1.0, 0.0).astype(jnp.bfloat16)
    for load in loads[9:]:
        load.wait()
    arrived(has_up, to_down, above)
    arrived(has_down, to_up, below)
    packed[...] += rows_product(row_dft.at[1], halo_rows[...])
    pl.when(has_left)(to_left.start)
    pl.when(has_right)(to_right.start)
    sums[...] = cols_product(packed[...], col_dft.at[0])
    plus[...] = jnp.zeros_like(plus)
    minus[...] = jnp.zeros_like(minus)
    swap_weights.wait()
    swap_spectra.wait()
    arrived(has_left, to_right, left)
    arrived(has_right, to_left, right)
    total = sums[...] + cols_product(halo_cols[...], col_dft.at[1])
    full = sum(dot(expand[...], piece) for piece in bf16_pieces(total, 3))
    scale = 1.0 / (ext * ext)
    spec_re[...] = (full[:BAND, :BAND] - full[BAND:, BAND:]) * scale
    spec_im[...] = (full[BAND:, :BAND] + full[:BAND, BAND:]) * -scale

    def inward(at, pair, k):
        k_re, k_im = kernels[at, k, 0], kernels[at, k, 1]
        re, im = spec_re[...], spec_im[...]
        product = jnp.concatenate([k_re * re - k_im * im, k_re * im + k_im * re], axis=0)
        hi, mid, lo = bf16_pieces(product, 3)
        upper, lower = jnp.concatenate([hi, mid], axis=1), jnp.concatenate([hi, lo], axis=1)
        inner = dot(upper, first[0]) + dot(upper, first[1]) + dot(lower, first[2])
        a, c, d, b = inner[:half, :half], inner[:half, half:], inner[half:, :half], inner[half:, half:]
        for slot, y in zip(pair, ((a - b, a + b), (c + d, d - c))):
            for side, part in enumerate(y):
                at_side = slice(side * half, (side + 1) * half)
                hi, mid, lo = bf16_pieces(part, 3)
                slot[0, :half, at_side] = hi
                slot[0, half:, at_side] = mid
                slot[1, :half, at_side] = hi
                slot[1, half:, at_side] = lo

    def outward(pair, weight):
        of_re, of_im = (
            dot(second[0], slot[0]) + dot(second[1], slot[0]) + dot(second[2], slot[1]) for slot in pair
        )
        a, c, d, b = of_re[:half], of_re[half:], of_im[:half], of_im[half:]
        p_re, p_im, m_re, m_im = a - b, c + d, a + b, d - c
        plus[...] += weight * (p_re * p_re + p_im * p_im)
        minus[...] += weight * (m_re * m_re + m_im * m_im)

    last = spectra.shape[0] - 1
    inward(0, slots[0], 0)
    inward(1, slots[1], 0)

    @pl.loop(0, spectra.shape[0] // 2)
    def _(i):
        k = 2 * i
        following = jnp.minimum(k + 2, last)
        outward(slots[0], my_weights[pl.ds(k, 1), :])
        inward(0, slots[2], k + 1)
        outward(slots[1], other_weights[pl.ds(k, 1), :])
        inward(1, slots[3], k + 1)
        outward(slots[2], my_weights[pl.ds(k + 1, 1), :])
        inward(0, slots[0], following)
        outward(slots[3], other_weights[pl.ds(k + 1, 1), :])
        inward(1, slots[1], following)

    hi, mid, lo = bf16_pieces(minus[...], 3)
    turned = dot(flip_rows[...], jnp.concatenate([hi, mid], axis=0)) + dot(flip_rows[:, :half], lo)
    both = jnp.concatenate([turned, plus[...]], axis=0)
    hi, mid, lo = bf16_pieces(both[:, half:], 3)
    turned = dot(jnp.concatenate([hi, mid], axis=1), flip_cols[...]) + dot(lo, flip_cols[:half])
    picture = jnp.concatenate([turned, both[:, :half]], axis=1)
    image[...] = picture
    grad_rows = (pltpu.roll(picture, tile - 1, 0) - pltpu.roll(picture, 1, 0)) * 0.5
    grad_cols = (pltpu.roll(picture, tile - 1, 1) - pltpu.roll(picture, 1, 1)) * 0.5
    slope = jnp.sqrt(grad_rows * grad_rows + grad_cols * grad_cols)
    field = (picture - LEVEL) / jnp.maximum(slope, SLOPE_FLOOR)
    field_hi, field_lo = bf16_pieces(field, 2)

    def to_other(source, target, number):
        return pltpu.make_async_remote_copy(
            src_ref=source, dst_ref=target, send_sem=near_send.at[n_near + number],
            recv_sem=near_recv.at[n_near + number], device_id={"ka": 1 - ka}, device_id_type=MESH,
        )

    send_image = to_other(image, image_in, 0)
    send_errors = to_other(errors, errors_in, 1)
    send_image.start()

    for chunk in range(chunks):
        at = slice(chunk * tile, (chunk + 1) * tile)
        sampled = dot(field_hi, wanted[:, at]) + dot(field_lo, wanted[:, at])
        sampled = jnp.where(place_at == sites[1, 0, :, at], sampled, 0.0)
        errors[:, at] = jnp.sum(sampled, axis=0, keepdims=True)

    found = errors[...]
    size = jnp.abs(found)
    limit = limits[ka].astype(jnp.float32) / 8.0
    peak = jnp.max(size, axis=1, keepdims=True)
    total = jnp.sum(1.0 / (1.0 + jnp.exp(SHARPNESS * (size - limit))), axis=1, keepdims=True)
    lane = lax.broadcasted_iota(jnp.int32, (1, 128), 1)
    is_peak = lane < 64
    near[place] = jnp.where(is_peak, peak, total)

    def small(buffer, mine, d, peer, send, recv):
        return pltpu.make_async_remote_copy(
            src_ref=buffer.at[mine], dst_ref=buffer.at[mine], send_sem=send.at[d], recv_sem=recv.at[mine],
            device_id=peer, device_id_type=MESH,
        )

    def swapped(buffer, mine, peers, send, recv):
        copies = [small(buffer, mine, d, peer, send, recv) for d, (_, peer) in peers]
        for copy in copies:
            copy.start()
        for d, (spot, peer) in peers:
            small(buffer, spot, d, peer, send, recv).wait_recv()
        return copies

    near_peers = [(d, near_peer(d)) for d in range(1, n_near)]

    @pl.when(n_below < len(far_spots))
    def _():
        pl.semaphore_wait(ready, len(far_spots) - n_below)

    copies = swapped(near, place, near_peers, near_send, near_recv)
    of_iteration = []
    for t in range(n_ka):
        found_t = [near[y * n_ka + t] for y in range(n_ty)]
        of_iteration.append(
            jnp.where(is_peak, functools.reduce(jnp.maximum, found_t), functools.reduce(jnp.add, found_t))
        )
    far[tx] = jnp.where((lane & 32) == 0, of_iteration[0], of_iteration[1])
    far_copies = [small(far, tx, i, {"tx": spot}, far_send, far_recv) for i, spot in enumerate(far_spots)]
    for copy in far_copies:
        copy.start()
    send_errors.start()
    send_image.wait()
    send_errors.wait()
    image_out[...] = jnp.where(ka == ITERS - 1, image[...], image_in[...])
    errors_out[0, 0, 0:1, :] = jnp.where(ka == 0, errors[...], errors_in[...])
    errors_out[0, 0, 1:2, :] = jnp.where(ka == 0, errors_in[...], errors[...])
    saves[1].start()
    saves[2].start()
    pl.when(has_up)(to_up.wait_send)
    pl.when(has_down)(to_down.wait_send)
    pl.when(has_left)(to_left.wait_send)
    pl.when(has_right)(to_right.wait_send)
    for copy in copies:
        copy.wait_send()

    def combined(spots):
        held = [far[spot] for spot in spots]
        return jnp.where(is_peak, functools.reduce(jnp.maximum, held), functools.reduce(jnp.add, held))

    def arrived_from(i):
        small(far, far_spots[i], i, {"tx": far_spots[i]}, far_send, far_recv).wait_recv()

    def relayed(side, spot):
        return pltpu.make_async_remote_copy(
            src_ref=relay_out.at[side], dst_ref=relay_in.at[side], send_sem=relay_send.at[side],
            recv_sem=relay_recv.at[side], device_id={"tx": spot}, device_id_type=MESH,
        )

    from_above = list(range(quarter - extra, quarter))
    from_below = [2 * reach - d for d in range(quarter - extra + 1, quarter)]
    relays, sides = [], []
    for side, chosen, to in ((0, from_above, 2 * reach - quarter), (1, from_below, quarter - 1)):
        if chosen:
            for i in chosen:
                arrived_from(i)
            relay_out[side] = combined([far_spots[i] for i in chosen])
            relays.append(relayed(side, far_spots[to]))
            relays[-1].start()
            sides.append(side)
    for i in range(2 * reach):
        if i not in from_above + from_below:
            arrived_from(i)
    whole = [combined([*far_spots, tx])]
    for copy in relays:
        copy.wait_recv()
    for side in sides:
        whole.append(relay_in[side])
    stats_out[...] = jnp.where(is_peak, functools.reduce(jnp.maximum, whole), functools.reduce(jnp.add, whole))
    saves[3].start()
    for copy in far_copies + relays:
        copy.wait_send()
    for save in saves:
        save.wait()


def deliver_kernel(
    n_sites, image, mask, errors, stats, intensity, new_mask, edge_errors, peaks, shares,
    image_at, mask_at, errors_at, stats_at, peaks_at, shares_at, sem,
):
    held = ((stats, stats_at, None), (image, image_at, intensity), (mask, mask_at, new_mask), (errors, errors_at, edge_errors))
    loads = [pltpu.make_async_copy(src, at, sem.at[0, i]) for i, (src, at, _) in enumerate(held)]
    copies = [pltpu.make_async_copy(at, dst, sem.at[1, i]) for i, (_, at, dst) in enumerate(held) if i > 0]
    for load in loads:
        load.start()
    loads[0].wait()
    final = stats_at[...]
    for t in range(ITERS):
        peaks_at[t] = final[0, 32 * t]
        shares_at[t] = final[0, 64 + 32 * t] * (1.0 / n_sites)
    pairs = ((peaks_at, peaks), (shares_at, shares))
    copies += [pltpu.make_async_copy(at, dst, sem.at[1, 4 * i]) for i, (at, dst) in enumerate(pairs)]
    for copy in copies[3:]:
        copy.start()
    for load, copy in zip(loads[1:], copies):
        load.wait()
        copy.start()
    for copy in copies:
        copy.wait()


def shards(
    mask_raster, frag_rows, frag_cols, frag_length, frag_orient, frag_moves,
    site_rows, site_cols, spectra, weights, tolerance,
):
    f32, i32, bf16 = jnp.float32, jnp.int32, jnp.bfloat16
    tile = mask_raster.shape[0]
    half = tile // 2
    n_sites = site_rows.shape[2]
    kernels = spectra.shape[0]
    n_near = lax.axis_size("ty") * lax.axis_size("ka")
    n_tx = lax.axis_size("tx")
    constants = [jnp.asarray(t) for t in tables(tile)]
    hbm = pl.BlockSpec(memory_space=pltpu.HBM)
    dma = pltpu.SemaphoreType.DMA
    errors_shape = jax.ShapeDtypeStruct((1, 1, ITERS, n_sites), f32)
    square = jax.ShapeDtypeStruct((tile, tile), f32)
    V = pltpu.VMEM
    new_mask, image, errors, stats = pl.pallas_call(
        opc_kernel,
        name="opc_kernel",
        out_shape=(square, square, errors_shape, jax.ShapeDtypeStruct((1, 128), f32)),
        in_specs=[hbm] * 18,
        out_specs=(hbm,) * 4,
        scratch_shapes=[
            V((tile, tile), f32), V((4, *frag_rows.shape), i32), V(frag_moves.shape, i32),
            V((2, *site_rows.shape), i32), V((2, *spectra.shape), f32), V((kernels, tile), f32),
            V((kernels, tile), f32), pltpu.SMEM(weights.shape, f32), pltpu.SMEM(tolerance.shape, i32),
            *(V(c.shape, c.dtype) for c in constants),
            V((2 * HALO, tile), f32), V((PACKED, tile), f32), V((PACKED, 2 * HALO), f32), V((PACKED, 2 * BAND), f32),
            V((BAND, BAND), f32), V((BAND, BAND), f32),
            V((tile, n_sites), bf16),
            V((half, tile), f32), V((half, tile), f32), V((tile, tile), f32), V((tile, tile), f32),
            V((1, n_sites), f32), V((1, n_sites), f32), V((n_near, 1, 128), f32), V((n_tx, 1, 128), f32),
            V((tile, tile), f32), V((tile, tile), f32), V(errors_shape.shape, f32), V((1, 128), f32),
            *([V((2, tile, tile), bf16)] * 8), dma((18,)), dma((4,)), dma((6,)), dma((6,)), dma((n_near + 2,)), dma((n_near + 2,)), dma((n_tx,)), dma((n_tx,)),
            V((2, 1, 128), f32), V((2, 1, 128), f32), dma((2,)), dma((2,)),
            pltpu.SemaphoreType.REGULAR,
        ],
        compiler_params=pltpu.CompilerParams(collective_id=0, has_side_effects=True),
        cost_estimate=pl.CostEstimate(flops=4 * 10**9, bytes_accessed=4 * 10**6, transcendentals=0),
    )(
        mask_raster, frag_rows, frag_cols, frag_length, frag_orient, frag_moves, site_rows, site_cols,
        spectra, weights, tolerance, *constants,
    )
    pair = jax.ShapeDtypeStruct((ITERS,), f32)
    return pl.pallas_call(
        functools.partial(deliver_kernel, float(n_sites * n_tx * lax.axis_size("ty"))),
        name="deliver_kernel",
        out_shape=(square, square, errors_shape, pair, pair),
        in_specs=[hbm] * 4,
        out_specs=(hbm,) * 5,
        scratch_shapes=[
            V((tile, tile), f32), V((tile, tile), f32), V(errors_shape.shape, f32), V((1, 128), f32),
            pltpu.SMEM((ITERS,), f32), pltpu.SMEM((ITERS,), f32), dma((2, 5)),
        ],
    )(image, new_mask, errors, stats)


def solution(mesh):
    placed = (
        P(("groups", "tx"), "ty"),
        P(("groups", "tx"), "ty", None),
        P(("groups", "tx"), "ty", None),
        P(("groups", "tx"), "ty", None),
        P(("groups", "tx"), "ty", None),
        P(("groups", "tx"), "ty", None, None),
        P(("groups", "tx"), "ty", None),
        P(("groups", "tx"), "ty", None),
        P("ka", None, None, None),
        P("ka"),
        P(),
    )
    return jax.shard_map(
        shards,
        mesh=mesh,
        in_specs=placed,
        out_specs=(
            P(("groups", "tx"), "ty"),
            P(("groups", "tx"), "ty"),
            P(("groups", "tx"), "ty", None, None),
            P("groups"),
            P("groups"),
        ),
        check_vma=False,
    )
```

```python
import functools
import math

import jax
import jax.numpy as jnp
import numpy as np
from jax import lax
from jax.experimental import pallas as pl
from jax.experimental.pallas import tpu as pltpu
from jax.sharding import PartitionSpec as P

HALO = 128
BAND = 128
ITERS = 2
LEVEL = 0.4
SLOPE_FLOOR = 0.05
SHARPNESS = 8.0
MESH = pl.DeviceIdType.MESH
SIN_AT = 72
PACKED = 144


def bf16_pieces(x, count):
    pieces = []
    for _ in range(count):
        pieces.append(x.astype(jnp.bfloat16))
        x = x - pieces[-1].astype(jnp.float32)
    return pieces


def host_pieces(x):
    pieces = []
    for _ in range(3):
        pieces.append(x.astype(jnp.bfloat16))
        x = x - pieces[-1].astype(np.float64)
    return pieces


def tables(tile):
    ext = tile + 2 * HALO
    half = tile // 2
    theta = 2.0 * math.pi / ext
    inside = np.arange(ext) - (ext - 1) / 2
    low = BAND // 2
    order = np.roll(np.arange(ext), -HALO)
    order = np.concatenate([order[:tile], order[-HALO:], order[tile:-HALO]])
    inside = inside[order]
    rows = np.zeros((PACKED, ext))
    rows[: low + 1] = np.cos(theta * np.outer(np.arange(low + 1), inside))
    rows[SIN_AT : SIN_AT + low] = np.sin(theta * np.outer(np.arange(1, low + 1), inside))
    rows = np.concatenate(host_pieces(rows), axis=0)
    rows = np.stack([rows[:, :tile], rows[:, tile:]])
    freq = np.arange(BAND) - low
    turns = theta * np.outer(inside, freq)
    cols = np.stack(host_pieces(np.concatenate([np.cos(turns), np.sin(turns)], axis=1)))
    cols = np.stack([cols[:, :tile], cols[:, tile:]])
    expand = np.zeros((2 * BAND, PACKED))
    for u, f in enumerate(freq):
        expand[u, abs(f)] = 1.0
        if f != 0:
            expand[BAND + u, SIN_AT + abs(f) - 1] = np.sign(f)
    out = theta * np.outer(freq, np.arange(half) + 0.5)
    basis = np.concatenate([np.cos(out), np.sin(out)], axis=1)
    hi, mid, lo = host_pieces(basis)
    first = np.stack([np.concatenate(b, axis=0) for b in ((hi, hi), (mid, mid), (lo, hi))])
    second = np.ascontiguousarray(first.swapaxes(1, 2))
    flip = np.eye(half)[::-1]
    flip = np.concatenate([flip, flip], axis=1)
    bf16 = jnp.bfloat16
    return rows, cols, expand.astype(bf16), first, second, flip.astype(bf16), flip.T.astype(bf16)


def dot(left, right):
    return jnp.dot(left, right, preferred_element_type=jnp.float32)


def pieces_sum(of_hi, of_mid, of_lo):
    n = of_lo.shape[0]
    return of_hi[:n] + ((of_mid[:n] + of_hi[n : 2 * n]) + ((of_lo + of_hi[2 * n :]) + of_mid[n:]))


def rows_product(table, x):
    n = PACKED
    hi, mid, lo = bf16_pieces(x, 3)
    return pieces_sum(dot(table[...], hi), dot(table[: 2 * n], mid), dot(table[:n], lo))


def cols_product(x, table):
    n = PACKED
    pieces = jnp.concatenate(bf16_pieces(x, 3), axis=0)
    return pieces_sum(dot(pieces, table[0]), dot(pieces[: 2 * n], table[1]), dot(pieces[:n], table[2]))


def opc_kernel(
    mask, rows_at, cols_at, lengths, orients, moves, site_rows, site_cols, spectra, weights, tolerance,
    row_dft_in, col_dft_in, expand_in, first_in, second_in, flip_rows_in, flip_cols_in,
    new_mask, intensity, edge_errors, stats,
    current, fragments, frag_moves, sites, kernels, my_weights, other_weights, weight_of, limits,
    row_dft, col_dft, expand, first, second, flip_rows, flip_cols,
    halo_rows, packed, halo_cols, sums, spec_re, spec_im, wanted,
    plus, minus, image, image_in, errors, errors_in, near, far, mask_out, image_out, errors_out, stats_out,
    slot_a, slot_b, slot_c, slot_d, slot_e, slot_f, slot_g, slot_h, load_sem, save_sem, halo_send, halo_recv, near_send, near_recv, far_send, far_recv, relay_out, relay_in, relay_send, relay_recv, ready,
):
    tx, ty, ka = lax.axis_index("tx"), lax.axis_index("ty"), lax.axis_index("ka")
    n_tx, n_ty, n_ka = lax.axis_size("tx"), lax.axis_size("ty"), lax.axis_size("ka")
    n_near = n_ty * n_ka
    place = ty * n_ka + ka
    tile = mask.shape[0]
    ext = tile + 2 * HALO
    half = tile // 2
    slots = ((slot_a, slot_b), (slot_c, slot_d), (slot_e, slot_f), (slot_g, slot_h))
    has_up, has_down = tx > 0, tx < n_tx - 1
    has_left, has_right = ty > 0, ty < n_ty - 1

    pairs = [
        (mask, current), (rows_at, fragments.at[0]), (cols_at, fragments.at[1]), (lengths, fragments.at[2]),
        (orients, fragments.at[3]), (moves, frag_moves), (weights, weight_of), (row_dft_in, row_dft),
        (site_cols, sites.at[0]), (col_dft_in, col_dft), (expand_in, expand), (spectra, kernels.at[0]),
        (first_in, first), (second_in, second), (flip_rows_in, flip_rows), (flip_cols_in, flip_cols),
        (site_rows, sites.at[1]), (tolerance, limits),
    ]
    loads = [pltpu.make_async_copy(src, dst, load_sem.at[i]) for i, (src, dst) in enumerate(pairs)]
    for load in loads:
        load.start()

    def near_peer(d):
        spot = lax.rem(place + d, n_near)
        return spot, {"ty": spot // n_ka, "ka": lax.rem(spot, n_ka)}

    quarter = n_tx // 4
    extra = 1
    reach = 2 * quarter - extra
    far_spots = [lax.rem(tx + d, n_tx) for d in (*range(1, reach + 1), *range(n_tx - reach, n_tx))]
    below_me = [spot < tx for spot in far_spots]
    n_below = sum(lower.astype(jnp.int32) for lower in below_me)

    barrier = pltpu.get_barrier_semaphore()
    for d in range(1, n_near):
        pl.semaphore_signal(barrier, inc=1, device_id=near_peer(d)[1], device_id_type=MESH)

    @pl.when(has_up)
    def _():
        pl.semaphore_signal(barrier, inc=1, device_id={"tx": tx - 1}, device_id_type=MESH)

    for spot, lower in zip(far_spots, below_me):
        @pl.when(jnp.logical_not(lower))
        def _():
            pl.semaphore_signal(barrier, inc=1, device_id={"tx": spot}, device_id_type=MESH)

    for load in loads[:7]:
        load.wait()
    position = lax.broadcasted_iota(jnp.int32, (tile, rows_at.shape[2]), 0)
    row, col, length = fragments[0, 0], fragments[1, 0], fragments[2, 0]
    along = fragments[3, 0] == 0
    steps = [current[...]]
    for t in range(ITERS):
        move = frag_moves[0, 0, t : t + 1, :]
        lower, upper = jnp.minimum(move, 0), jnp.maximum(move, 0)
        row_low = jnp.where(along, row, row + lower)
        row_high = jnp.where(along, row + length, row + upper)
        col_low = jnp.where(along, col + lower, col)
        col_high = jnp.where(along, col + upper, col + length)
        sign = jnp.where(move > 0, 1.0, 0.0) - jnp.where(move < 0, 1.0, 0.0)
        in_rows = jnp.where((position >= row_low) & (position < row_high), sign, 0.0)
        in_cols = jnp.where((position >= col_low) & (position < col_high), 1.0, 0.0)
        strips = lax.dot_general(
            in_rows.astype(jnp.bfloat16), in_cols.astype(jnp.bfloat16), (((1,), (1,)), ((), ())),
            preferred_element_type=jnp.float32,
        )
        steps.append(jnp.clip(steps[-1] + strips, 0.0, 1.0))
    mask_out[...] = steps[2]
    current[...] = jnp.where(ka == 0, steps[1], steps[2])
    for k in range(my_weights.shape[0]):
        my_weights[pl.ds(k, 1), :] = jnp.full((1, my_weights.shape[1]), weight_of[k], jnp.float32)

    pl.semaphore_wait(barrier, n_near - 1 + n_below + has_down.astype(jnp.int32))

    def hop(source, target, number, device):
        return pltpu.make_async_remote_copy(
            src_ref=source, dst_ref=target, send_sem=halo_send.at[number], recv_sem=halo_recv.at[number],
            device_id=device, device_id_type=MESH,
        )

    above, below = halo_rows.at[pl.ds(0, HALO)], halo_rows.at[pl.ds(HALO, HALO)]
    left, right = halo_cols.at[:, pl.ds(0, HALO)], halo_cols.at[:, pl.ds(HALO, HALO)]
    to_up = hop(current.at[pl.ds(0, half)], below, 0, {"tx": tx - 1})
    to_down = hop(current.at[pl.ds(half, half)], above, 1, {"tx": tx + 1})
    to_left = hop(packed.at[:, pl.ds(0, half)], right, 2, {"ty": ty - 1})
    to_right = hop(packed.at[:, pl.ds(half, half)], left, 3, {"ty": ty + 1})
    swap_weights = hop(my_weights, other_weights, 4, {"ka": 1 - ka})
    swap_spectra = hop(spectra, kernels.at[1], 5, {"ka": 1 - ka})
    pl.when(has_up)(to_up.start)
    pl.when(has_down)(to_down.start)
    swap_spectra.start()
    swap_weights.start()
    pairs = ((mask_out, new_mask), (image_out, intensity), (errors_out, edge_errors), (stats_out, stats))
    saves = [pltpu.make_async_copy(src, dst, save_sem.at[i]) for i, (src, dst) in enumerate(pairs)]
    saves[0].start()
    for spot, lower in zip(far_spots, below_me):
        @pl.when(lower)
        def _():
            pl.semaphore_signal(ready, inc=1, device_id={"tx": spot}, device_id_type=MESH)

    def arrived(there, copy, buffer):
        pl.when(there)(copy.wait_recv)

        @pl.when(jnp.logical_not(there))
        def _():
            buffer[...] = jnp.zeros_like(buffer)

    loads[7].wait()
    packed[...] = rows_product(row_dft.at[0], current[...])
    loads[8].wait()
    place_at = lax.broadcasted_iota(jnp.int32, (tile, tile), 0)
    chunks = site_rows.shape[2] // tile
    for chunk in range(chunks):
        at = slice(chunk * tile, (chunk + 1) * tile)
        wanted[:, at] = jnp.where(place_at == sites[0, 0, :, at], 1.0, 0.0).astype(jnp.bfloat16)
    for load in loads[9:]:
        load.wait()
    arrived(has_up, to_down, above)
    arrived(has_down, to_up, below)
    packed[...] += rows_product(row_dft.at[1], halo_rows[...])
    pl.when(has_left)(to_left.start)
    pl.when(has_right)(to_right.start)
    sums[...] = cols_product(packed[...], col_dft.at[0])
    plus[...] = jnp.zeros_like(plus)
    minus[...] = jnp.zeros_like(minus)
    swap_weights.wait()
    swap_spectra.wait()
    arrived(has_left, to_right, left)
    arrived(has_right, to_left, right)
    total = sums[...] + cols_product(halo_cols[...], col_dft.at[1])
    full = sum(dot(expand[...], piece) for piece in bf16_pieces(total, 3))
    scale = 1.0 / (ext * ext)
    spec_re[...] = (full[:BAND, :BAND] - full[BAND:, BAND:]) * scale
    spec_im[...] = (full[BAND:, :BAND] + full[:BAND, BAND:]) * -scale

    def inward(at, pair, k):
        k_re, k_im = kernels[at, k, 0], kernels[at, k, 1]
        re, im = spec_re[...], spec_im[...]
        product = jnp.concatenate([k_re * re - k_im * im, k_re * im + k_im * re], axis=0)
        hi, mid, lo = bf16_pieces(product, 3)
        upper, lower = jnp.concatenate([hi, mid], axis=1), jnp.concatenate([hi, lo], axis=1)
        inner = dot(upper, first[0]) + dot(upper, first[1]) + dot(lower, first[2])
        a, c, d, b = inner[:half, :half], inner[:half, half:], inner[half:, :half], inner[half:, half:]
        for slot, y in zip(pair, ((a - b, a + b), (c + d, d - c))):
            for side, part in enumerate(y):
                at_side = slice(side * half, (side + 1) * half)
                hi, mid, lo = bf16_pieces(part, 3)
                slot[0, :half, at_side] = hi
                slot[0, half:, at_side] = mid
                slot[1, :half, at_side] = hi
                slot[1, half:, at_side] = lo

    def outward(pair, weight):
        of_re, of_im = (
            dot(second[0], slot[0]) + dot(second[1], slot[0]) + dot(second[2], slot[1]) for slot in pair
        )
        a, c, d, b = of_re[:half], of_re[half:], of_im[:half], of_im[half:]
        p_re, p_im, m_re, m_im = a - b, c + d, a + b, d - c
        plus[...] += weight * (p_re * p_re + p_im * p_im)
        minus[...] += weight * (m_re * m_re + m_im * m_im)

    last = spectra.shape[0] - 1
    inward(0, slots[0], 0)
    inward(1, slots[1], 0)

    @pl.loop(0, spectra.shape[0] // 2)
    def _(i):
        k = 2 * i
        following = jnp.minimum(k + 2, last)
        inward(0, slots[2], k + 1)
        outward(slots[0], my_weights[pl.ds(k, 1), :])
        inward(1, slots[3], k + 1)
        outward(slots[1], other_weights[pl.ds(k, 1), :])
        inward(0, slots[0], following)
        outward(slots[2], my_weights[pl.ds(k + 1, 1), :])
        inward(1, slots[1], following)
        outward(slots[3], other_weights[pl.ds(k + 1, 1), :])

    hi, mid, lo = bf16_pieces(minus[...], 3)
    turned = dot(flip_rows[...], jnp.concatenate([hi, mid], axis=0)) + dot(flip_rows[:, :half], lo)
    both = jnp.concatenate([turned, plus[...]], axis=0)
    hi, mid, lo = bf16_pieces(both[:, half:], 3)
    turned = dot(jnp.concatenate([hi, mid], axis=1), flip_cols[...]) + dot(lo, flip_cols[:half])
    picture = jnp.concatenate([turned, both[:, :half]], axis=1)
    image[...] = picture
    grad_rows = (pltpu.roll(picture, tile - 1, 0) - pltpu.roll(picture, 1, 0)) * 0.5
    grad_cols = (pltpu.roll(picture, tile - 1, 1) - pltpu.roll(picture, 1, 1)) * 0.5
    slope = jnp.sqrt(grad_rows * grad_rows + grad_cols * grad_cols)
    field = (picture - LEVEL) / jnp.maximum(slope, SLOPE_FLOOR)
    field_hi, field_lo = bf16_pieces(field, 2)

    def to_other(source, target, number):
        return pltpu.make_async_remote_copy(
            src_ref=source, dst_ref=target, send_sem=near_send.at[n_near + number],
            recv_sem=near_recv.at[n_near + number], device_id={"ka": 1 - ka}, device_id_type=MESH,
        )

    send_image = to_other(image, image_in, 0)
    send_errors = to_other(errors, errors_in, 1)
    send_image.start()

    for chunk in range(chunks):
        at = slice(chunk * tile, (chunk + 1) * tile)
        sampled = dot(field_hi, wanted[:, at]) + dot(field_lo, wanted[:, at])
        sampled = jnp.where(place_at == sites[1, 0, :, at], sampled, 0.0)
        errors[:, at] = jnp.sum(sampled, axis=0, keepdims=True)

    found = errors[...]
    size = jnp.abs(found)
    limit = limits[ka].astype(jnp.float32) / 8.0
    peak = jnp.max(size, axis=1, keepdims=True)
    total = jnp.sum(1.0 / (1.0 + jnp.exp(SHARPNESS * (size - limit))), axis=1, keepdims=True)
    lane = lax.broadcasted_iota(jnp.int32, (1, 128), 1)
    is_peak = lane < 64
    near[place] = jnp.where(is_peak, peak, total)

    def small(buffer, mine, d, peer, send, recv):
        return pltpu.make_async_remote_copy(
            src_ref=buffer.at[mine], dst_ref=buffer.at[mine], send_sem=send.at[d], recv_sem=recv.at[mine],
            device_id=peer, device_id_type=MESH,
        )

    def swapped(buffer, mine, peers, send, recv):
        copies = [small(buffer, mine, d, peer, send, recv) for d, (_, peer) in peers]
        for copy in copies:
            copy.start()
        for d, (spot, peer) in peers:
            small(buffer, spot, d, peer, send, recv).wait_recv()
        return copies

    near_peers = [(d, near_peer(d)) for d in range(1, n_near)]

    @pl.when(n_below < len(far_spots))
    def _():
        pl.semaphore_wait(ready, len(far_spots) - n_below)

    copies = swapped(near, place, near_peers, near_send, near_recv)
    of_iteration = []
    for t in range(n_ka):
        found_t = [near[y * n_ka + t] for y in range(n_ty)]
        of_iteration.append(
            jnp.where(is_peak, functools.reduce(jnp.maximum, found_t), functools.reduce(jnp.add, found_t))
        )
    far[tx] = jnp.where((lane & 32) == 0, of_iteration[0], of_iteration[1])
    far_copies = [small(far, tx, i, {"tx": spot}, far_send, far_recv) for i, spot in enumerate(far_spots)]
    for copy in far_copies:
        copy.start()
    send_errors.start()
    send_image.wait()
    send_errors.wait()
    image_out[...] = jnp.where(ka == ITERS - 1, image[...], image_in[...])
    errors_out[0, 0, 0:1, :] = jnp.where(ka == 0, errors[...], errors_in[...])
    errors_out[0, 0, 1:2, :] = jnp.where(ka == 0, errors_in[...], errors[...])
    saves[1].start()
    saves[2].start()
    pl.when(has_up)(to_up.wait_send)
    pl.when(has_down)(to_down.wait_send)
    pl.when(has_left)(to_left.wait_send)
    pl.when(has_right)(to_right.wait_send)
    for copy in copies:
        copy.wait_send()

    def combined(spots):
        held = [far[spot] for spot in spots]
        return jnp.where(is_peak, functools.reduce(jnp.maximum, held), functools.reduce(jnp.add, held))

    def arrived_from(i):
        small(far, far_spots[i], i, {"tx": far_spots[i]}, far_send, far_recv).wait_recv()

    def relayed(side, spot):
        return pltpu.make_async_remote_copy(
            src_ref=relay_out.at[side], dst_ref=relay_in.at[side], send_sem=relay_send.at[side],
            recv_sem=relay_recv.at[side], device_id={"tx": spot}, device_id_type=MESH,
        )

    from_above = list(range(quarter - extra, quarter))
    from_below = [2 * reach - d for d in range(quarter - extra + 1, quarter)]
    relays, sides = [], []
    for side, chosen, to in ((0, from_above, 2 * reach - quarter), (1, from_below, quarter - 1)):
        if chosen:
            for i in chosen:
                arrived_from(i)
            relay_out[side] = combined([far_spots[i] for i in chosen])
            relays.append(relayed(side, far_spots[to]))
            relays[-1].start()
            sides.append(side)
    for i in range(2 * reach):
        if i not in from_above + from_below:
            arrived_from(i)
    whole = [combined([*far_spots, tx])]
    for copy in relays:
        copy.wait_recv()
    for side in sides:
        whole.append(relay_in[side])
    stats_out[...] = jnp.where(is_peak, functools.reduce(jnp.maximum, whole), functools.reduce(jnp.add, whole))
    saves[3].start()
    for copy in far_copies + relays:
        copy.wait_send()
    for save in saves:
        save.wait()


def deliver_kernel(
    n_sites, image, mask, errors, stats, intensity, new_mask, edge_errors, peaks, shares,
    image_at, mask_at, errors_at, stats_at, peaks_at, shares_at, sem,
):
    held = ((stats, stats_at, None), (image, image_at, intensity), (mask, mask_at, new_mask), (errors, errors_at, edge_errors))
    loads = [pltpu.make_async_copy(src, at, sem.at[0, i]) for i, (src, at, _) in enumerate(held)]
    copies = [pltpu.make_async_copy(at, dst, sem.at[1, i]) for i, (_, at, dst) in enumerate(held) if i > 0]
    for load in loads:
        load.start()
    loads[0].wait()
    final = stats_at[...]
    for t in range(ITERS):
        peaks_at[t] = final[0, 32 * t]
        shares_at[t] = final[0, 64 + 32 * t] * (1.0 / n_sites)
    pairs = ((peaks_at, peaks), (shares_at, shares))
    copies += [pltpu.make_async_copy(at, dst, sem.at[1, 4 * i]) for i, (at, dst) in enumerate(pairs)]
    for copy in copies[3:]:
        copy.start()
    for load, copy in zip(loads[1:], copies):
        load.wait()
        copy.start()
    for copy in copies:
        copy.wait()


def shards(
    mask_raster, frag_rows, frag_cols, frag_length, frag_orient, frag_moves,
    site_rows, site_cols, spectra, weights, tolerance,
):
    f32, i32, bf16 = jnp.float32, jnp.int32, jnp.bfloat16
    tile = mask_raster.shape[0]
    half = tile // 2
    n_sites = site_rows.shape[2]
    kernels = spectra.shape[0]
    n_near = lax.axis_size("ty") * lax.axis_size("ka")
    n_tx = lax.axis_size("tx")
    constants = [jnp.asarray(t) for t in tables(tile)]
    hbm = pl.BlockSpec(memory_space=pltpu.HBM)
    dma = pltpu.SemaphoreType.DMA
    errors_shape = jax.ShapeDtypeStruct((1, 1, ITERS, n_sites), f32)
    square = jax.ShapeDtypeStruct((tile, tile), f32)
    V = pltpu.VMEM
    new_mask, image, errors, stats = pl.pallas_call(
        opc_kernel,
        name="opc_kernel",
        out_shape=(square, square, errors_shape, jax.ShapeDtypeStruct((1, 128), f32)),
        in_specs=[hbm] * 18,
        out_specs=(hbm,) * 4,
        scratch_shapes=[
            V((tile, tile), f32), V((4, *frag_rows.shape), i32), V(frag_moves.shape, i32),
            V((2, *site_rows.shape), i32), V((2, *spectra.shape), f32), V((kernels, tile), f32),
            V((kernels, tile), f32), pltpu.SMEM(weights.shape, f32), pltpu.SMEM(tolerance.shape, i32),
            *(V(c.shape, c.dtype) for c in constants),
            V((2 * HALO, tile), f32), V((PACKED, tile), f32), V((PACKED, 2 * HALO), f32), V((PACKED, 2 * BAND), f32),
            V((BAND, BAND), f32), V((BAND, BAND), f32),
            V((tile, n_sites), bf16),
            V((half, tile), f32), V((half, tile), f32), V((tile, tile), f32), V((tile, tile), f32),
            V((1, n_sites), f32), V((1, n_sites), f32), V((n_near, 1, 128), f32), V((n_tx, 1, 128), f32),
            V((tile, tile), f32), V((tile, tile), f32), V(errors_shape.shape, f32), V((1, 128), f32),
            *([V((2, tile, tile), bf16)] * 8), dma((18,)), dma((4,)), dma((6,)), dma((6,)), dma((n_near + 2,)), dma((n_near + 2,)), dma((n_tx,)), dma((n_tx,)),
            V((2, 1, 128), f32), V((2, 1, 128), f32), dma((2,)), dma((2,)),
            pltpu.SemaphoreType.REGULAR,
        ],
        compiler_params=pltpu.CompilerParams(collective_id=0, has_side_effects=True),
        cost_estimate=pl.CostEstimate(flops=4 * 10**9, bytes_accessed=4 * 10**6, transcendentals=0),
    )(
        mask_raster, frag_rows, frag_cols, frag_length, frag_orient, frag_moves, site_rows, site_cols,
        spectra, weights, tolerance, *constants,
    )
    pair = jax.ShapeDtypeStruct((ITERS,), f32)
    return pl.pallas_call(
        functools.partial(deliver_kernel, float(n_sites * n_tx * lax.axis_size("ty"))),
        name="deliver_kernel",
        out_shape=(square, square, errors_shape, pair, pair),
        in_specs=[hbm] * 4,
        out_specs=(hbm,) * 5,
        scratch_shapes=[
            V((tile, tile), f32), V((tile, tile), f32), V(errors_shape.shape, f32), V((1, 128), f32),
            pltpu.SMEM((ITERS,), f32), pltpu.SMEM((ITERS,), f32), dma((2, 5)),
        ],
    )(image, new_mask, errors, stats)


def solution(mesh):
    placed = (
        P(("groups", "tx"), "ty"),
        P(("groups", "tx"), "ty", None),
        P(("groups", "tx"), "ty", None),
        P(("groups", "tx"), "ty", None),
        P(("groups", "tx"), "ty", None),
        P(("groups", "tx"), "ty", None, None),
        P(("groups", "tx"), "ty", None),
        P(("groups", "tx"), "ty", None),
        P("ka", None, None, None),
        P("ka"),
        P(),
    )
    return jax.shard_map(
        shards,
        mesh=mesh,
        in_specs=placed,
        out_specs=(
            P(("groups", "tx"), "ty"),
            P(("groups", "tx"), "ty"),
            P(("groups", "tx"), "ty", None, None),
            P("groups"),
            P("groups"),
        ),
        check_vma=False,
    )
```

```python
import functools
import math

import jax
import jax.numpy as jnp
import numpy as np
from jax import lax
from jax.experimental import pallas as pl
from jax.experimental.pallas import tpu as pltpu
from jax.sharding import PartitionSpec as P

HALO = 128
BAND = 128
ITERS = 2
LEVEL = 0.4
SLOPE_FLOOR = 0.05
SHARPNESS = 8.0
MESH = pl.DeviceIdType.MESH
SIN_AT = 72
PACKED = 144


def bf16_pieces(x, count):
    pieces = []
    for _ in range(count):
        pieces.append(x.astype(jnp.bfloat16))
        x = x - pieces[-1].astype(jnp.float32)
    return pieces


def host_pieces(x):
    pieces = []
    for _ in range(3):
        pieces.append(x.astype(jnp.bfloat16))
        x = x - pieces[-1].astype(np.float64)
    return pieces


def tables(tile):
    ext = tile + 2 * HALO
    half = tile // 2
    theta = 2.0 * math.pi / ext
    inside = np.arange(ext) - (ext - 1) / 2
    low = BAND // 2
    order = np.roll(np.arange(ext), -HALO)
    order = np.concatenate([order[:tile], order[-HALO:], order[tile:-HALO]])
    inside = inside[order]
    rows = np.zeros((PACKED, ext))
    rows[: low + 1] = np.cos(theta * np.outer(np.arange(low + 1), inside))
    rows[SIN_AT : SIN_AT + low] = np.sin(theta * np.outer(np.arange(1, low + 1), inside))
    rows = np.concatenate(host_pieces(rows), axis=0)
    rows = np.stack([rows[:, :tile], rows[:, tile:]])
    freq = np.arange(BAND) - low
    turns = theta * np.outer(inside, freq)
    cols = np.stack(host_pieces(np.concatenate([np.cos(turns), np.sin(turns)], axis=1)))
    cols = np.stack([cols[:, :tile], cols[:, tile:]])
    expand = np.zeros((2 * BAND, PACKED))
    for u, f in enumerate(freq):
        expand[u, abs(f)] = 1.0
        if f != 0:
            expand[BAND + u, SIN_AT + abs(f) - 1] = np.sign(f)
    out = theta * np.outer(freq, np.arange(half) + 0.5)
    basis = np.concatenate([np.cos(out), np.sin(out)], axis=1)
    hi, mid, lo = host_pieces(basis)
    first = np.stack([np.concatenate(b, axis=0) for b in ((hi, hi), (mid, mid), (lo, hi))])
    second = np.ascontiguousarray(first.swapaxes(1, 2))
    flip = np.eye(half)[::-1]
    flip = np.concatenate([flip, flip], axis=1)
    bf16 = jnp.bfloat16
    return rows, cols, expand.astype(bf16), first, second, flip.astype(bf16), flip.T.astype(bf16)


def dot(left, right):
    return jnp.dot(left, right, preferred_element_type=jnp.float32)


def pieces_sum(of_hi, of_mid, of_lo):
    n = of_lo.shape[0]
    return of_hi[:n] + ((of_mid[:n] + of_hi[n : 2 * n]) + ((of_lo + of_hi[2 * n :]) + of_mid[n:]))


def rows_product(table, x):
    n = PACKED
    hi, mid, lo = bf16_pieces(x, 3)
    return pieces_sum(dot(table[...], hi), dot(table[: 2 * n], mid), dot(table[:n], lo))


def cols_product(x, table):
    n = PACKED
    pieces = jnp.concatenate(bf16_pieces(x, 3), axis=0)
    return pieces_sum(dot(pieces, table[0]), dot(pieces[: 2 * n], table[1]), dot(pieces[:n], table[2]))


def opc_kernel(
    mask, rows_at, cols_at, lengths, orients, moves, site_rows, site_cols, spectra, weights, tolerance,
    row_dft_in, col_dft_in, expand_in, first_in, second_in, flip_rows_in, flip_cols_in,
    new_mask, intensity, edge_errors, stats,
    current, fragments, frag_moves, sites, kernels, my_weights, other_weights, weight_of, limits,
    row_dft, col_dft, expand, first, second, flip_rows, flip_cols,
    halo_rows, packed, halo_cols, sums, spec_re, spec_im, wanted,
    plus, minus, image, image_in, errors, errors_in, near, far, mask_out, image_out, errors_out, stats_out,
    slot_a, slot_b, slot_c, slot_d, slot_e, slot_f, slot_g, slot_h, load_sem, save_sem, halo_send, halo_recv, near_send, near_recv, far_send, far_recv, ready,
):
    tx, ty, ka = lax.axis_index("tx"), lax.axis_index("ty"), lax.axis_index("ka")
    n_tx, n_ty, n_ka = lax.axis_size("tx"), lax.axis_size("ty"), lax.axis_size("ka")
    n_near = n_ty * n_ka
    place = ty * n_ka + ka
    tile = mask.shape[0]
    ext = tile + 2 * HALO
    half = tile // 2
    slots = ((slot_a, slot_b), (slot_c, slot_d), (slot_e, slot_f), (slot_g, slot_h))
    has_up, has_down = tx > 0, tx < n_tx - 1
    has_left, has_right = ty > 0, ty < n_ty - 1

    pairs = [
        (mask, current), (rows_at, fragments.at[0]), (cols_at, fragments.at[1]), (lengths, fragments.at[2]),
        (orients, fragments.at[3]), (moves, frag_moves), (weights, weight_of), (row_dft_in, row_dft),
        (site_cols, sites.at[0]), (col_dft_in, col_dft), (expand_in, expand), (spectra, kernels.at[0]),
        (first_in, first), (second_in, second), (flip_rows_in, flip_rows), (flip_cols_in, flip_cols),
        (site_rows, sites.at[1]), (tolerance, limits),
    ]
    loads = [pltpu.make_async_copy(src, dst, load_sem.at[i]) for i, (src, dst) in enumerate(pairs)]
    for load in loads:
        load.start()

    def near_peer(d):
        spot = lax.rem(place + d, n_near)
        return spot, {"ty": spot // n_ka, "ka": lax.rem(spot, n_ka)}

    def far_peer(d):
        spot = lax.rem(tx + d, n_tx)
        return spot, {"tx": spot}

    barrier = pltpu.get_barrier_semaphore()
    for d in range(1, n_near):
        pl.semaphore_signal(barrier, inc=1, device_id=near_peer(d)[1], device_id_type=MESH)

    @pl.when(has_up)
    def _():
        pl.semaphore_signal(barrier, inc=1, device_id={"tx": tx - 1}, device_id_type=MESH)

    for d in range(1, n_tx):
        @pl.when(tx + d < n_tx)
        def _():
            pl.semaphore_signal(barrier, inc=1, device_id={"tx": tx + d}, device_id_type=MESH)

    for load in loads[:7]:
        load.wait()
    position = lax.broadcasted_iota(jnp.int32, (tile, rows_at.shape[2]), 0)
    row, col, length = fragments[0, 0], fragments[1, 0], fragments[2, 0]
    along = fragments[3, 0] == 0
    steps = [current[...]]
    for t in range(ITERS):
        move = frag_moves[0, 0, t : t + 1, :]
        lower, upper = jnp.minimum(move, 0), jnp.maximum(move, 0)
        row_low = jnp.where(along, row, row + lower)
        row_high = jnp.where(along, row + length, row + upper)
        col_low = jnp.where(along, col + lower, col)
        col_high = jnp.where(along, col + upper, col + length)
        sign = jnp.where(move > 0, 1.0, 0.0) - jnp.where(move < 0, 1.0, 0.0)
        in_rows = jnp.where((position >= row_low) & (position < row_high), sign, 0.0)
        in_cols = jnp.where((position >= col_low) & (position < col_high), 1.0, 0.0)
        strips = lax.dot_general(
            in_rows.astype(jnp.bfloat16), in_cols.astype(jnp.bfloat16), (((1,), (1,)), ((), ())),
            preferred_element_type=jnp.float32,
        )
        steps.append(jnp.clip(steps[-1] + strips, 0.0, 1.0))
    mask_out[...] = steps[2]
    current[...] = jnp.where(ka == 0, steps[1], steps[2])
    for k in range(my_weights.shape[0]):
        my_weights[pl.ds(k, 1), :] = jnp.full((1, my_weights.shape[1]), weight_of[k], jnp.float32)

    pl.semaphore_wait(barrier, n_near - 1 + tx + has_down.astype(jnp.int32))

    def hop(source, target, number, device):
        return pltpu.make_async_remote_copy(
            src_ref=source, dst_ref=target, send_sem=halo_send.at[number], recv_sem=halo_recv.at[number],
            device_id=device, device_id_type=MESH,
        )

    above, below = halo_rows.at[pl.ds(0, HALO)], halo_rows.at[pl.ds(HALO, HALO)]
    left, right = halo_cols.at[:, pl.ds(0, HALO)], halo_cols.at[:, pl.ds(HALO, HALO)]
    to_up = hop(current.at[pl.ds(0, half)], below, 0, {"tx": tx - 1})
    to_down = hop(current.at[pl.ds(half, half)], above, 1, {"tx": tx + 1})
    to_left = hop(packed.at[:, pl.ds(0, half)], right, 2, {"ty": ty - 1})
    to_right = hop(packed.at[:, pl.ds(half, half)], left, 3, {"ty": ty + 1})
    swap_weights = hop(my_weights, other_weights, 4, {"ka": 1 - ka})
    swap_spectra = hop(spectra, kernels.at[1], 5, {"ka": 1 - ka})
    pl.when(has_up)(to_up.start)
    pl.when(has_down)(to_down.start)
    swap_spectra.start()
    swap_weights.start()
    pairs = ((mask_out, new_mask), (image_out, intensity), (errors_out, edge_errors), (stats_out, stats))
    saves = [pltpu.make_async_copy(src, dst, save_sem.at[i]) for i, (src, dst) in enumerate(pairs)]
    saves[0].start()
    for d in range(1, n_tx):
        @pl.when(tx - d >= 0)
        def _():
            pl.semaphore_signal(ready, inc=1, device_id={"tx": tx - d}, device_id_type=MESH)

    def arrived(there, copy, buffer):
        pl.when(there)(copy.wait_recv)

        @pl.when(jnp.logical_not(there))
        def _():
            buffer[...] = jnp.zeros_like(buffer)

    loads[7].wait()
    packed[...] = rows_product(row_dft.at[0], current[...])
    loads[8].wait()
    place_at = lax.broadcasted_iota(jnp.int32, (tile, tile), 0)
    chunks = site_rows.shape[2] // tile
    for chunk in range(chunks):
        at = slice(chunk * tile, (chunk + 1) * tile)
        wanted[:, at] = jnp.where(place_at == sites[0, 0, :, at], 1.0, 0.0).astype(jnp.bfloat16)
    for load in loads[9:]:
        load.wait()
    arrived(has_up, to_down, above)
    arrived(has_down, to_up, below)
    packed[...] += rows_product(row_dft.at[1], halo_rows[...])
    pl.when(has_left)(to_left.start)
    pl.when(has_right)(to_right.start)
    sums[...] = cols_product(packed[...], col_dft.at[0])
    plus[...] = jnp.zeros_like(plus)
    minus[...] = jnp.zeros_like(minus)
    swap_weights.wait()
    swap_spectra.wait()
    arrived(has_left, to_right, left)
    arrived(has_right, to_left, right)
    total = sums[...] + cols_product(halo_cols[...], col_dft.at[1])
    full = sum(dot(expand[...], piece) for piece in bf16_pieces(total, 3))
    scale = 1.0 / (ext * ext)
    spec_re[...] = (full[:BAND, :BAND] - full[BAND:, BAND:]) * scale
    spec_im[...] = (full[BAND:, :BAND] + full[:BAND, BAND:]) * -scale

    def inward(at, pair, k):
        k_re, k_im = kernels[at, k, 0], kernels[at, k, 1]
        re, im = spec_re[...], spec_im[...]
        product = jnp.concatenate([k_re * re - k_im * im, k_re * im + k_im * re], axis=0)
        hi, mid, lo = bf16_pieces(product, 3)
        upper, lower = jnp.concatenate([hi, mid], axis=1), jnp.concatenate([hi, lo], axis=1)
        inner = dot(upper, first[0]) + dot(upper, first[1]) + dot(lower, first[2])
        a, c, d, b = inner[:half, :half], inner[:half, half:], inner[half:, :half], inner[half:, half:]
        for slot, y in zip(pair, ((a - b, a + b), (c + d, d - c))):
            for side, part in enumerate(y):
                at_side = slice(side * half, (side + 1) * half)
                hi, mid, lo = bf16_pieces(part, 3)
                slot[0, :half, at_side] = hi
                slot[0, half:, at_side] = mid
                slot[1, :half, at_side] = hi
                slot[1, half:, at_side] = lo

    def outward(pair, weight):
        of_re, of_im = (
            dot(second[0], slot[0]) + dot(second[1], slot[0]) + dot(second[2], slot[1]) for slot in pair
        )
        a, c, d, b = of_re[:half], of_re[half:], of_im[:half], of_im[half:]
        p_re, p_im, m_re, m_im = a - b, c + d, a + b, d - c
        plus[...] += weight * (p_re * p_re + p_im * p_im)
        minus[...] += weight * (m_re * m_re + m_im * m_im)

    last = spectra.shape[0] - 1
    inward(0, slots[0], 0)
    inward(1, slots[1], 0)

    @pl.loop(0, spectra.shape[0] // 2)
    def _(i):
        k = 2 * i
        following = jnp.minimum(k + 2, last)
        inward(0, slots[2], k + 1)
        outward(slots[0], my_weights[pl.ds(k, 1), :])
        inward(1, slots[3], k + 1)
        outward(slots[1], other_weights[pl.ds(k, 1), :])
        inward(0, slots[0], following)
        outward(slots[2], my_weights[pl.ds(k + 1, 1), :])
        inward(1, slots[1], following)
        outward(slots[3], other_weights[pl.ds(k + 1, 1), :])

    hi, mid, lo = bf16_pieces(minus[...], 3)
    turned = dot(flip_rows[...], jnp.concatenate([hi, mid], axis=0)) + dot(flip_rows[:, :half], lo)
    both = jnp.concatenate([turned, plus[...]], axis=0)
    hi, mid, lo = bf16_pieces(both[:, half:], 3)
    turned = dot(jnp.concatenate([hi, mid], axis=1), flip_cols[...]) + dot(lo, flip_cols[:half])
    picture = jnp.concatenate([turned, both[:, :half]], axis=1)
    image[...] = picture
    grad_rows = (pltpu.roll(picture, tile - 1, 0) - pltpu.roll(picture, 1, 0)) * 0.5
    grad_cols = (pltpu.roll(picture, tile - 1, 1) - pltpu.roll(picture, 1, 1)) * 0.5
    slope = jnp.sqrt(grad_rows * grad_rows + grad_cols * grad_cols)
    field = (picture - LEVEL) / jnp.maximum(slope, SLOPE_FLOOR)
    field_hi, field_lo = bf16_pieces(field, 2)

    def to_other(source, target, number):
        return pltpu.make_async_remote_copy(
            src_ref=source, dst_ref=target, send_sem=near_send.at[n_near + number],
            recv_sem=near_recv.at[n_near + number], device_id={"ka": 1 - ka}, device_id_type=MESH,
        )

    send_image = to_other(image, image_in, 0)
    send_errors = to_other(errors, errors_in, 1)
    send_image.start()

    for chunk in range(chunks):
        at = slice(chunk * tile, (chunk + 1) * tile)
        sampled = dot(field_hi, wanted[:, at]) + dot(field_lo, wanted[:, at])
        sampled = jnp.where(place_at == sites[1, 0, :, at], sampled, 0.0)
        errors[:, at] = jnp.sum(sampled, axis=0, keepdims=True)

    found = errors[...]
    size = jnp.abs(found)
    limit = limits[ka].astype(jnp.float32) / 8.0
    peak = jnp.max(size, axis=1, keepdims=True)
    total = jnp.sum(1.0 / (1.0 + jnp.exp(SHARPNESS * (size - limit))), axis=1, keepdims=True)
    lane = lax.broadcasted_iota(jnp.int32, (1, 128), 1)
    is_peak = lane < 64
    near[place] = jnp.where(is_peak, peak, total)

    def small(buffer, mine, d, peer, send, recv):
        return pltpu.make_async_remote_copy(
            src_ref=buffer.at[mine], dst_ref=buffer.at[mine], send_sem=send.at[d], recv_sem=recv.at[mine],
            device_id=peer, device_id_type=MESH,
        )

    def swapped(buffer, mine, peers, send, recv):
        copies = [small(buffer, mine, d, peer, send, recv) for d, (_, peer) in peers]
        for copy in copies:
            copy.start()
        for d, (spot, peer) in peers:
            small(buffer, spot, d, peer, send, recv).wait_recv()
        return copies

    near_peers = [(d, near_peer(d)) for d in range(1, n_near)]

    @pl.when(has_down)
    def _():
        pl.semaphore_wait(ready, n_tx - 1 - tx)

    copies = swapped(near, place, near_peers, near_send, near_recv)
    of_iteration = []
    for t in range(n_ka):
        found_t = [near[y * n_ka + t] for y in range(n_ty)]
        of_iteration.append(
            jnp.where(is_peak, functools.reduce(jnp.maximum, found_t), functools.reduce(jnp.add, found_t))
        )
    far[tx] = jnp.where((lane & 32) == 0, of_iteration[0], of_iteration[1])
    far_copies = [small(far, tx, d, far_peer(d)[1], far_send, far_recv) for d in range(1, n_tx)]
    for copy in far_copies:
        copy.start()
    send_errors.start()
    send_image.wait()
    send_errors.wait()
    image_out[...] = jnp.where(ka == ITERS - 1, image[...], image_in[...])
    errors_out[0, 0, 0:1, :] = jnp.where(ka == 0, errors[...], errors_in[...])
    errors_out[0, 0, 1:2, :] = jnp.where(ka == 0, errors_in[...], errors[...])
    saves[1].start()
    saves[2].start()
    pl.when(has_up)(to_up.wait_send)
    pl.when(has_down)(to_down.wait_send)
    pl.when(has_left)(to_left.wait_send)
    pl.when(has_right)(to_right.wait_send)
    for copy in copies:
        copy.wait_send()
    for d in range(1, n_tx):
        spot, peer = far_peer(d)
        small(far, spot, 0, peer, far_send, far_recv).wait_recv()
    stats_out[...] = jnp.where(is_peak, jnp.max(far[...], axis=0), jnp.sum(far[...], axis=0))
    saves[3].start()
    for copy in far_copies:
        copy.wait_send()
    for save in saves:
        save.wait()


def deliver_kernel(
    n_sites, image, mask, errors, stats, intensity, new_mask, edge_errors, peaks, shares,
    image_at, mask_at, errors_at, stats_at, peaks_at, shares_at, sem,
):
    held = ((stats, stats_at, None), (image, image_at, intensity), (mask, mask_at, new_mask), (errors, errors_at, edge_errors))
    loads = [pltpu.make_async_copy(src, at, sem.at[0, i]) for i, (src, at, _) in enumerate(held)]
    copies = [pltpu.make_async_copy(at, dst, sem.at[1, i]) for i, (_, at, dst) in enumerate(held) if i > 0]
    for load in loads:
        load.start()
    loads[0].wait()
    final = stats_at[...]
    for t in range(ITERS):
        peaks_at[t] = final[0, 32 * t]
        shares_at[t] = final[0, 64 + 32 * t] * (1.0 / n_sites)
    pairs = ((peaks_at, peaks), (shares_at, shares))
    copies += [pltpu.make_async_copy(at, dst, sem.at[1, 4 * i]) for i, (at, dst) in enumerate(pairs)]
    for copy in copies[3:]:
        copy.start()
    for load, copy in zip(loads[1:], copies):
        load.wait()
        copy.start()
    for copy in copies:
        copy.wait()


def shards(
    mask_raster, frag_rows, frag_cols, frag_length, frag_orient, frag_moves,
    site_rows, site_cols, spectra, weights, tolerance,
):
    f32, i32, bf16 = jnp.float32, jnp.int32, jnp.bfloat16
    tile = mask_raster.shape[0]
    half = tile // 2
    n_sites = site_rows.shape[2]
    kernels = spectra.shape[0]
    n_near = lax.axis_size("ty") * lax.axis_size("ka")
    n_tx = lax.axis_size("tx")
    constants = [jnp.asarray(t) for t in tables(tile)]
    hbm = pl.BlockSpec(memory_space=pltpu.HBM)
    dma = pltpu.SemaphoreType.DMA
    errors_shape = jax.ShapeDtypeStruct((1, 1, ITERS, n_sites), f32)
    square = jax.ShapeDtypeStruct((tile, tile), f32)
    V = pltpu.VMEM
    new_mask, image, errors, stats = pl.pallas_call(
        opc_kernel,
        name="opc_kernel",
        out_shape=(square, square, errors_shape, jax.ShapeDtypeStruct((1, 128), f32)),
        in_specs=[hbm] * 18,
        out_specs=(hbm,) * 4,
        scratch_shapes=[
            V((tile, tile), f32), V((4, *frag_rows.shape), i32), V(frag_moves.shape, i32),
            V((2, *site_rows.shape), i32), V((2, *spectra.shape), f32), V((kernels, tile), f32),
            V((kernels, tile), f32), pltpu.SMEM(weights.shape, f32), pltpu.SMEM(tolerance.shape, i32),
            *(V(c.shape, c.dtype) for c in constants),
            V((2 * HALO, tile), f32), V((PACKED, tile), f32), V((PACKED, 2 * HALO), f32), V((PACKED, 2 * BAND), f32),
            V((BAND, BAND), f32), V((BAND, BAND), f32),
            V((tile, n_sites), bf16),
            V((half, tile), f32), V((half, tile), f32), V((tile, tile), f32), V((tile, tile), f32),
            V((1, n_sites), f32), V((1, n_sites), f32), V((n_near, 1, 128), f32), V((n_tx, 1, 128), f32),
            V((tile, tile), f32), V((tile, tile), f32), V(errors_shape.shape, f32), V((1, 128), f32),
            *([V((2, tile, tile), bf16)] * 8), dma((18,)), dma((4,)), dma((6,)), dma((6,)), dma((n_near + 2,)), dma((n_near + 2,)), dma((n_tx,)), dma((n_tx,)),
            pltpu.SemaphoreType.REGULAR,
        ],
        compiler_params=pltpu.CompilerParams(collective_id=0, has_side_effects=True),
        cost_estimate=pl.CostEstimate(flops=4 * 10**9, bytes_accessed=4 * 10**6, transcendentals=0),
    )(
        mask_raster, frag_rows, frag_cols, frag_length, frag_orient, frag_moves, site_rows, site_cols,
        spectra, weights, tolerance, *constants,
    )
    pair = jax.ShapeDtypeStruct((ITERS,), f32)
    return pl.pallas_call(
        functools.partial(deliver_kernel, float(n_sites * n_tx * lax.axis_size("ty"))),
        name="deliver_kernel",
        out_shape=(square, square, errors_shape, pair, pair),
        in_specs=[hbm] * 4,
        out_specs=(hbm,) * 5,
        scratch_shapes=[
            V((tile, tile), f32), V((tile, tile), f32), V(errors_shape.shape, f32), V((1, 128), f32),
            pltpu.SMEM((ITERS,), f32), pltpu.SMEM((ITERS,), f32), dma((2, 5)),
        ],
    )(image, new_mask, errors, stats)


def solution(mesh):
    placed = (
        P(("groups", "tx"), "ty"),
        P(("groups", "tx"), "ty", None),
        P(("groups", "tx"), "ty", None),
        P(("groups", "tx"), "ty", None),
        P(("groups", "tx"), "ty", None),
        P(("groups", "tx"), "ty", None, None),
        P(("groups", "tx"), "ty", None),
        P(("groups", "tx"), "ty", None),
        P("ka", None, None, None),
        P("ka"),
        P(),
    )
    return jax.shard_map(
        shards,
        mesh=mesh,
        in_specs=placed,
        out_specs=(
            P(("groups", "tx"), "ty"),
            P(("groups", "tx"), "ty"),
            P(("groups", "tx"), "ty", None, None),
            P("groups"),
            P("groups"),
        ),
        check_vma=False,
    )
```
